32 devices in a mesh: section: 2 (over x), ctx: 4 (over z), tp: 4 (over y, core).
Axes of the slice: x: 2, y: 2, z: 4, core: 2. Of those that a mesh axis runs over, the one named last changes fastest.
Arguments:
- boundary: bfloat16 [2, 2, 1024, 2048], P('section', None, 'ctx', 'tp'), may hold values from -6 to 6
- doc_ids: int32 [2, 1024], replicated, may hold values from 0 to 3, never falling along the last dimension, each value on 1 to 512 neighbouring positions
- qkv_weight: bfloat16 [2, 3, 2048, 2048], P('section', None, 'ctx', 'tp'), may hold values from -0.125 to 0.125
- qkv_bias: bfloat16 [2, 3, 2048], P('section', None, ('tp', 'ctx')), may hold values from -3 to 3
- out_weight: bfloat16 [2, 2048, 2048], P('section', 'tp', 'ctx'), may hold values from -0.5 to 0.5
- out_bias: bfloat16 [2, 2048], P('section', ('tp', 'ctx')), may hold values from -3 to 3
- fc1_weight: bfloat16 [2, 2048, 8192], P('section', 'ctx', 'tp'), may hold values from -0.125 to 0.125
- fc1_bias: bfloat16 [2, 8192], P('section', ('tp', 'ctx')), may hold values from -3 to 3
- fc2_weight: bfloat16 [2, 8192, 2048], P('section', 'tp', 'ctx'), may hold values from -0.0625 to 0.0625
- fc2_bias: bfloat16 [2, 2048], P('section', ('tp', 'ctx')), may hold values from -3 to 3
- norm_gain: bfloat16 [2, 2048], P('section', ('tp', 'ctx')), may hold values from 0.099609375 to 1.8984375
- norm_shift: bfloat16 [2, 2048], P('section', ('tp', 'ctx')), may hold values from -3 to 3
Outputs:
- acts: bfloat16 [2, 2, 1024, 2048], P('section', None, 'ctx', 'tp')
- input_grads: bfloat16 [2, 2, 1024, 2048], P('section', None, 'ctx', 'tp')
- grad_qkv_weight: float32 [2, 3, 2048, 2048], P('section', None, 'ctx', 'tp')
- grad_qkv_bias: float32 [2, 3, 2048], P('section', None, ('tp', 'ctx'))
- grad_out_weight: float32 [2, 2048, 2048], P('section', 'tp', 'ctx')
- grad_out_bias: float32 [2, 2048], P('section', ('tp', 'ctx'))
- grad_fc1_weight: float32 [2, 2048, 8192], P('section', 'ctx', 'tp')
- grad_fc1_bias: float32 [2, 8192], P('section', ('tp', 'ctx'))
- grad_fc2_weight: float32 [2, 8192, 2048], P('section', 'tp', 'ctx')
- grad_fc2_bias: float32 [2, 2048], P('section', ('tp', 'ctx'))
- grad_norm_gain: float32 [2, 2048], P('section', ('tp', 'ctx'))
- grad_norm_shift: float32 [2, 2048], P('section', ('tp', 'ctx'))
The draws below stay inside these ranges and needn't reach their ends.
Inputs may be any that keep to these rules, and one draw needn't show every extreme that they name: `doc_ids`: in each sequence the ids never fall; every id 0 to 3 covers 1 to 512 consecutive positions, and some id covers exactly 512.
All inputs are finite; a program needn't handle non-finite values.
Results may differ from the reference program's by a relative error of at most 0.024.
Values may be sent and summed in bfloat16 or wider, within the bound.
A program may use at most 320 MiB of HBM per device.

```python
import math
import jax
import jax.numpy as jnp
import numpy as np
from jax import lax

D = 2048
H = 32
HD = 64
FF = 8192
ROT = 32
SEQ = 1024
MICRO = 2
DOCS = 4
N_SECTION = 2


def level_of(key, shape, split, smallest, largest):
    level = 1.0
    for position, parts in split:
        heights = jax.random.uniform(jax.random.fold_in(jax.random.fold_in(key, 6), position), (parts,), jnp.float32, smallest / len(split), largest / len(split))
        level = level * jnp.repeat(jnp.exp(heights), shape[position] // parts).reshape((-1,) + (1,) * (len(shape) - 1 - position))
    return level


def split_up(number_of, total, reach, skew):
    loads = [(1 << 20) // math.isqrt(grade ** skew) + 1 for grade in range(2, number_of + 1)]
    spare, given = total - reach - (number_of - 1), [1] * (number_of - 1)
    while spare > 0:
        movable = [i for i in range(number_of - 1) if given[i] < reach]
        whole, left = sum([loads[i] for i in movable]), spare
        for i in movable:
            addition = min(reach - given[i], max(1, left * loads[i] // whole), spare)
            given[i] = given[i] + addition
            spare = spare - addition
    return np.array([reach] + given)


def uneven(stream_key, amount, total, limit, slope):
    if amount == 2:
        one = jax.random.randint(stream_key, (), max(1, total - limit), min(limit, total - 1) + 1)
        return jnp.stack([one, total - one])
    tallies = jnp.asarray(split_up(amount, total, limit, slope), jnp.int32)
    pairs = (amount - 1) // 2
    giver, taker = tallies[1:1 + 2 * pairs:2], tallies[2:2 + 2 * pairs:2]
    room = jnp.minimum(giver - 1, limit - taker)
    shifted = jax.random.randint(jax.random.fold_in(stream_key, 1), (pairs,), 0, 1 << 20) % (room + 1)
    tallies = tallies.at[1:1 + 2 * pairs:2].set(giver - shifted).at[2:2 + 2 * pairs:2].set(taker + shifted)
    return tallies[jax.random.permutation(jax.random.fold_in(stream_key, 2), amount)]


def centred(own_key, dims, deviation, limit, split=(), kind=jnp.bfloat16):
    factor_of = level_of(own_key, dims, split, -0.22, 0.18) if split else 1.0
    entries = jax.random.normal(own_key, dims, jnp.float32) * deviation * factor_of
    return jnp.minimum(jnp.maximum(entries, -limit), limit).astype(kind)


def setup_inputs(seed: int = 0) -> dict:
    key_of = jax.random.split(jax.random.key(seed), 13)
    boundary = centred(key_of[0], (N_SECTION, MICRO, SEQ, D), 1.0, 6.0, ((0, 2), (2, 4), (3, 4)))
    doc_ids = jax.vmap(lambda own: jnp.searchsorted(jnp.cumsum(uneven(own, DOCS, SEQ, SEQ // 2, 0)), jnp.arange(SEQ), side="right"))(jax.random.split(key_of[1], MICRO)).reshape((MICRO, SEQ)).astype(jnp.int32)
    qkv_weight = centred(key_of[2], (N_SECTION, 3, D, D), D ** -0.5, 0.125, ((0, 2), (2, 4), (3, 4)))
    qkv_bias = centred(key_of[3], (N_SECTION, 3, D), 0.5, 3.0, ((0, 2), (2, 16)))
    out_weight = centred(key_of[4], (N_SECTION, D, D), (D // 16) ** -0.5, 0.5, ((0, 2), (1, 4), (2, 4)))
    out_bias = centred(key_of[5], (N_SECTION, D), 0.5, 3.0, ((0, 2), (1, 16)))
    fc1_weight = centred(key_of[6], (N_SECTION, D, FF), D ** -0.5, 0.125, ((0, 2), (1, 4), (2, 4)))
    fc1_bias = centred(key_of[7], (N_SECTION, FF), 0.5, 3.0, ((0, 2), (1, 16)))
    fc2_weight = centred(key_of[8], (N_SECTION, FF, D), FF ** -0.5, 0.0625, ((0, 2), (1, 4), (2, 4)))
    fc2_bias = centred(key_of[9], (N_SECTION, D), 0.5, 3.0, ((0, 2), (1, 16)))
    norm_gain = jnp.clip(1.0 + 0.18 * jax.random.normal(key_of[10], (N_SECTION, D), jnp.float32), 0.099609375, 1.8984375).astype(jnp.bfloat16)
    norm_shift = centred(key_of[11], (N_SECTION, D), 0.5, 3.0, ((0, 2), (1, 16)))
    return {"boundary": boundary, "doc_ids": doc_ids, "qkv_weight": qkv_weight, "qkv_bias": qkv_bias, "out_weight": out_weight, "out_bias": out_bias, "fc1_weight": fc1_weight, "fc1_bias": fc1_bias, "fc2_weight": fc2_weight, "fc2_bias": fc2_bias, "norm_gain": norm_gain, "norm_shift": norm_shift}


EPS = 1e-05
GELU_C = 0.7978845608028654
GELU_K = 0.044715

def gelu(value):
    inner = jnp.tanh(GELU_C * (value + GELU_K * value * value * value))
    return 0.5 * value * (1.0 + inner)

def gelu_slope(value):
    inner = jnp.tanh(GELU_C * (value + GELU_K * value * value * value))
    return 0.5 * (1.0 + inner) + 0.5 * value * (1.0 - inner * inner) * GELU_C * (1.0 + 3.0 * GELU_K * value * value)

def rope_tables(positions):
    half = ROT // 2
    freq = 10000.0 ** (-(jnp.arange(half).astype(jnp.float32) * 2.0 / ROT))
    angle = positions.astype(jnp.float32)[:, None] * freq[None, :]
    return (jnp.cos(angle), jnp.sin(angle))

def rotate(field, cosine, sine, sign):
    half = ROT // 2
    first = field[..., :half]
    second = field[..., half:ROT]
    cosine = cosine[:, None, :]
    sine = sine[:, None, :] * sign
    return jnp.concatenate([first * cosine - second * sine, second * cosine + first * sine, field[..., ROT:]], axis=-1)

def doc_layout(ids):
    start = lax.optimization_barrier(jnp.sum((ids[None, :] < ids[:, None]).astype(jnp.int32), axis=1))
    where_at = jnp.arange(SEQ, dtype=jnp.int32)
    allowed = (where_at[None, :] <= where_at[:, None]) & (ids[None, :] == ids[:, None])
    return (where_at - start, allowed)

def forward_pieces(layer_in, positions, allowed, params):
    w_qkv, b_qkv, w_out, b_out, w_up, b_up, w_down, b_down, gain, shift = params
    wide_in = layer_in.astype(jnp.float32)
    row_mean = lax.optimization_barrier(jnp.mean(wide_in, axis=1, keepdims=True))
    variance = lax.optimization_barrier(jnp.mean(wide_in * wide_in, axis=1, keepdims=True)) - row_mean * row_mean
    inverse_std = lax.rsqrt(variance + EPS)
    centered = (wide_in - row_mean) * inverse_std
    normed = (centered * gain.astype(jnp.float32) + shift.astype(jnp.float32)).astype(jnp.bfloat16)
    projected = jnp.stack([jnp.dot(normed, w_qkv[which], preferred_element_type=jnp.float32) for which in range(3)])
    projected = projected + b_qkv.astype(jnp.float32)[:, None, :]
    cosine, sine = rope_tables(positions)
    query = rotate(projected[0].reshape(SEQ, H, HD), cosine, sine, 1.0).astype(jnp.bfloat16)
    keys = rotate(projected[1].reshape(SEQ, H, HD), cosine, sine, 1.0).astype(jnp.bfloat16)
    values = projected[2].reshape(SEQ, H, HD).astype(jnp.bfloat16)

    def one_head(inputs):
        query_head, key_head, value_head = inputs
        scores = jnp.dot(query_head, key_head.T, preferred_element_type=jnp.float32) * HD ** (-0.5)
        totals = lax.optimization_barrier(jnp.sum(jnp.where(allowed, jnp.exp(scores), 0.0), axis=1))
        log_total = jnp.log(totals)
        probs = jnp.where(allowed, jnp.exp(scores - log_total[:, None]), 0.0).astype(jnp.bfloat16)
        result = jnp.dot(probs, value_head, preferred_element_type=jnp.float32).astype(jnp.bfloat16)
        return (result, log_total)
    head_outs, log_total = lax.map(one_head, (query.transpose(1, 0, 2), keys.transpose(1, 0, 2), values.transpose(1, 0, 2)))
    attended = head_outs.transpose(1, 0, 2).reshape(SEQ, D)
    hidden_pre = jnp.dot(normed, w_up, preferred_element_type=jnp.float32) + b_up.astype(jnp.float32)
    hidden = gelu(hidden_pre).astype(jnp.bfloat16)
    result = wide_in + jnp.dot(attended, w_out, preferred_element_type=jnp.float32)
    result = result + jnp.dot(hidden, w_down, preferred_element_type=jnp.float32)
    result = result + b_out.astype(jnp.float32) + b_down.astype(jnp.float32)
    pieces = (centered, inverse_std, normed, query, keys, values, attended, log_total, hidden_pre, hidden)
    return (result.astype(jnp.bfloat16), pieces)

def backward_pieces(incoming, pieces, positions, allowed, params):
    w_qkv, b_qkv, w_out, b_out, w_up, b_up, w_down, b_down, gain, shift = params
    centered, inverse_std, normed, query, keys, values, attended, log_total, hidden_pre, hidden = pieces
    wide_grad = incoming.astype(jnp.float32)
    grad_out_bias = lax.optimization_barrier(jnp.sum(wide_grad, axis=0))
    grad_out = jnp.dot(attended.T, incoming, preferred_element_type=jnp.float32)
    d_attended = jnp.dot(incoming, w_out.T, preferred_element_type=jnp.float32).astype(jnp.bfloat16)
    grad_down = jnp.dot(hidden.T, incoming, preferred_element_type=jnp.float32)
    d_pre = jnp.dot(incoming, w_down.T, preferred_element_type=jnp.float32) * gelu_slope(hidden_pre)
    grad_up_bias = lax.optimization_barrier(jnp.sum(d_pre, axis=0))
    d_hidden = d_pre.astype(jnp.bfloat16)
    grad_up = jnp.dot(normed.T, d_hidden, preferred_element_type=jnp.float32)
    d_heads = d_attended.reshape(SEQ, H, HD).transpose(1, 0, 2)
    out_heads = attended.reshape(SEQ, H, HD).transpose(1, 0, 2)

    def one_head(inputs):
        query_head, key_head, value_head, out_head, grad_head, lse_head = inputs
        scores = jnp.dot(query_head, key_head.T, preferred_element_type=jnp.float32) * HD ** (-0.5)
        probs = jnp.where(allowed, jnp.exp(scores - lse_head[:, None]), 0.0)
        delta = lax.optimization_barrier(jnp.sum(grad_head.astype(jnp.float32) * out_head.astype(jnp.float32), axis=1))
        d_probs = jnp.dot(grad_head, value_head.T, preferred_element_type=jnp.float32)
        d_scores = (probs * (d_probs - delta[:, None]) * HD ** (-0.5)).astype(jnp.bfloat16)
        d_query = jnp.dot(d_scores, key_head, preferred_element_type=jnp.float32)
        d_key = jnp.dot(d_scores.T, query_head, preferred_element_type=jnp.float32)
        d_value = jnp.dot(probs.astype(jnp.bfloat16).T, grad_head, preferred_element_type=jnp.float32)
        return (d_query, d_key, d_value)
    d_query, d_key, d_value = lax.map(one_head, (query.transpose(1, 0, 2), keys.transpose(1, 0, 2), values.transpose(1, 0, 2), out_heads, d_heads, log_total))
    cosine, sine = rope_tables(positions)
    d_projected = jnp.stack([rotate(d_query.transpose(1, 0, 2), cosine, sine, -1.0), rotate(d_key.transpose(1, 0, 2), cosine, sine, -1.0), d_value.transpose(1, 0, 2)]).reshape(3, SEQ, D)
    grad_qkv_bias = lax.optimization_barrier(jnp.sum(d_projected, axis=1))
    d_qkv = d_projected.astype(jnp.bfloat16)
    grad_qkv = jnp.stack([jnp.dot(normed.T, d_qkv[which], preferred_element_type=jnp.float32) for which in range(3)])
    d_normed = jnp.dot(d_hidden, w_up.T, preferred_element_type=jnp.float32)
    for which in range(3):
        d_normed = d_normed + jnp.dot(d_qkv[which], w_qkv[which].T, preferred_element_type=jnp.float32)
    grad_gain = lax.optimization_barrier(jnp.sum(d_normed * centered, axis=0))
    grad_shift = lax.optimization_barrier(jnp.sum(d_normed, axis=0))
    scaled = d_normed * gain.astype(jnp.float32)
    grad_in = wide_grad + inverse_std * (scaled - lax.optimization_barrier(jnp.mean(scaled, axis=1, keepdims=True)) - centered * lax.optimization_barrier(jnp.mean(scaled * centered, axis=1, keepdims=True)))
    grads = (grad_qkv, grad_qkv_bias, grad_out, grad_out_bias, grad_up, grad_up_bias, grad_down, grad_out_bias, grad_gain, grad_shift)
    return (grad_in.astype(jnp.bfloat16), grads)

def reference(boundary, doc_ids, qkv_weight, qkv_bias, out_weight, out_bias, fc1_weight, fc1_bias, fc2_weight, fc2_bias, norm_gain, norm_shift):
    weights = (qkv_weight, qkv_bias, out_weight, out_bias, fc1_weight, fc1_bias, fc2_weight, fc2_bias, norm_gain, norm_shift)
    first_params = tuple((array[0] for array in weights))
    second_params = tuple((array[1] for array in weights))

    def step(totals, inputs):
        layer_in, cotangent, ids = inputs
        positions, allowed = doc_layout(ids)
        middle, first_pieces = forward_pieces(layer_in, positions, allowed, first_params)
        final, second_pieces = forward_pieces(middle, positions, allowed, second_params)
        back_middle, second_grads = backward_pieces(cotangent, second_pieces, positions, allowed, second_params)
        back_first, first_grads = backward_pieces(back_middle, first_pieces, positions, allowed, first_params)
        totals = tuple((total + jnp.stack([one, two]) for total, one, two in zip(totals, first_grads, second_grads)))
        return (totals, (middle, final, back_first, back_middle))
    start = tuple((jnp.zeros(array.shape, jnp.float32) for array in weights))
    totals, outputs = lax.scan(step, start, (boundary[0], boundary[1], doc_ids))
    middle, final, back_first, back_middle = outputs
    acts = jnp.stack([middle, final])
    input_grads = jnp.stack([back_first, back_middle])
    return (acts, input_grads, totals[0], totals[1], totals[2], totals[3], totals[4], totals[5], totals[6], totals[7], totals[8], totals[9])
```

```python
import jax
import jax.numpy as jnp
from jax import lax
from jax.sharding import PartitionSpec as P

D = 2048
HD = 64
ROT = 32
EPS = 1e-05
GELU_C = 0.7978845608028654
GELU_K = 0.044715
BF16 = jnp.bfloat16
F32 = jnp.float32


def rope_tables(positions):
    half = ROT // 2
    freq = 10000.0 ** (-(jnp.arange(half).astype(F32) * 2.0 / ROT))
    angle = positions.astype(F32)[:, None] * freq[None, :]
    return (jnp.cos(angle), jnp.sin(angle))


def rotate(field, cosine, sine, sign):
    half = ROT // 2
    first = field[..., :half]
    second = field[..., half:ROT]
    cosine = cosine[:, None, :]
    sine = sine[:, None, :] * sign
    return jnp.concatenate(
        [first * cosine - second * sine, second * cosine + first * sine, field[..., ROT:]], axis=-1
    )


def doc_layout(ids):
    length = ids.shape[0]
    start = jnp.sum((ids[None, :] < ids[:, None]).astype(jnp.int32), axis=1)
    at = jnp.arange(length, dtype=jnp.int32)
    allowed = (at[None, :] <= at[:, None]) & (ids[None, :] == ids[:, None])
    cosine, sine = rope_tables(at - start)
    return (allowed, cosine, sine)


def gather_rows(block):
    return lax.all_gather(
        lax.all_gather(block, "ctx", axis=0, tiled=True), "tp", axis=1, tiled=True
    )


def scatter_rows(partial):
    return lax.psum_scatter(
        lax.psum_scatter(partial, "tp", scatter_dimension=1, tiled=True),
        "ctx",
        scatter_dimension=0,
        tiled=True,
    )


def swap_section(value):
    return lax.ppermute(value, "section", [(0, 1), (1, 0)])


def both_layers(own):
    first = lax.axis_index("section") == 0
    other = swap_section(own)
    return (jnp.where(first, own, other), jnp.where(first, other, own))


def forward(x_full, layout, params):
    w_qkv, b_qkv, w_out, w_up, b_up, w_down, gain, shift = params
    allowed, cosine, sine = layout
    tokens = x_full.shape[0]
    heads = w_qkv.shape[2] // HD
    wide = x_full.astype(F32)
    mean = jnp.mean(wide, axis=1, keepdims=True)
    variance = jnp.mean(wide * wide, axis=1, keepdims=True) - mean * mean
    inverse_std = lax.rsqrt(variance + EPS)
    normed = (
        (wide - mean) * inverse_std * gain.astype(F32)[None] + shift.astype(F32)[None]
    ).astype(BF16)
    projected = (
        jnp.einsum("td,cde->cte", normed, w_qkv, preferred_element_type=F32)
        + b_qkv.astype(F32)[:, None, :]
    )
    query = rotate(projected[0].reshape(tokens, heads, HD), cosine, sine, 1.0).astype(BF16)
    key = rotate(projected[1].reshape(tokens, heads, HD), cosine, sine, 1.0).astype(BF16)
    value = projected[2].reshape(tokens, heads, HD).astype(BF16)
    scores = jnp.einsum("thd,shd->hts", query, key, preferred_element_type=F32) * HD ** (-0.5)
    totals = jnp.sum(jnp.where(allowed[None], jnp.exp(scores), 0.0), axis=2)
    log_total = jnp.log(totals)
    probs = jnp.where(allowed[None], jnp.exp(scores - log_total[:, :, None]), 0.0).astype(BF16)
    attended = (
        jnp.einsum("hts,shd->thd", probs, value, preferred_element_type=F32)
        .astype(BF16)
        .reshape(tokens, heads * HD)
    )
    hidden_pre = jnp.dot(normed, w_up, preferred_element_type=F32) + b_up.astype(F32)
    inner = jnp.tanh(GELU_C * (hidden_pre + GELU_K * hidden_pre * hidden_pre * hidden_pre))
    hidden = (0.5 * hidden_pre * (1.0 + inner)).astype(BF16)
    partial = jnp.dot(attended, w_out, preferred_element_type=F32) + jnp.dot(
        hidden, w_down, preferred_element_type=F32
    )
    saved = (mean, inverse_std, normed, query, key, value, attended, log_total, hidden_pre, hidden)
    return (partial.astype(BF16), saved)


def backward(g_full, saved, layout, params):
    w_qkv, b_qkv, w_out, w_up, b_up, w_down, gain, shift = params
    mean, inverse_std, normed, query, key, value, attended, log_total, hidden_pre, hidden = saved
    allowed, cosine, sine = layout
    tokens, heads = query.shape[:2]
    grad_out = jnp.einsum("tk,te->ke", attended, g_full, preferred_element_type=F32)
    d_attended = jnp.einsum("te,ke->tk", g_full, w_out, preferred_element_type=F32).astype(BF16)
    grad_down = jnp.einsum("tf,te->fe", hidden, g_full, preferred_element_type=F32)
    inner = jnp.tanh(GELU_C * (hidden_pre + GELU_K * hidden_pre * hidden_pre * hidden_pre))
    slope = 0.5 * (1.0 + inner) + 0.5 * hidden_pre * (1.0 - inner * inner) * GELU_C * (
        1.0 + 3.0 * GELU_K * hidden_pre * hidden_pre
    )
    d_pre = jnp.einsum("te,fe->tf", g_full, w_down, preferred_element_type=F32) * slope
    grad_up_bias = jnp.sum(d_pre, axis=0)
    d_hidden = d_pre.astype(BF16)
    grad_up = jnp.einsum("td,tf->df", normed, d_hidden, preferred_element_type=F32)
    d_heads = d_attended.reshape(tokens, heads, HD)
    out_heads = attended.reshape(tokens, heads, HD)
    delta = jnp.sum(d_heads.astype(F32) * out_heads.astype(F32), axis=2)
    scores = jnp.einsum("thd,shd->hts", query, key, preferred_element_type=F32) * HD ** (-0.5)
    probs = jnp.where(allowed[None], jnp.exp(scores - log_total[:, :, None]), 0.0)
    d_probs = jnp.einsum("thd,shd->hts", d_heads, value, preferred_element_type=F32)
    d_scores = (probs * (d_probs - delta.T[:, :, None]) * HD ** (-0.5)).astype(BF16)
    d_query = jnp.einsum("hts,shd->thd", d_scores, key, preferred_element_type=F32)
    d_key = jnp.einsum("hts,thd->shd", d_scores, query, preferred_element_type=F32)
    d_value = jnp.einsum("hts,thd->shd", probs.astype(BF16), d_heads, preferred_element_type=F32)
    d_projected = jnp.stack(
        [rotate(d_query, cosine, sine, -1.0), rotate(d_key, cosine, sine, -1.0), d_value]
    ).reshape(3, tokens, heads * HD)
    grad_qkv_bias = jnp.sum(d_projected, axis=1)
    d_qkv = d_projected.astype(BF16)
    grad_qkv = jnp.einsum("td,cte->cde", normed, d_qkv, preferred_element_type=F32)
    partial = jnp.einsum("cte,cde->td", d_qkv, w_qkv, preferred_element_type=F32) + jnp.einsum(
        "tf,df->td", d_hidden, w_up, preferred_element_type=F32
    )
    return (partial.astype(BF16), (grad_qkv, grad_qkv_bias, grad_out, grad_up, grad_up_bias, grad_down))


def shards(
    boundary,
    doc_ids,
    qkv_weight,
    qkv_bias,
    out_weight,
    out_bias,
    fc1_weight,
    fc1_bias,
    fc2_weight,
    fc2_bias,
    norm_gain,
    norm_shift,
):
    section = lax.axis_index("section")
    ctx = lax.axis_index("ctx")
    tp = lax.axis_index("tp")
    first = section == 0
    tokens, part = boundary.shape[2], boundary.shape[3]
    n_ctx = lax.axis_size("ctx")
    own = boundary[0]
    mine = lax.dynamic_index_in_dim(own, section, 0, keepdims=False)
    theirs = swap_section(lax.dynamic_index_in_dim(own, 1 - section, 0, keepdims=False))
    x_block = jnp.where(first, mine, theirs)
    cotangent = jnp.where(first, theirs, mine)
    ids = lax.dynamic_index_in_dim(doc_ids, section, 0, keepdims=False)
    layout = doc_layout(ids)

    def turn(weight, split, join):
        return both_layers(
            lax.all_to_all(weight, "ctx", split_axis=split, concat_axis=join, tiled=True)
        )

    w_qkv = turn(qkv_weight[0], 2, 1)
    w_out = turn(out_weight[0], 0, 1)
    w_up = turn(fc1_weight[0], 1, 0)
    w_down = turn(fc2_weight[0], 0, 1)
    b_qkv = both_layers(qkv_bias[0])
    b_up = both_layers(fc1_bias[0])
    vectors = jnp.concatenate([out_bias, fc2_bias, norm_gain, norm_shift], axis=0)
    vectors = both_layers(
        lax.all_gather(
            lax.all_gather(vectors, "ctx", axis=1, tiled=True), "tp", axis=1, tiled=True
        )
    )
    params = [
        (w_qkv[l], b_qkv[l], w_out[l], w_up[l], b_up[l], w_down[l], vectors[l][2], vectors[l][3])
        for l in (0, 1)
    ]

    def own_part(vector):
        return lax.dynamic_slice_in_dim(vector, tp * part, part)

    def add_up(block, partial, layer):
        bias = own_part(vectors[layer][0]).astype(F32) + own_part(vectors[layer][1]).astype(F32)
        return (block.astype(F32) + scatter_rows(partial).astype(F32) + bias).astype(BF16)

    def rows_of(array):
        return lax.dynamic_slice_in_dim(array, ctx * tokens, tokens)

    def step_back(g_block, x_block, partial, saved, layer):
        d_normed = scatter_rows(partial).astype(F32)
        mean, inverse_std = (rows_of(saved[0]), rows_of(saved[1]))
        centered = (x_block.astype(F32) - mean) * inverse_std
        scaled = d_normed * own_part(vectors[layer][2]).astype(F32)
        terms = lax.psum((jnp.sum(scaled, axis=1), jnp.sum(scaled * centered, axis=1)), "tp")
        width = part * lax.axis_size("tp")
        grad = g_block.astype(F32) + inverse_std * (
            scaled - terms[0][:, None] / width - centered * (terms[1][:, None] / width)
        )
        return (grad.astype(BF16), jnp.sum(d_normed * centered, axis=0), jnp.sum(d_normed, axis=0))

    x_full = gather_rows(x_block)
    g_full = gather_rows(cotangent)
    partial, saved0 = forward(x_full, layout, params[0])
    act0 = add_up(x_block, partial, 0)
    x1_full = gather_rows(act0)
    partial, saved1 = forward(x1_full, layout, params[1])
    act1 = add_up(act0, partial, 1)
    partial, grads1 = backward(g_full, saved1, layout, params[1])
    grad1, gain1, shift1 = step_back(cotangent, act0, partial, saved1, 1)
    g1_full = gather_rows(grad1)
    partial, grads0 = backward(g1_full, saved0, layout, params[0])
    grad0, gain0, shift0 = step_back(grad1, x_block, partial, saved0, 0)

    def home(zero, one):
        sent = swap_section(jnp.where(first, one, zero).astype(BF16))
        return jnp.where(first, zero, one) + sent.astype(F32)

    def back(zero, one, split, join):
        total = home(zero, one)
        return lax.all_to_all(
            total.astype(BF16), "ctx", split_axis=split, concat_axis=join, tiled=True
        ).astype(F32)

    def pair(zero, one):
        sent = swap_section(jnp.where(first, one, zero))
        kept = jnp.where(first, zero, one)
        return jnp.where(first, jnp.stack([kept, sent]), jnp.stack([sent, kept]))[None]

    def column_sum(full):
        slab = lax.dynamic_slice_in_dim(
            full, tp * part + ctx * (part // n_ctx), part // n_ctx, axis=1
        )
        return jnp.sum(slab.astype(F32), axis=0)

    def over_ctx(zero, one):
        return lax.psum_scatter(home(zero, one), "ctx", scatter_dimension=0, tiled=True)

    bias_out = home(column_sum(g1_full), column_sum(g_full))[None]
    return (
        pair(act0, act1),
        pair(grad0, grad1),
        back(grads0[0], grads1[0], 1, 2)[None],
        home(grads0[1], grads1[1])[None],
        back(grads0[2], grads1[2], 1, 0)[None],
        bias_out,
        back(grads0[3], grads1[3], 0, 1)[None],
        home(grads0[4], grads1[4])[None],
        back(grads0[5], grads1[5], 1, 0)[None],
        bias_out,
        over_ctx(gain0, gain1)[None],
        over_ctx(shift0, shift1)[None],
    )


def from_behind(value, axis, steps):
    count = lax.axis_size(axis)
    leading, last = (max(0, -steps), min(count, count - steps))
    return lax.ppermute(value, axis, [(source, source + steps) for source in range(leading, last)])


def gelu(value):
    inner = jnp.tanh(GELU_C * (value + GELU_K * value * value * value))
    return 0.5 * value * (1.0 + inner)


def gelu_slope(value):
    inner = jnp.tanh(GELU_C * (value + GELU_K * value * value * value))
    return 0.5 * (1.0 + inner) + 0.5 * value * (1.0 - inner * inner) * GELU_C * (
        1.0 + 3.0 * GELU_K * value * value
    )


def local_layout(ids_full, ctx_index, tokens):
    length = ids_full.shape[0]
    local_ids = lax.dynamic_slice_in_dim(ids_full, ctx_index * tokens, tokens)
    start = jnp.sum((ids_full[None, :] < local_ids[:, None]).astype(jnp.int32), axis=1)
    query_at = ctx_index * tokens + jnp.arange(tokens, dtype=jnp.int32)
    key_at = jnp.arange(length, dtype=jnp.int32)
    allowed = (key_at[None, :] <= query_at[:, None]) & (ids_full[None, :] == local_ids[:, None])
    return (query_at - start, allowed)


def score_block(query, keys):
    return jnp.einsum("thd,shd->hts", query, keys, preferred_element_type=jnp.float32) * HD ** (
        -0.5
    )


def forward_layer(layer_in, ids_full, params, ctx_index):
    w_qkv, b_qkv, w_out, b_out, w_up, b_up, w_down, b_down, gain, shift = params
    tokens = layer_in.shape[0]
    heads = w_qkv.shape[2] // HD
    wide_in = layer_in.astype(jnp.float32)
    row_sums = lax.psum((jnp.sum(wide_in, axis=1), jnp.sum(wide_in * wide_in, axis=1)), "tp")
    row_mean = row_sums[0] / D
    variance = row_sums[1] / D - row_mean * row_mean
    inverse_std = lax.rsqrt(variance + EPS)
    centered = (wide_in - row_mean[:, None]) * inverse_std[:, None]
    normed_part = (centered * gain.astype(jnp.float32) + shift.astype(jnp.float32)).astype(
        jnp.bfloat16
    )
    normed = lax.all_gather(normed_part, "tp", axis=1, tiled=True)
    positions, allowed = local_layout(ids_full, ctx_index, tokens)
    cosine, sine = rope_tables(positions)
    projected = (
        jnp.einsum("td,cde->cte", normed, w_qkv, preferred_element_type=jnp.float32)
        + b_qkv.astype(jnp.float32)[:, None, :]
    )
    query = rotate(projected[0].reshape(tokens, heads, HD), cosine, sine, 1.0).astype(jnp.bfloat16)
    key_rot = rotate(projected[1].reshape(tokens, heads, HD), cosine, sine, 1.0).astype(
        jnp.bfloat16
    )
    value_part = projected[2].reshape(tokens, heads, HD).astype(jnp.bfloat16)
    key_all, value_all = (
        lax.all_gather(key_rot, "ctx", axis=0, tiled=True),
        lax.all_gather(value_part, "ctx", axis=0, tiled=True),
    )
    scores = score_block(query, key_all)
    totals = jnp.sum(jnp.where(allowed[None], jnp.exp(scores), 0.0), axis=2)
    log_total = jnp.log(totals)
    probs = jnp.where(allowed[None], jnp.exp(scores - log_total[:, :, None]), 0.0).astype(
        jnp.bfloat16
    )
    attended = (
        jnp.einsum("hts,shd->thd", probs, value_all, preferred_element_type=jnp.float32)
        .astype(jnp.bfloat16)
        .reshape(tokens, heads * HD)
    )
    hidden_pre = jnp.dot(normed, w_up, preferred_element_type=jnp.float32) + b_up.astype(
        jnp.float32
    )
    hidden = gelu(hidden_pre).astype(jnp.bfloat16)
    summands = jnp.dot(attended, w_out, preferred_element_type=jnp.float32) + jnp.dot(
        hidden, w_down, preferred_element_type=jnp.float32
    )
    mixed = lax.psum_scatter(summands, "tp", scatter_dimension=1, tiled=True)
    layer_out = (wide_in + mixed + b_out.astype(jnp.float32) + b_down.astype(jnp.float32)).astype(
        jnp.bfloat16
    )
    kept = (key_rot, value_part)
    return (
        layer_out,
        (centered, inverse_std, normed, query, kept, attended, log_total, hidden_pre, hidden),
    )


def backward_layer(incoming, saved, ids_full, params, ctx_index):
    w_qkv, b_qkv, w_out, b_out, w_up, b_up, w_down, b_down, gain, shift = params
    centered, inverse_std, normed, query, kept, attended, log_total, hidden_pre, hidden = saved
    tokens = query.shape[0]
    heads = query.shape[1]
    wide_grad = incoming.astype(jnp.float32)
    grad_rows = lax.all_gather(incoming, "tp", axis=1, tiled=True)
    grad_out_bias = jnp.sum(wide_grad, axis=0)
    grad_out = jnp.einsum("tk,te->ke", attended, grad_rows, preferred_element_type=jnp.float32)
    d_attended = jnp.einsum(
        "te,ke->tk", grad_rows, w_out, preferred_element_type=jnp.float32
    ).astype(jnp.bfloat16)
    grad_down = jnp.einsum("tf,te->fe", hidden, grad_rows, preferred_element_type=jnp.float32)
    d_pre = jnp.einsum(
        "te,fe->tf", grad_rows, w_down, preferred_element_type=jnp.float32
    ) * gelu_slope(hidden_pre)
    grad_up_bias = jnp.sum(d_pre, axis=0)
    d_hidden = d_pre.astype(jnp.bfloat16)
    grad_up = jnp.einsum("td,tf->df", normed, d_hidden, preferred_element_type=jnp.float32)
    key_all, value_all = (
        lax.all_gather(kept[0], "ctx", axis=0, tiled=True),
        lax.all_gather(kept[1], "ctx", axis=0, tiled=True),
    )
    positions, allowed = local_layout(ids_full, ctx_index, tokens)
    cosine, sine = rope_tables(positions)
    d_heads = d_attended.reshape(tokens, heads, HD)
    out_heads = attended.reshape(tokens, heads, HD)
    delta = jnp.sum(d_heads.astype(jnp.float32) * out_heads.astype(jnp.float32), axis=2)
    scores = score_block(query, key_all)
    probs = jnp.where(allowed[None], jnp.exp(scores - log_total[:, :, None]), 0.0)
    d_probs = jnp.einsum("thd,shd->hts", d_heads, value_all, preferred_element_type=jnp.float32)
    d_scores = (probs * (d_probs - delta.T[:, :, None]) * HD ** (-0.5)).astype(jnp.bfloat16)
    d_query = jnp.einsum("hts,shd->thd", d_scores, key_all, preferred_element_type=jnp.float32)
    key_terms = jnp.einsum("hts,thd->shd", d_scores, query, preferred_element_type=jnp.float32)
    value_terms = jnp.einsum(
        "hts,thd->shd", probs.astype(jnp.bfloat16), d_heads, preferred_element_type=jnp.float32
    )
    d_key, d_value = (
        lax.psum_scatter(
            key_terms.astype(jnp.bfloat16), "ctx", scatter_dimension=0, tiled=True
        ).astype(jnp.float32),
        lax.psum_scatter(
            value_terms.astype(jnp.bfloat16), "ctx", scatter_dimension=0, tiled=True
        ).astype(jnp.float32),
    )
    d_projected = jnp.stack(
        [rotate(d_query, cosine, sine, -1.0), rotate(d_key, cosine, sine, -1.0), d_value]
    ).reshape(3, tokens, heads * HD)
    grad_qkv_bias = jnp.sum(d_projected, axis=1)
    d_qkv = d_projected.astype(jnp.bfloat16)
    grad_qkv = jnp.einsum("td,cte->cde", normed, d_qkv, preferred_element_type=jnp.float32)
    normed_terms = jnp.einsum("cte,cde->td", d_qkv, w_qkv, preferred_element_type=jnp.float32)
    normed_terms = normed_terms + jnp.einsum(
        "tf,df->td", d_hidden, w_up, preferred_element_type=jnp.float32
    )
    d_normed = lax.psum_scatter(
        normed_terms.astype(jnp.bfloat16), "tp", scatter_dimension=1, tiled=True
    ).astype(jnp.float32)
    grad_gain = jnp.sum(d_normed * centered, axis=0)
    grad_shift = jnp.sum(d_normed, axis=0)
    scaled = d_normed * gain.astype(jnp.float32)
    row_terms = lax.psum((jnp.sum(scaled, axis=1), jnp.sum(scaled * centered, axis=1)), "tp")
    grad_in = wide_grad + inverse_std[:, None] * (
        scaled - row_terms[0][:, None] / D - centered * (row_terms[1][:, None] / D)
    )
    grads = (
        grad_qkv,
        grad_qkv_bias,
        grad_out,
        grad_out_bias,
        grad_up,
        grad_up_bias,
        grad_down,
        grad_out_bias,
        grad_gain,
        grad_shift,
    )
    return (grad_in.astype(jnp.bfloat16), grads)


def base_shards(
    boundary,
    doc_ids,
    qkv_weight,
    qkv_bias,
    out_weight,
    out_bias,
    fc1_weight,
    fc1_bias,
    fc2_weight,
    fc2_bias,
    norm_gain,
    norm_shift,
):
    section = lax.axis_index("section")
    ctx_index = lax.axis_index("ctx")
    micro = boundary.shape[1]
    tokens = boundary.shape[2]
    width_part = boundary.shape[3]
    params = (
        lax.all_gather(qkv_weight[0], "ctx", axis=1, tiled=True),
        lax.all_gather(qkv_bias[0], "ctx", axis=1, tiled=True),
        lax.all_gather(out_weight[0], "ctx", axis=1, tiled=True),
        lax.all_gather(out_bias[0], "ctx", axis=0, tiled=True),
        lax.all_gather(fc1_weight[0], "ctx", axis=0, tiled=True),
        lax.all_gather(fc1_bias[0], "ctx", axis=0, tiled=True),
        lax.all_gather(fc2_weight[0], "ctx", axis=1, tiled=True),
        lax.all_gather(fc2_bias[0], "ctx", axis=0, tiled=True),
        lax.all_gather(norm_gain[0], "ctx", axis=0, tiled=True),
        lax.all_gather(norm_shift[0], "ctx", axis=0, tiled=True),
    )
    inputs = boundary[0]
    ticks = jnp.arange(micro + 1, dtype=jnp.int32)

    def forward_tick(received, tick):
        index = jnp.clip(tick - section, 0, micro - 1)
        first = lax.dynamic_index_in_dim(inputs, index, 0, keepdims=False)
        layer_in = jnp.where(section == 0, first, received)
        ids_full = lax.dynamic_index_in_dim(doc_ids, index, 0, keepdims=False)
        layer_out, saved = forward_layer(layer_in, ids_full, params, ctx_index)
        passed = from_behind(layer_out, "section", 1)
        return (passed, (layer_out, saved))

    start_zero = jnp.zeros((tokens, width_part), jnp.bfloat16)
    leftover, (outs_all, saved_all) = lax.scan(forward_tick, start_zero, ticks)
    held = lax.optimization_barrier(
        (
            (
                qkv_weight[0],
                qkv_bias[0],
                out_weight[0],
                out_bias[0],
                fc1_weight[0],
                fc1_bias[0],
                fc2_weight[0],
                fc2_bias[0],
                norm_gain[0],
                norm_shift[0],
            ),
            outs_all,
        )
    )[0]
    back_params = (
        lax.all_gather(held[0], "ctx", axis=1, tiled=True),
        lax.all_gather(held[1], "ctx", axis=1, tiled=True),
        lax.all_gather(held[2], "ctx", axis=1, tiled=True),
        lax.all_gather(held[3], "ctx", axis=0, tiled=True),
        lax.all_gather(held[4], "ctx", axis=0, tiled=True),
        lax.all_gather(held[5], "ctx", axis=0, tiled=True),
        lax.all_gather(held[6], "ctx", axis=1, tiled=True),
        lax.all_gather(held[7], "ctx", axis=0, tiled=True),
        lax.all_gather(held[8], "ctx", axis=0, tiled=True),
        lax.all_gather(held[9], "ctx", axis=0, tiled=True),
    )
    zero_grads = tuple((jnp.zeros(weight.shape, jnp.float32) for weight in params))

    def backward_tick(carry, tick):
        received, totals = carry
        raw_index = tick - (1 - section)
        valid = (raw_index >= 0) & (raw_index < micro)
        index = jnp.clip(raw_index, 0, micro - 1)
        cotangent = lax.dynamic_index_in_dim(inputs, index, 0, keepdims=False)
        incoming = jnp.where(section == 1, cotangent, received)
        incoming = jnp.where(valid, incoming, jnp.zeros_like(incoming))
        position_slot = index + section
        saved = jax.tree.map(
            lambda stacked: lax.dynamic_index_in_dim(stacked, position_slot, 0, keepdims=False),
            saved_all,
        )
        ids_full = lax.dynamic_index_in_dim(doc_ids, index, 0, keepdims=False)
        grad_in, terms = backward_layer(incoming, saved, ids_full, back_params, ctx_index)
        totals = tuple((total + term for total, term in zip(totals, terms)))
        passed = from_behind(grad_in, "section", -1)
        return ((passed, totals), grad_in)

    (leftover_grad, totals), grads_all = lax.scan(backward_tick, (start_zero, zero_grads), ticks)
    acts = lax.dynamic_slice_in_dim(outs_all, section, micro, 0)[None]
    input_grads = lax.dynamic_slice_in_dim(grads_all, 1 - section, micro, 0)[None]
    shares = (
        lax.psum_scatter(
            totals[0].astype(jnp.bfloat16), "ctx", scatter_dimension=1, tiled=True
        ).astype(jnp.float32),
        lax.psum_scatter(
            totals[1].astype(jnp.bfloat16), "ctx", scatter_dimension=1, tiled=True
        ).astype(jnp.float32),
        lax.psum_scatter(
            totals[2].astype(jnp.bfloat16), "ctx", scatter_dimension=1, tiled=True
        ).astype(jnp.float32),
        lax.psum_scatter(
            totals[3].astype(jnp.bfloat16), "ctx", scatter_dimension=0, tiled=True
        ).astype(jnp.float32),
        lax.psum_scatter(
            totals[4].astype(jnp.bfloat16), "ctx", scatter_dimension=0, tiled=True
        ).astype(jnp.float32),
        lax.psum_scatter(
            totals[5].astype(jnp.bfloat16), "ctx", scatter_dimension=0, tiled=True
        ).astype(jnp.float32),
        lax.psum_scatter(
            totals[6].astype(jnp.bfloat16), "ctx", scatter_dimension=1, tiled=True
        ).astype(jnp.float32),
        lax.psum_scatter(
            totals[7].astype(jnp.bfloat16), "ctx", scatter_dimension=0, tiled=True
        ).astype(jnp.float32),
        lax.psum_scatter(
            totals[8].astype(jnp.bfloat16), "ctx", scatter_dimension=0, tiled=True
        ).astype(jnp.float32),
        lax.psum_scatter(
            totals[9].astype(jnp.bfloat16), "ctx", scatter_dimension=0, tiled=True
        ).astype(jnp.float32),
    )
    return (
        acts,
        input_grads,
        shares[0][None],
        shares[1][None],
        shares[2][None],
        shares[3][None],
        shares[4][None],
        shares[5][None],
        shares[6][None],
        shares[7][None],
        shares[8][None],
        shares[9][None],
    )


def solution(mesh):
    specs = {
        "token": P("section", None, "ctx", "tp"),
        "rows": P("section", "tp", "ctx"),
        "columns": P("section", "ctx", "tp"),
        "vector": P("section", ("tp", "ctx")),
        "vectors": P("section", None, ("tp", "ctx")),
    }
    weights = ("token", "vectors", "rows", "vector", "columns", "vector", "rows", "vector", "vector", "vector")
    placed = tuple(specs[name] for name in weights)
    heads = D // HD
    whole_heads = heads % (mesh.shape["tp"] * mesh.shape["ctx"]) == 0
    return jax.shard_map(
        shards if whole_heads and mesh.shape["section"] == 2 else base_shards,
        mesh=mesh,
        in_specs=(specs["token"], P(), *placed),
        out_specs=(specs["token"], specs["token"], *placed),
        check_vma=False,
    )
```

```python
import functools
import itertools

import jax
import jax.numpy as jnp
from jax import lax
from jax.experimental import pallas as pl
from jax.experimental.pallas import tpu as pltpu
from jax.sharding import PartitionSpec as P

D = 2048
HD = 64
ROT = 32
EPS = 1e-05
GELU_C = 0.7978845608028654
GELU_K = 0.044715
BF16 = jnp.bfloat16
F32 = jnp.float32


def rope_tables(positions):
    half = ROT // 2
    freq = 10000.0 ** (-(jnp.arange(half).astype(F32) * 2.0 / ROT))
    angle = positions.astype(F32)[:, None] * freq[None, :]
    return (jnp.cos(angle), jnp.sin(angle))


def rotate(field, cosine, sine, sign):
    half = ROT // 2
    first = field[..., :half]
    second = field[..., half:ROT]
    cosine = cosine[:, None, :]
    sine = sine[:, None, :] * sign
    return jnp.concatenate(
        [first * cosine - second * sine, second * cosine + first * sine, field[..., ROT:]], axis=-1
    )


def doc_layout(ids):
    length = ids.shape[0]
    start = jnp.sum((ids[None, :] < ids[:, None]).astype(jnp.int32), axis=1)
    at = jnp.arange(length, dtype=jnp.int32)
    allowed = (at[None, :] <= at[:, None]) & (ids[None, :] == ids[:, None])
    cosine, sine = rope_tables(at - start)
    return (allowed, cosine, sine)


MESH = pl.DeviceIdType.MESH
FWD, BWD, LAST, START = 0, 1, 2, 3


class Wire:
    def __init__(self, send_sems, recv_sems):
        self.send_sems, self.recv_sems = send_sems, recv_sems
        self.copies = []
        self.section = lax.axis_index("section")
        self.c = lax.axis_index("ctx")
        self.t = lax.axis_index("tp")
        self.y = self.t // 2
        self.k = self.t % 2
        self.c_up = (self.c + 1) % 4
        self.c_far = (self.c + 2) % 4
        self.c_down = (self.c + 3) % 4
        self.t_y = (self.t + 2) % 4
        self.t_core = self.t + 1 - 2 * self.k
        self.up = {"ctx": self.c_up}
        self.down = {"ctx": self.c_down}
        self.beside = {"tp": self.t_y}
        self.core = {"tp": self.t_core}
        self.across = {"section": 1 - self.section}
        self.others = [(2, self.c_far), (1, self.c_up), (3, self.c_down)]

    def greet(self, targets):
        barrier = pltpu.get_barrier_semaphore()
        for target in targets:
            pl.semaphore_signal(barrier, inc=1, device_id=target, device_id_type=MESH)
        pl.semaphore_wait(barrier, len(targets))

    def send(self, source, target, device):
        index = len(self.copies)
        copy = pltpu.make_async_remote_copy(
            src_ref=source,
            dst_ref=target,
            send_sem=self.send_sems.at[index],
            recv_sem=self.recv_sems.at[index],
            device_id=device,
            device_id_type=MESH,
        )
        copy.start()
        self.copies.append(copy)
        return copy

    def send_one_of(self, first, source, other_source, target, device):
        index = len(self.copies)
        copies = [
            pltpu.make_async_remote_copy(
                src_ref=ref,
                dst_ref=target,
                send_sem=self.send_sems.at[index],
                recv_sem=self.recv_sems.at[index],
                device_id=device,
                device_id_type=MESH,
            )
            for ref in (source, other_source)
        ]
        pl.when(first)(copies[0].start)
        pl.when(jnp.logical_not(first))(copies[1].start)
        self.copies.append(copies[0])
        return copies[0]

    def drain(self):
        for copy in self.copies:
            copy.wait_send()


class Gather:
    def __init__(self, wire, full, rows, part):
        self.w, self.full, self.rows, self.part = wire, full, rows, part
        self.far, self.beside, self.core = {}, {}, []

    def region(self, c, t, group):
        size = self.rows // 2
        return self.full.at[
            pl.ds(pl.multiple_of(c * self.rows + group * size, 16), size),
            pl.ds(pl.multiple_of(t * self.part, 128), self.part),
        ]

    def pass_on(self, device, c, t, group):
        spot = self.region(c, t, group)
        return self.w.send(spot, spot, device)

    def begin(self, group):
        w = self.w
        for step, place in w.others:
            self.far[group, step] = self.pass_on({"ctx": place}, w.c, w.t, group)
        self.beside[group, 0] = self.pass_on(w.beside, w.c, w.t, group)
        self.core.append(self.pass_on(w.core, w.c, w.t, group))

    def finish(self):
        w = self.w
        steps = [(step, group) for group in (0, 1) for step in (1, 3, 2)]
        for step, group in steps:
            source = (w.c + 4 - step) % 4
            self.far[group, step].wait_recv()
            self.beside[group, step] = self.pass_on(w.beside, source, w.t, group)
            self.core.append(self.pass_on(w.core, source, w.t, group))
        for step, group in [(0, 0), (0, 1)] + steps:
            self.beside[group, step].wait_recv()
            self.core.append(self.pass_on(w.core, (w.c + 4 - step) % 4, w.t_y, group))
        for copy in self.core:
            copy.wait_recv()


def scatter_scratch(rows, part):
    return [
        pltpu.VMEM((2, 4 * rows, part), BF16),
        pltpu.VMEM((2, 4 * rows, part), BF16),
        pltpu.VMEM((4 * rows, part), BF16),
        pltpu.VMEM((3, rows, part), BF16),
    ]


class Scatter:
    def __init__(self, wire, partial, scratch, rows, part):
        self.w, self.partial, self.rows, self.part = wire, partial, rows, part
        self.theirs, self.chip, self.from_y, self.from_far = scratch
        w = wire
        self.places = [(2, w.c_far), (1, w.c_up), (3, w.c_down), (0, w.c)]
        self.order = [
            (group, c, y)
            for group in (0, 1)
            for y in (1 - w.y, w.y)
            for _, c in self.places
        ]
        self.far = {}

    def span(self, group, c):
        size = self.rows // 2
        return pl.ds(pl.multiple_of(c * self.rows + group * size, 16), size)

    def begin(self):
        w = self.w
        self.cores = []
        for group, c, y in self.order:
            columns = pl.ds(pl.multiple_of((2 * y + 1 - w.k) * self.part, 128), self.part)
            self.cores.append(
                w.send(
                    self.partial.at[self.span(group, c), columns],
                    self.theirs.at[y, self.span(group, c)],
                    w.core,
                )
            )

    def take(self, index):
        group, c, y = self.order[index]
        self.cores[index].wait_recv()
        rows = self.span(group, c)
        columns = pl.ds(pl.multiple_of((2 * y + self.w.k) * self.part, 128), self.part)
        return self.partial[rows, columns].astype(F32) + self.theirs[y, rows].astype(F32)

    def run(self):
        for _ in self.steps():
            pass

    def steps(self):
        w = self.w
        half = self.rows // 2
        beside = {}
        for group in (0, 1):
            for slot, (_, c) in enumerate(self.places):
                rows = self.span(group, c)
                self.chip[1 - w.y, rows] = self.take(8 * group + slot).astype(BF16)
                beside[group, slot] = w.send(
                    self.chip.at[1 - w.y, rows], self.from_y.at[rows], w.beside
                )
                yield
        for group in (0, 1):
            for slot, (step, c) in enumerate(self.places):
                rows = self.span(group, c)
                value = self.take(8 * group + 4 + slot)
                beside[group, slot].wait_recv()
                self.chip[w.y, rows] = (value + self.from_y[rows].astype(F32)).astype(BF16)
                if step:
                    self.far[group, step] = w.send(
                        self.chip.at[w.y, rows],
                        self.from_far.at[step - 1, pl.ds(group * half, half)],
                        {"ctx": c},
                    )
                yield

    def total(self, group):
        half = self.rows // 2
        value = self.chip[self.w.y, self.span(group, self.w.c)].astype(F32)
        for step in (1, 3, 2):
            self.far[group, step].wait_recv()
            value += self.from_far[step - 1, pl.ds(group * half, half)].astype(F32)
        return value


def neighbours(w):
    return [{"ctx": place} for _, place in w.others] + [w.beside, w.core]


def next_layer_kernel(rows, part, partial, block, bias, act, full, *rest):
    *scratch, send_sems, recv_sems = rest
    w = Wire(send_sems, recv_sems)
    w.greet(neighbours(w))
    scatter = Scatter(w, partial, scratch, rows, part)
    scatter.begin()
    scatter.run()
    gather = Gather(w, full, rows, part)
    half = rows // 2
    for group in (0, 1):
        own = slice(group * half, (group + 1) * half)
        value = (block[own].astype(F32) + scatter.total(group) + bias[...]).astype(BF16)
        act[own] = value
        gather.region(w.c, w.t, group)[...] = value
        gather.begin(group)
    gather.finish()
    w.drain()


def next_layer(partial, block, bias):
    rows, part = block.shape
    vmem = pl.BlockSpec(memory_space=pltpu.VMEM)
    return pl.pallas_call(
        functools.partial(next_layer_kernel, rows, part),
        out_shape=(
            jax.ShapeDtypeStruct((rows, part), BF16),
            jax.ShapeDtypeStruct((4 * rows, 4 * part), BF16),
        ),
        in_specs=[vmem] * 3,
        out_specs=(vmem, vmem),
        scratch_shapes=scatter_scratch(rows, part)
        + [pltpu.SemaphoreType.DMA((80,)), pltpu.SemaphoreType.DMA((80,))],
        compiler_params=pltpu.CompilerParams(
            collective_id=FWD, has_side_effects=True, vmem_limit_bytes=40 << 20
        ),
        name="next_layer",
    )(partial, block, bias)


def diagonal(w):
    return {"tp": (w.t_core + 2) % 4}


def back_scratch(rows, part):
    return [
        pltpu.VMEM((rows, part), F32),
        pltpu.VMEM((2, 8, 128), F32),
        pltpu.VMEM((2, 3, 8, 128), F32),
    ]


def norm_back(w, scatter, blocks, scratch, rows, part, grad, sums, done):
    g_block, x_block, mean, inverse_std, gain = blocks
    d_normed, row_out, row_in = scratch
    half = rows // 2
    width = 4 * part
    lane = lax.broadcasted_iota(jnp.int32, (half, 128), 1)
    sent = []
    gain_sum = jnp.zeros((1, part), F32)
    shift_sum = jnp.zeros((1, part), F32)
    for group in (0, 1):
        own = slice(group * half, (group + 1) * half)
        value = scatter.total(group)
        d_normed[own] = value
        centered = (x_block[own].astype(F32) - mean[own]) * inverse_std[own]
        weighted = value * centered
        gain_sum += jnp.sum(weighted, axis=0, keepdims=True)
        shift_sum += jnp.sum(value, axis=0, keepdims=True)
        first = jnp.sum(value * gain[...], axis=1, keepdims=True)
        second = jnp.sum(weighted * gain[...], axis=1, keepdims=True)
        packed = jnp.where(lane == 0, first, jnp.where(lane == 1, second, 0.0))
        row_out[group] = packed.T[:8]
        sent.append(
            [
                w.send(row_out.at[group], row_in.at[group, slot], peer)
                for slot, peer in enumerate((w.beside, w.core, diagonal(w)))
            ]
        )
    sums[...] = jnp.concatenate(
        [gain_sum, shift_sum, jnp.zeros((6, part), F32)], axis=0
    )
    for group in (0, 1):
        own = slice(group * half, (group + 1) * half)
        for copy in sent[group]:
            copy.wait_recv()
        rows_sum = row_out[group] + row_in[group, 0] + row_in[group, 1] + row_in[group, 2]
        columns = jnp.concatenate([rows_sum, jnp.zeros((half - 8, 128), F32)], axis=0).T
        centered = (x_block[own].astype(F32) - mean[own]) * inverse_std[own]
        scaled = d_normed[own] * gain[...]
        value = g_block[own].astype(F32) + inverse_std[own] * (
            scaled - columns[:, 0:1] / width - centered * (columns[:, 1:2] / width)
        )
        grad[own] = value.astype(BF16)
        done(group)


def previous_layer_kernel(
    rows, part, partial, g_block, x_block, mean, inverse_std, gain, grad, full, sums, *rest
):
    *scratch, send_sems, recv_sems = rest
    w = Wire(send_sems, recv_sems)
    w.greet(neighbours(w) + [diagonal(w)])
    scatter = Scatter(w, partial, scratch[:4], rows, part)
    scatter.begin()
    scatter.run()
    gather = Gather(w, full, rows, part)
    half = rows // 2

    def done(group):
        gather.region(w.c, w.t, group)[...] = grad[group * half : (group + 1) * half]
        gather.begin(group)

    norm_back(
        w, scatter, (g_block, x_block, mean, inverse_std, gain), scratch[4:], rows, part, grad, sums, done
    )
    gather.finish()
    w.drain()


def previous_layer(partial, g_block, x_block, mean, inverse_std, gain):
    rows, part = g_block.shape
    vmem = pl.BlockSpec(memory_space=pltpu.VMEM)
    return pl.pallas_call(
        functools.partial(previous_layer_kernel, rows, part),
        out_shape=(
            jax.ShapeDtypeStruct((rows, part), BF16),
            jax.ShapeDtypeStruct((4 * rows, 4 * part), BF16),
            jax.ShapeDtypeStruct((8, part), F32),
        ),
        in_specs=[vmem] * 6,
        out_specs=(vmem,) * 3,
        scratch_shapes=scatter_scratch(rows, part)
        + back_scratch(rows, part)
        + [pltpu.SemaphoreType.DMA((90,)), pltpu.SemaphoreType.DMA((90,))],
        compiler_params=pltpu.CompilerParams(
            collective_id=BWD, has_side_effects=True, vmem_limit_bytes=44 << 20
        ),
        name="previous_layer",
    )(partial, g_block, x_block, mean, inverse_std, gain)


def whole(size, start=0):
    return pl.ds(start, size)


class Turn:
    def __init__(self, d_part, e_part, f_part):
        self.d, self.e, self.f = d_part, e_part, f_part

    def rows(self, name):
        return {"qkv": self.d, "out": self.e, "up": self.d, "down": self.f}[name]

    def inner(self, name, half):
        size = self.rows(name)
        return (0, size) if half is None else (half * size // 2, size // 2)

    def shard(self, name, ref, c, half=None):
        start, size = self.inner(name, half)
        if name == "qkv":
            return ref.at[:, pl.ds(start, size), pl.ds(pl.multiple_of(c * self.e, 128), self.e)]
        if name == "up":
            return ref.at[pl.ds(start, size), pl.ds(pl.multiple_of(c * self.f, 128), self.f)]
        stride = self.e if name == "out" else self.f
        return ref.at[pl.ds(pl.multiple_of(c * stride + start, 16), size)]

    def turned(self, name, ref, c, half=None):
        start, size = self.inner(name, half)
        if name == "qkv":
            return ref.at[:, pl.ds(pl.multiple_of(c * self.d + start, 16), size)]
        if name == "up":
            return ref.at[pl.ds(pl.multiple_of(c * self.d + start, 16), size)]
        return ref.at[pl.ds(start, size), pl.ds(pl.multiple_of(c * self.d, 128), self.d)]

    def piece_shape(self, name, halved=False):
        size = self.rows(name) // (2 if halved else 1)
        return {
            "qkv": (3, size, self.e),
            "out": (size, self.d),
            "up": (size, self.f),
            "down": (size, self.d),
        }[name]

    def turned_shape(self, name):
        return {
            "qkv": (3, 4 * self.d, self.e),
            "out": (self.e, 4 * self.d),
            "up": (4 * self.d, self.f),
            "down": (self.f, 4 * self.d),
        }[name]


NAMES = ("qkv", "out", "up", "down")


def everyone(w):
    return [
        {"section": (w.section + ds) % 2, "ctx": (w.c + dc) % 4, "tp": (w.t + dt) % 4}
        for ds in range(2)
        for dc in range(4)
        for dt in range(4)
        if (ds, dc, dt) != (0, 0, 0)
    ]


def begin_kernel(turn, rows, part, own, vector, *rest):
    shards = dict(zip(NAMES, rest[:4]))
    turned = dict(zip(NAMES, rest[4:8]))
    x_full, g_full, x_block, g_block, vectors = rest[8:13]
    bounce = dict(zip(NAMES, rest[13:17]))
    other, local_sems, send_sems, recv_sems = rest[17:]
    w = Wire(send_sems, recv_sems)
    s = w.section
    peers = everyone(w)
    w.greet(peers)
    mine = {name: turned[name].at[s] for name in NAMES}
    swap = w.send(own.at[1 - s], other, w.across)
    vectors[s, w.c, w.t] = vector[...]
    told = [w.send(vector, vectors.at[s, w.c, w.t], peer) for peer in peers]
    local, far, across = {}, {}, []
    for i, name in enumerate(NAMES):
        own_piece = turn.shard(name, shards[name], w.c)
        across.append(w.send(own_piece, turn.turned(name, mine[name], w.c), w.across))
        local[name] = pltpu.make_async_copy(own_piece, bounce[name], local_sems.at[i])
        local[name].start()
        for step, place in w.others:
            far[name, step] = w.send(
                turn.shard(name, shards[name], place),
                turn.turned(name, mine[name], w.c),
                {"ctx": place},
            )
    swap.wait_recv()
    mine_block = own[s]
    x_block[...] = jnp.where(s == 0, mine_block, other[...])
    g_block[...] = jnp.where(s == 0, other[...], mine_block)
    half = rows // 2
    gathers = [Gather(w, x_full, rows, part), Gather(w, g_full, rows, part)]
    for gather, block in zip(gathers, (x_block, g_block)):
        for group in (0, 1):
            gather.region(w.c, w.t, group)[...] = block[group * half : (group + 1) * half]
            gather.begin(group)
    puts = []
    for i, name in enumerate(NAMES):
        local[name].wait()
        puts.append(
            pltpu.make_async_copy(bounce[name], turn.turned(name, mine[name], w.c), local_sems.at[4 + i])
        )
        puts[-1].start()
    for name in NAMES:
        for step in (1, 3, 2):
            far[name, step].wait_recv()
            spot = turn.turned(name, mine[name], (w.c + 4 - step) % 4)
            across.append(w.send(spot, spot, w.across))
    for gather in gathers:
        gather.finish()
    for copy in told + across:
        copy.wait_recv()
    for put in puts:
        put.wait()
    w.drain()


def begin(own, vector, shards):
    _, rows, part = own.shape
    turn = Turn(shards["qkv"].shape[1], shards["qkv"].shape[2] // 4, shards["up"].shape[1] // 4)
    vmem = pl.BlockSpec(memory_space=pltpu.VMEM)
    hbm = pl.BlockSpec(memory_space=pl.ANY)
    shape = jax.ShapeDtypeStruct
    full = shape((4 * rows, 4 * part), BF16)
    block = shape((rows, part), BF16)
    return pl.pallas_call(
        functools.partial(begin_kernel, turn, rows, part),
        out_shape=tuple(shape((2,) + turn.turned_shape(name), BF16) for name in NAMES)
        + (full, full, block, block, shape((2, 4, 4) + vector.shape, F32)),
        in_specs=[vmem, vmem] + [hbm] * 4,
        out_specs=(hbm,) * 4 + (vmem,) * 5,
        scratch_shapes=[pltpu.VMEM(turn.piece_shape(name), BF16) for name in NAMES]
        + [
            pltpu.VMEM((rows, part), BF16),
            pltpu.SemaphoreType.DMA((8,)),
            pltpu.SemaphoreType.DMA((200,)),
            pltpu.SemaphoreType.DMA((200,)),
        ],
        compiler_params=pltpu.CompilerParams(
            collective_id=START, has_side_effects=True, vmem_limit_bytes=40 << 20
        ),
        name="begin",
    )(own, vector, *(shards[name] for name in NAMES))


SENT = ("down", "out", "up", "qkv")


def end_kernel(turn, rows, part, *refs):
    grads0, grads1 = dict(zip(NAMES, refs[:4])), dict(zip(NAMES, refs[4:8]))
    partial_x, block, bias = refs[8:11]
    partial_g, *blocks = refs[11:17]
    small, sums1 = refs[17:19]
    outs = dict(zip(NAMES, refs[19:23]))
    act, grad, small_sum, norm_sum = refs[23:27]
    rest = refs[27:]
    kept, arrived = dict(zip(NAMES, rest[:4])), dict(zip(NAMES, rest[4:8]))
    landed = dict(zip(NAMES, rest[8:12]))
    scratch_x, scratch_g, scratch_n = rest[12:16], rest[16:20], rest[20:23]
    small_in, sums0, norm_out, norm_in = rest[23:27]
    local_sems, send_sems, recv_sems = rest[27:]
    w = Wire(send_sems, recv_sems)
    s = w.section
    half = rows // 2
    moves = [(ds, dc) for ds in (0, 1) for dc in range(4) if (ds, dc) != (0, 0)]

    def away(ds, dc):
        return {"section": (s + ds) % 2, "ctx": (w.c + dc) % 4}

    w.greet([away(*move) for move in moves] + [w.beside, w.core, diagonal(w)])
    places = [(2, w.c_far), (1, w.c_up), (3, w.c_down), (0, w.c)]
    small_copy = w.send(small.at[1 - s], small_in, w.across)
    across = {}
    for i, name in enumerate(SENT):
        for layer, grads in ((0, grads0), (1, grads1)):
            keep = pltpu.make_async_copy(grads[name], kept[name], local_sems.at[i])
            pl.when(s == layer)(keep.start)
        for step, c in places:
            target = turn.turned(name, arrived[name], c)
            across[name, step] = w.send_one_of(
                s == 0,
                turn.turned(name, grads1[name], c),
                turn.turned(name, grads0[name], c),
                target,
                w.across,
            )
    scatter_x = Scatter(w, partial_x, scratch_x, rows, part)
    scatter_g = Scatter(w, partial_g, scratch_g, rows, part)
    scatter_x.begin()
    scatter_g.begin()
    work = itertools.chain(scatter_x.steps(), scatter_g.steps())
    home = {}
    for i, name in enumerate(SENT):
        pltpu.make_async_copy(grads0[name], kept[name], local_sems.at[i]).wait()
        for step, c in places:
            across[name, step].wait_recv()
            mine = turn.turned(name, kept[name], c)
            theirs = turn.turned(name, arrived[name], c)
            total = mine[...].astype(F32) + theirs[...].astype(F32)
            if step:
                theirs[...] = total.astype(BF16)
                home[name, step] = w.send(theirs, landed[name].at[step - 1], {"ctx": c})
            else:
                turn.shard(name, outs[name], w.c)[...] = total
            for _ in range(5):
                next(work, None)
    for _ in work:
        pass
    for group in (0, 1):
        own = slice(group * half, (group + 1) * half)
        value = block[own].astype(F32) + scatter_x.total(group) + bias[...]
        act[own] = value.astype(BF16)
    norm_back(w, scatter_g, blocks, scratch_n, rows, part, grad, sums0, lambda group: None)
    for layer, sums in ((0, sums0), (1, sums1)):
        for c in range(4):
            norm_out[layer, c] = sums[:, c * 128 : (c + 1) * 128]
    told = []
    for slot, (ds, dc) in enumerate(moves):
        told.append(
            w.send(
                norm_out.at[(s + ds) % 2, (w.c + dc) % 4], norm_in.at[slot], away(ds, dc)
            )
        )
    small_copy.wait_recv()
    small_sum[...] = small[s] + small_in[...]
    for name in SENT:
        for step in (1, 3, 2):
            home[name, step].wait_recv()
            spot = turn.shard(name, outs[name], (w.c + 4 - step) % 4)
            spot[...] = landed[name][step - 1].astype(F32)
    total = norm_out[s, w.c]
    for slot, copy in enumerate(told):
        copy.wait_recv()
        total += norm_in[slot]
    norm_sum[...] = total
    w.drain()


def end(grads0, grads1, partial_x, block, bias, partial_g, blocks, small, sums1):
    rows, part = block.shape
    d_part = grads0["qkv"].shape[1] // 4
    turn = Turn(d_part, grads0["qkv"].shape[2], grads0["up"].shape[1])
    shape = jax.ShapeDtypeStruct
    vmem = pl.BlockSpec(memory_space=pltpu.VMEM)
    hbm = pl.BlockSpec(memory_space=pl.ANY)
    e, f = 4 * turn.e, 4 * turn.f
    homes = {
        "qkv": (3, d_part, e),
        "out": (e, d_part),
        "up": (d_part, f),
        "down": (f, d_part),
    }
    return pl.pallas_call(
        functools.partial(end_kernel, turn, rows, part),
        out_shape=tuple(shape(homes[name], F32) for name in NAMES)
        + (
            shape((rows, part), BF16),
            shape((rows, part), BF16),
            shape(small.shape[1:], F32),
            shape((8, 128), F32),
        ),
        in_specs=[hbm] * 8 + [vmem] * 11,
        out_specs=(vmem,) * 8,
        scratch_shapes=[pltpu.VMEM(turn.turned_shape(name), BF16) for name in NAMES] * 2
        + [pltpu.VMEM((3,) + turn.piece_shape(name), BF16) for name in NAMES]
        + scatter_scratch(rows, part) * 2
        + back_scratch(rows, part)
        + [
            pltpu.VMEM(small.shape[1:], F32),
            pltpu.VMEM((8, part), F32),
            pltpu.VMEM((2, 4, 8, 128), F32),
            pltpu.VMEM((7, 8, 128), F32),
            pltpu.SemaphoreType.DMA((4,)),
            pltpu.SemaphoreType.DMA((120,)),
            pltpu.SemaphoreType.DMA((120,)),
        ],
        compiler_params=pltpu.CompilerParams(
            collective_id=LAST, has_side_effects=True, vmem_limit_bytes=63 << 20
        ),
        name="end",
    )(
        *(grads0[name] for name in NAMES),
        *(grads1[name] for name in NAMES),
        partial_x,
        block,
        bias,
        partial_g,
        *blocks,
        small,
        sums1,
    )


def forward(x_full, layout, params):
    w_qkv, b_qkv, w_out, w_up, b_up, w_down, gain, shift = params
    allowed, cosine, sine = layout
    tokens = x_full.shape[0]
    heads = w_qkv.shape[2] // HD
    wide = x_full.astype(F32)
    mean = jnp.mean(wide, axis=1, keepdims=True)
    variance = jnp.mean(wide * wide, axis=1, keepdims=True) - mean * mean
    inverse_std = lax.rsqrt(variance + EPS)
    normed = (
        (wide - mean) * inverse_std * gain.astype(F32)[None] + shift.astype(F32)[None]
    ).astype(BF16)
    projected = (
        jnp.einsum("td,cde->cte", normed, w_qkv, preferred_element_type=F32)
        + b_qkv.astype(F32)[:, None, :]
    )
    query = rotate(projected[0].reshape(tokens, heads, HD), cosine, sine, 1.0).astype(BF16)
    key = rotate(projected[1].reshape(tokens, heads, HD), cosine, sine, 1.0).astype(BF16)
    value = projected[2].reshape(tokens, heads, HD).astype(BF16)
    scores = jnp.einsum("thd,shd->hts", query, key, preferred_element_type=F32) * HD ** (-0.5)
    totals = jnp.sum(jnp.where(allowed[None], jnp.exp(scores), 0.0), axis=2)
    log_total = jnp.log(totals)
    probs = jnp.where(allowed[None], jnp.exp(scores - log_total[:, :, None]), 0.0).astype(BF16)
    attended = (
        jnp.einsum("hts,shd->thd", probs, value, preferred_element_type=F32)
        .astype(BF16)
        .reshape(tokens, heads * HD)
    )
    hidden_pre = jnp.dot(normed, w_up, preferred_element_type=F32) + b_up.astype(F32)
    inner = jnp.tanh(GELU_C * (hidden_pre + GELU_K * hidden_pre * hidden_pre * hidden_pre))
    hidden = (0.5 * hidden_pre * (1.0 + inner)).astype(BF16)
    partial = jnp.dot(attended, w_out, preferred_element_type=F32) + jnp.dot(
        hidden, w_down, preferred_element_type=F32
    )
    saved = (mean, inverse_std, normed, query, key, value, attended, log_total, hidden_pre, hidden)
    return (partial.astype(BF16), saved)


def backward(g_full, saved, layout, params):
    w_qkv, b_qkv, w_out, w_up, b_up, w_down, gain, shift = params
    mean, inverse_std, normed, query, key, value, attended, log_total, hidden_pre, hidden = saved
    allowed, cosine, sine = layout
    tokens, heads = query.shape[:2]
    grad_out = jnp.einsum("tk,te->ke", attended, g_full, preferred_element_type=F32)
    d_attended = jnp.einsum("te,ke->tk", g_full, w_out, preferred_element_type=F32).astype(BF16)
    grad_down = jnp.einsum("tf,te->fe", hidden, g_full, preferred_element_type=F32)
    inner = jnp.tanh(GELU_C * (hidden_pre + GELU_K * hidden_pre * hidden_pre * hidden_pre))
    slope = 0.5 * (1.0 + inner) + 0.5 * hidden_pre * (1.0 - inner * inner) * GELU_C * (
        1.0 + 3.0 * GELU_K * hidden_pre * hidden_pre
    )
    d_pre = jnp.einsum("te,fe->tf", g_full, w_down, preferred_element_type=F32) * slope
    grad_up_bias = jnp.sum(d_pre, axis=0)
    d_hidden = d_pre.astype(BF16)
    grad_up = jnp.einsum("td,tf->df", normed, d_hidden, preferred_element_type=F32)
    d_heads = d_attended.reshape(tokens, heads, HD)
    out_heads = attended.reshape(tokens, heads, HD)
    delta = jnp.sum(d_heads.astype(F32) * out_heads.astype(F32), axis=2)
    scores = jnp.einsum("thd,shd->hts", query, key, preferred_element_type=F32) * HD ** (-0.5)
    probs = jnp.where(allowed[None], jnp.exp(scores - log_total[:, :, None]), 0.0)
    d_probs = jnp.einsum("thd,shd->hts", d_heads, value, preferred_element_type=F32)
    d_scores = (probs * (d_probs - delta.T[:, :, None]) * HD ** (-0.5)).astype(BF16)
    d_query = jnp.einsum("hts,shd->thd", d_scores, key, preferred_element_type=F32)
    d_key = jnp.einsum("hts,thd->shd", d_scores, query, preferred_element_type=F32)
    d_value = jnp.einsum("hts,thd->shd", probs.astype(BF16), d_heads, preferred_element_type=F32)
    d_projected = jnp.stack(
        [rotate(d_query, cosine, sine, -1.0), rotate(d_key, cosine, sine, -1.0), d_value]
    ).reshape(3, tokens, heads * HD)
    grad_qkv_bias = jnp.sum(d_projected, axis=1)
    d_qkv = d_projected.astype(BF16)
    grad_qkv = jnp.einsum("td,cte->cde", normed, d_qkv, preferred_element_type=F32)
    partial = jnp.einsum("cte,cde->td", d_qkv, w_qkv, preferred_element_type=F32) + jnp.einsum(
        "tf,df->td", d_hidden, w_up, preferred_element_type=F32
    )
    grads = {
        "qkv": grad_qkv.astype(BF16),
        "out": grad_out.astype(BF16),
        "up": grad_up.astype(BF16),
        "down": grad_down.astype(BF16),
    }
    return (partial.astype(BF16), grads, (grad_qkv_bias, grad_up_bias))


def shards(
    boundary,
    doc_ids,
    qkv_weight,
    qkv_bias,
    out_weight,
    out_bias,
    fc1_weight,
    fc1_bias,
    fc2_weight,
    fc2_bias,
    norm_gain,
    norm_shift,
):
    section = lax.axis_index("section")
    ctx = lax.axis_index("ctx")
    tp = lax.axis_index("tp")
    rows, part = boundary.shape[2:]
    slab = out_bias.shape[1]
    layout = doc_layout(lax.dynamic_index_in_dim(doc_ids, section, 0, keepdims=False))
    n_up = fc1_bias.shape[1] // slab
    vector = jnp.concatenate(
        [
            (out_bias.astype(F32) + fc2_bias.astype(F32)),
            norm_gain.astype(F32),
            norm_shift.astype(F32),
            qkv_bias[0].astype(F32),
            fc1_bias.astype(F32).reshape(n_up, slab),
        ]
    )
    vector = jnp.pad(vector, ((0, 16 - vector.shape[0]), (0, 0)))
    shard_of = {"qkv": qkv_weight[0], "out": out_weight[0], "up": fc1_weight[0], "down": fc2_weight[0]}
    *turned, x_full, g_full, x_block, g_block, vectors = begin(boundary[0], vector, shard_of)
    turned = dict(zip(NAMES, turned))
    wide = vectors.transpose(0, 3, 2, 1, 4).reshape(2, 16, -1)
    local = lax.dynamic_index_in_dim(
        lax.dynamic_index_in_dim(vectors, ctx, 1, keepdims=False), tp, 1, keepdims=False
    )
    params = [
        (
            turned["qkv"][layer],
            local[layer, 3:6],
            turned["out"][layer],
            turned["up"][layer],
            local[layer, 6 : 6 + n_up].reshape(-1),
            turned["down"][layer],
            wide[layer, 1],
            wide[layer, 2],
        )
        for layer in (0, 1)
    ]
    own = lax.dynamic_slice_in_dim(wide, tp * part, part, axis=2)
    bias = own[:, 0:1]
    gain = own[:, 1:2]

    def norm_rows(saved):
        return tuple(lax.dynamic_slice_in_dim(array, ctx * rows, rows) for array in saved[:2])

    partial, saved0 = forward(x_full, layout, params[0])
    act0, x1_full = next_layer(partial, x_block, bias[0])
    partial_x, saved1 = forward(x1_full, layout, params[1])
    partial, grads1, small1 = backward(g_full, saved1, layout, params[1])
    grad1, g1_full, sums1 = previous_layer(
        partial, g_block, act0, *norm_rows(saved1), gain[1]
    )
    partial_g, grads0, small0 = backward(g1_full, saved0, layout, params[0])

    def column_sum(full):
        start = tp * part + ctx * slab
        return jnp.sum(lax.dynamic_slice_in_dim(full, start, slab, axis=1).astype(F32), axis=0)

    small = jnp.stack(
        [
            jnp.concatenate([grad[0], grad[1].reshape(n_up, slab), column_sum(full)[None]])
            for grad, full in ((small0, g1_full), (small1, g_full))
        ]
    )
    *weight_grads, act1, grad0, small, norms = end(
        grads0,
        grads1,
        partial_x,
        act0,
        bias[1],
        partial_g,
        (grad1, x_block, *norm_rows(saved0), gain[0]),
        small,
        sums1,
    )
    g_qkv, g_out, g_up, g_down = weight_grads
    first = section == 0

    def pair(zero, one):
        sent = lax.ppermute(jnp.where(first, one, zero), "section", [(0, 1), (1, 0)])
        kept = jnp.where(first, zero, one)
        return jnp.where(first, jnp.stack([kept, sent]), jnp.stack([sent, kept]))[None]

    bias_out = small[3 + n_up][None]
    return (
        pair(act0, act1),
        pair(grad0, grad1),
        g_qkv[None],
        small[None, :3],
        g_out[None],
        bias_out,
        g_up[None],
        small[3 : 3 + n_up].reshape(1, -1),
        g_down[None],
        bias_out,
        norms[0:1],
        norms[1:2],
    )


def from_behind(value, axis, steps):
    count = lax.axis_size(axis)
    leading, last = (max(0, -steps), min(count, count - steps))
    return lax.ppermute(value, axis, [(source, source + steps) for source in range(leading, last)])


def gelu(value):
    inner = jnp.tanh(GELU_C * (value + GELU_K * value * value * value))
    return 0.5 * value * (1.0 + inner)


def gelu_slope(value):
    inner = jnp.tanh(GELU_C * (value + GELU_K * value * value * value))
    return 0.5 * (1.0 + inner) + 0.5 * value * (1.0 - inner * inner) * GELU_C * (
        1.0 + 3.0 * GELU_K * value * value
    )


def local_layout(ids_full, ctx_index, tokens):
    length = ids_full.shape[0]
    local_ids = lax.dynamic_slice_in_dim(ids_full, ctx_index * tokens, tokens)
    start = jnp.sum((ids_full[None, :] < local_ids[:, None]).astype(jnp.int32), axis=1)
    query_at = ctx_index * tokens + jnp.arange(tokens, dtype=jnp.int32)
    key_at = jnp.arange(length, dtype=jnp.int32)
    allowed = (key_at[None, :] <= query_at[:, None]) & (ids_full[None, :] == local_ids[:, None])
    return (query_at - start, allowed)


def score_block(query, keys):
    return jnp.einsum("thd,shd->hts", query, keys, preferred_element_type=jnp.float32) * HD ** (
        -0.5
    )


def forward_layer(layer_in, ids_full, params, ctx_index):
    w_qkv, b_qkv, w_out, b_out, w_up, b_up, w_down, b_down, gain, shift = params
    tokens = layer_in.shape[0]
    heads = w_qkv.shape[2] // HD
    wide_in = layer_in.astype(jnp.float32)
    row_sums = lax.psum((jnp.sum(wide_in, axis=1), jnp.sum(wide_in * wide_in, axis=1)), "tp")
    row_mean = row_sums[0] / D
    variance = row_sums[1] / D - row_mean * row_mean
    inverse_std = lax.rsqrt(variance + EPS)
    centered = (wide_in - row_mean[:, None]) * inverse_std[:, None]
    normed_part = (centered * gain.astype(jnp.float32) + shift.astype(jnp.float32)).astype(
        jnp.bfloat16
    )
    normed = lax.all_gather(normed_part, "tp", axis=1, tiled=True)
    positions, allowed = local_layout(ids_full, ctx_index, tokens)
    cosine, sine = rope_tables(positions)
    projected = (
        jnp.einsum("td,cde->cte", normed, w_qkv, preferred_element_type=jnp.float32)
        + b_qkv.astype(jnp.float32)[:, None, :]
    )
    query = rotate(projected[0].reshape(tokens, heads, HD), cosine, sine, 1.0).astype(jnp.bfloat16)
    key_rot = rotate(projected[1].reshape(tokens, heads, HD), cosine, sine, 1.0).astype(
        jnp.bfloat16
    )
    value_part = projected[2].reshape(tokens, heads, HD).astype(jnp.bfloat16)
    key_all, value_all = (
        lax.all_gather(key_rot, "ctx", axis=0, tiled=True),
        lax.all_gather(value_part, "ctx", axis=0, tiled=True),
    )
    scores = score_block(query, key_all)
    totals = jnp.sum(jnp.where(allowed[None], jnp.exp(scores), 0.0), axis=2)
    log_total = jnp.log(totals)
    probs = jnp.where(allowed[None], jnp.exp(scores - log_total[:, :, None]), 0.0).astype(
        jnp.bfloat16
    )
    attended = (
        jnp.einsum("hts,shd->thd", probs, value_all, preferred_element_type=jnp.float32)
        .astype(jnp.bfloat16)
        .reshape(tokens, heads * HD)
    )
    hidden_pre = jnp.dot(normed, w_up, preferred_element_type=jnp.float32) + b_up.astype(
        jnp.float32
    )
    hidden = gelu(hidden_pre).astype(jnp.bfloat16)
    summands = jnp.dot(attended, w_out, preferred_element_type=jnp.float32) + jnp.dot(
        hidden, w_down, preferred_element_type=jnp.float32
    )
    mixed = lax.psum_scatter(summands, "tp", scatter_dimension=1, tiled=True)
    layer_out = (wide_in + mixed + b_out.astype(jnp.float32) + b_down.astype(jnp.float32)).astype(
        jnp.bfloat16
    )
    kept = (key_rot, value_part)
    return (
        layer_out,
        (centered, inverse_std, normed, query, kept, attended, log_total, hidden_pre, hidden),
    )


def backward_layer(incoming, saved, ids_full, params, ctx_index):
    w_qkv, b_qkv, w_out, b_out, w_up, b_up, w_down, b_down, gain, shift = params
    centered, inverse_std, normed, query, kept, attended, log_total, hidden_pre, hidden = saved
    tokens = query.shape[0]
    heads = query.shape[1]
    wide_grad = incoming.astype(jnp.float32)
    grad_rows = lax.all_gather(incoming, "tp", axis=1, tiled=True)
    grad_out_bias = jnp.sum(wide_grad, axis=0)
    grad_out = jnp.einsum("tk,te->ke", attended, grad_rows, preferred_element_type=jnp.float32)
    d_attended = jnp.einsum(
        "te,ke->tk", grad_rows, w_out, preferred_element_type=jnp.float32
    ).astype(jnp.bfloat16)
    grad_down = jnp.einsum("tf,te->fe", hidden, grad_rows, preferred_element_type=jnp.float32)
    d_pre = jnp.einsum(
        "te,fe->tf", grad_rows, w_down, preferred_element_type=jnp.float32
    ) * gelu_slope(hidden_pre)
    grad_up_bias = jnp.sum(d_pre, axis=0)
    d_hidden = d_pre.astype(jnp.bfloat16)
    grad_up = jnp.einsum("td,tf->df", normed, d_hidden, preferred_element_type=jnp.float32)
    key_all, value_all = (
        lax.all_gather(kept[0], "ctx", axis=0, tiled=True),
        lax.all_gather(kept[1], "ctx", axis=0, tiled=True),
    )
    positions, allowed = local_layout(ids_full, ctx_index, tokens)
    cosine, sine = rope_tables(positions)
    d_heads = d_attended.reshape(tokens, heads, HD)
    out_heads = attended.reshape(tokens, heads, HD)
    delta = jnp.sum(d_heads.astype(jnp.float32) * out_heads.astype(jnp.float32), axis=2)
    scores = score_block(query, key_all)
    probs = jnp.where(allowed[None], jnp.exp(scores - log_total[:, :, None]), 0.0)
    d_probs = jnp.einsum("thd,shd->hts", d_heads, value_all, preferred_element_type=jnp.float32)
    d_scores = (probs * (d_probs - delta.T[:, :, None]) * HD ** (-0.5)).astype(jnp.bfloat16)
    d_query = jnp.einsum("hts,shd->thd", d_scores, key_all, preferred_element_type=jnp.float32)
    key_terms = jnp.einsum("hts,thd->shd", d_scores, query, preferred_element_type=jnp.float32)
    value_terms = jnp.einsum(
        "hts,thd->shd", probs.astype(jnp.bfloat16), d_heads, preferred_element_type=jnp.float32
    )
    d_key, d_value = (
        lax.psum_scatter(
            key_terms.astype(jnp.bfloat16), "ctx", scatter_dimension=0, tiled=True
        ).astype(jnp.float32),
        lax.psum_scatter(
            value_terms.astype(jnp.bfloat16), "ctx", scatter_dimension=0, tiled=True
        ).astype(jnp.float32),
    )
    d_projected = jnp.stack(
        [rotate(d_query, cosine, sine, -1.0), rotate(d_key, cosine, sine, -1.0), d_value]
    ).reshape(3, tokens, heads * HD)
    grad_qkv_bias = jnp.sum(d_projected, axis=1)
    d_qkv = d_projected.astype(jnp.bfloat16)
    grad_qkv = jnp.einsum("td,cte->cde", normed, d_qkv, preferred_element_type=jnp.float32)
    normed_terms = jnp.einsum("cte,cde->td", d_qkv, w_qkv, preferred_element_type=jnp.float32)
    normed_terms = normed_terms + jnp.einsum(
        "tf,df->td", d_hidden, w_up, preferred_element_type=jnp.float32
    )
    d_normed = lax.psum_scatter(
        normed_terms.astype(jnp.bfloat16), "tp", scatter_dimension=1, tiled=True
    ).astype(jnp.float32)
    grad_gain = jnp.sum(d_normed * centered, axis=0)
    grad_shift = jnp.sum(d_normed, axis=0)
    scaled = d_normed * gain.astype(jnp.float32)
    row_terms = lax.psum((jnp.sum(scaled, axis=1), jnp.sum(scaled * centered, axis=1)), "tp")
    grad_in = wide_grad + inverse_std[:, None] * (
        scaled - row_terms[0][:, None] / D - centered * (row_terms[1][:, None] / D)
    )
    grads = (
        grad_qkv,
        grad_qkv_bias,
        grad_out,
        grad_out_bias,
        grad_up,
        grad_up_bias,
        grad_down,
        grad_out_bias,
        grad_gain,
        grad_shift,
    )
    return (grad_in.astype(jnp.bfloat16), grads)


def base_shards(
    boundary,
    doc_ids,
    qkv_weight,
    qkv_bias,
    out_weight,
    out_bias,
    fc1_weight,
    fc1_bias,
    fc2_weight,
    fc2_bias,
    norm_gain,
    norm_shift,
):
    section = lax.axis_index("section")
    ctx_index = lax.axis_index("ctx")
    micro = boundary.shape[1]
    tokens = boundary.shape[2]
    width_part = boundary.shape[3]
    params = (
        lax.all_gather(qkv_weight[0], "ctx", axis=1, tiled=True),
        lax.all_gather(qkv_bias[0], "ctx", axis=1, tiled=True),
        lax.all_gather(out_weight[0], "ctx", axis=1, tiled=True),
        lax.all_gather(out_bias[0], "ctx", axis=0, tiled=True),
        lax.all_gather(fc1_weight[0], "ctx", axis=0, tiled=True),
        lax.all_gather(fc1_bias[0], "ctx", axis=0, tiled=True),
        lax.all_gather(fc2_weight[0], "ctx", axis=1, tiled=True),
        lax.all_gather(fc2_bias[0], "ctx", axis=0, tiled=True),
        lax.all_gather(norm_gain[0], "ctx", axis=0, tiled=True),
        lax.all_gather(norm_shift[0], "ctx", axis=0, tiled=True),
    )
    inputs = boundary[0]
    ticks = jnp.arange(micro + 1, dtype=jnp.int32)

    def forward_tick(received, tick):
        index = jnp.clip(tick - section, 0, micro - 1)
        first = lax.dynamic_index_in_dim(inputs, index, 0, keepdims=False)
        layer_in = jnp.where(section == 0, first, received)
        ids_full = lax.dynamic_index_in_dim(doc_ids, index, 0, keepdims=False)
        layer_out, saved = forward_layer(layer_in, ids_full, params, ctx_index)
        passed = from_behind(layer_out, "section", 1)
        return (passed, (layer_out, saved))

    start_zero = jnp.zeros((tokens, width_part), jnp.bfloat16)
    leftover, (outs_all, saved_all) = lax.scan(forward_tick, start_zero, ticks)
    held = lax.optimization_barrier(
        (
            (
                qkv_weight[0],
                qkv_bias[0],
                out_weight[0],
                out_bias[0],
                fc1_weight[0],
                fc1_bias[0],
                fc2_weight[0],
                fc2_bias[0],
                norm_gain[0],
                norm_shift[0],
            ),
            outs_all,
        )
    )[0]
    back_params = (
        lax.all_gather(held[0], "ctx", axis=1, tiled=True),
        lax.all_gather(held[1], "ctx", axis=1, tiled=True),
        lax.all_gather(held[2], "ctx", axis=1, tiled=True),
        lax.all_gather(held[3], "ctx", axis=0, tiled=True),
        lax.all_gather(held[4], "ctx", axis=0, tiled=True),
        lax.all_gather(held[5], "ctx", axis=0, tiled=True),
        lax.all_gather(held[6], "ctx", axis=1, tiled=True),
        lax.all_gather(held[7], "ctx", axis=0, tiled=True),
        lax.all_gather(held[8], "ctx", axis=0, tiled=True),
        lax.all_gather(held[9], "ctx", axis=0, tiled=True),
    )
    zero_grads = tuple((jnp.zeros(weight.shape, jnp.float32) for weight in params))

    def backward_tick(carry, tick):
        received, totals = carry
        raw_index = tick - (1 - section)
        valid = (raw_index >= 0) & (raw_index < micro)
        index = jnp.clip(raw_index, 0, micro - 1)
        cotangent = lax.dynamic_index_in_dim(inputs, index, 0, keepdims=False)
        incoming = jnp.where(section == 1, cotangent, received)
        incoming = jnp.where(valid, incoming, jnp.zeros_like(incoming))
        position_slot = index + section
        saved = jax.tree.map(
            lambda stacked: lax.dynamic_index_in_dim(stacked, position_slot, 0, keepdims=False),
            saved_all,
        )
        ids_full = lax.dynamic_index_in_dim(doc_ids, index, 0, keepdims=False)
        grad_in, terms = backward_layer(incoming, saved, ids_full, back_params, ctx_index)
        totals = tuple((total + term for total, term in zip(totals, terms)))
        passed = from_behind(grad_in, "section", -1)
        return ((passed, totals), grad_in)

    (leftover_grad, totals), grads_all = lax.scan(backward_tick, (start_zero, zero_grads), ticks)
    acts = lax.dynamic_slice_in_dim(outs_all, section, micro, 0)[None]
    input_grads = lax.dynamic_slice_in_dim(grads_all, 1 - section, micro, 0)[None]
    shares = (
        lax.psum_scatter(
            totals[0].astype(jnp.bfloat16), "ctx", scatter_dimension=1, tiled=True
        ).astype(jnp.float32),
        lax.psum_scatter(
            totals[1].astype(jnp.bfloat16), "ctx", scatter_dimension=1, tiled=True
        ).astype(jnp.float32),
        lax.psum_scatter(
            totals[2].astype(jnp.bfloat16), "ctx", scatter_dimension=1, tiled=True
        ).astype(jnp.float32),
        lax.psum_scatter(
            totals[3].astype(jnp.bfloat16), "ctx", scatter_dimension=0, tiled=True
        ).astype(jnp.float32),
        lax.psum_scatter(
            totals[4].astype(jnp.bfloat16), "ctx", scatter_dimension=0, tiled=True
        ).astype(jnp.float32),
        lax.psum_scatter(
            totals[5].astype(jnp.bfloat16), "ctx", scatter_dimension=0, tiled=True
        ).astype(jnp.float32),
        lax.psum_scatter(
            totals[6].astype(jnp.bfloat16), "ctx", scatter_dimension=1, tiled=True
        ).astype(jnp.float32),
        lax.psum_scatter(
            totals[7].astype(jnp.bfloat16), "ctx", scatter_dimension=0, tiled=True
        ).astype(jnp.float32),
        lax.psum_scatter(
            totals[8].astype(jnp.bfloat16), "ctx", scatter_dimension=0, tiled=True
        ).astype(jnp.float32),
        lax.psum_scatter(
            totals[9].astype(jnp.bfloat16), "ctx", scatter_dimension=0, tiled=True
        ).astype(jnp.float32),
    )
    return (
        acts,
        input_grads,
        shares[0][None],
        shares[1][None],
        shares[2][None],
        shares[3][None],
        shares[4][None],
        shares[5][None],
        shares[6][None],
        shares[7][None],
        shares[8][None],
        shares[9][None],
    )


def solution(mesh):
    specs = {
        "token": P("section", None, "ctx", "tp"),
        "rows": P("section", "tp", "ctx"),
        "columns": P("section", "ctx", "tp"),
        "vector": P("section", ("tp", "ctx")),
        "vectors": P("section", None, ("tp", "ctx")),
    }
    weights = ("token", "vectors", "rows", "vector", "columns", "vector", "rows", "vector", "vector", "vector")
    placed = tuple(specs[name] for name in weights)
    heads = D // HD
    place = {"section": 2, "ctx": 4, "tp": 4}
    whole_heads = heads % (mesh.shape["tp"] * mesh.shape["ctx"]) == 0
    return jax.shard_map(
        shards if whole_heads and dict(mesh.shape) == place else base_shards,
        mesh=mesh,
        in_specs=(specs["token"], P(), *placed),
        out_specs=(specs["token"], specs["token"], *placed),
        check_vma=False,
    )
```

```python
import functools
import itertools

import jax
import jax.numpy as jnp
from jax import lax
from jax.experimental import pallas as pl
from jax.experimental.pallas import tpu as pltpu
from jax.sharding import PartitionSpec as P

D = 2048
HD = 64
ROT = 32
EPS = 1e-05
GELU_C = 0.7978845608028654
GELU_K = 0.044715
ACT = "act"
ACTS = "acts"
ARRIVED = "arrived_"
ATT = "att"
BOUNCE = "bounce_"
B_QKV = "b_qkv"
B_UP = "b_up"
COLUMNS = "columns"
CORES = "cores"
COSINE = "cosine"
CTX = "ctx"
DOWN = "down"
D_W = "d_w_"
G = "g"
G1 = "g1"
GAIN = "gain"
GAIN_BLOCK = "gain_block"
GRAD = "grad"
GRADS = "grads"
G_BLOCK = "g_block"
HEADS_EQ = "hts,shd->thd"
HIDDEN = "hidden"
HOME = "home_"
INVERSE_STD = "inverse_std"
KEPT = "kept_"
KEYS_EQ = "hts,thd->shd"
LSE = "lse"
MEAN = "mean"
MEAN_BLOCK = "mean_block"
NORMED = "normed"
NORM_SUM = "norm_sum"
N_START = "start"
ONE = "one_"
OUT = "out"
PARTIAL = "partial"
QKV = "qkv"
ROWS = "rows"
SCORES_EQ = "thd,shd->hts"
SECTION = "section"
SHARD = "shard_"
SHIFT = "shift"
SINE = "sine"
SLOPE = "slope"
SMALL_SUM = "small_sum"
STD_BLOCK = "std_block"
SUMS = "sums"
TOKEN = "token"
TP = "tp"
TURNED = "turned_"
UP = "up"
VECTOR = "vector"
VECTORS = "vectors"
W = "w_"
X = "x"
X1 = "x1"
X_BLOCK = "x_block"
BF16 = jnp.bfloat16
F32 = jnp.float32


def rope_tables(positions):
    half = ROT // 2
    freq = 10000.0 ** (-(jnp.arange(half).astype(F32) * 2.0 / ROT))
    angle = positions.astype(F32)[:, None] * freq[None, :]
    return (jnp.cos(angle), jnp.sin(angle))


def rotate(field, cosine, sine, sign):
    half = ROT // 2
    first = field[..., :half]
    second = field[..., half:ROT]
    cosine = cosine[:, None, :]
    sine = sine[:, None, :] * sign
    return jnp.concatenate(
        [first * cosine - second * sine, second * cosine + first * sine, field[..., ROT:]], axis=-1
    )


def doc_tables(ids, heads):
    length = ids.shape[0]
    start = jnp.sum((ids[None, :] < ids[:, None]).astype(jnp.int32), axis=1)
    cosine, sine = rope_tables(jnp.arange(length, dtype=jnp.int32) - start)
    still = jnp.ones((length, HD - ROT), F32)
    cosine = jnp.tile(jnp.concatenate([cosine, cosine, still], axis=1), (1, heads))
    sine = jnp.tile(jnp.concatenate([-sine, sine, 0.0 * still], axis=1), (1, heads))
    return {N_START: start[:, None], COSINE: cosine, SINE: sine}


MESH = pl.DeviceIdType.MESH
FWD, BWD, LAST, START = 0, 1, 2, 3
GROUPS = 2


class Wire:
    def __init__(self, send_sems, recv_sems):
        self.send_sems, self.recv_sems = send_sems, recv_sems
        self.copies = []
        self.section = lax.axis_index(SECTION)
        self.c = lax.axis_index(CTX)
        self.t = lax.axis_index(TP)
        self.y = self.t // 2
        self.k = self.t % 2
        self.c_up = (self.c + 1) % 4
        self.c_far = (self.c + 2) % 4
        self.c_down = (self.c + 3) % 4
        self.t_y = (self.t + 2) % 4
        self.t_core = self.t + 1 - 2 * self.k
        self.up = {CTX: jnp.minimum(self.c + 1, 3)}
        self.down = {CTX: jnp.maximum(self.c - 1, 0)}
        self.beside = {TP: self.t_y}
        self.core = {TP: self.t_core}
        self.across = {SECTION: 1 - self.section}
        self.others = [(2, self.c_far), (1, self.c_up), (3, self.c_down)]

    def greet(self, targets):
        barrier = pltpu.get_barrier_semaphore()
        for target in targets:
            pl.semaphore_signal(barrier, inc=1, device_id=target, device_id_type=MESH)
        pl.semaphore_wait(barrier, len(targets))

    def send(self, source, target, device, when=None):
        index = len(self.copies)
        copy = pltpu.make_async_remote_copy(
            src_ref=source,
            dst_ref=target,
            send_sem=self.send_sems.at[index],
            recv_sem=self.recv_sems.at[index],
            device_id=device,
            device_id_type=MESH,
        )
        if when is None:
            copy.start()
        else:
            pl.when(when)(copy.start)
        self.copies.append((copy, when))
        return copy

    def send_one_of(self, first, source, other_source, target, device):
        index = len(self.copies)
        copies = [
            pltpu.make_async_remote_copy(
                src_ref=ref,
                dst_ref=target,
                send_sem=self.send_sems.at[index],
                recv_sem=self.recv_sems.at[index],
                device_id=device,
                device_id_type=MESH,
            )
            for ref in (source, other_source)
        ]
        pl.when(first)(copies[0].start)
        pl.when(jnp.logical_not(first))(copies[1].start)
        self.copies.append((copies[0], None))
        return copies[0]

    def flush(self, indices):
        for index in indices:
            if self.copies[index] is not None:
                copy, when = self.copies[index]
                self.copies[index] = None
                if when is None:
                    copy.wait_send()
                else:
                    pl.when(when)(copy.wait_send)

    def drain(self):
        self.flush(range(len(self.copies)))

    def meet(self, semaphore, peers):
        for peer in peers:
            pl.semaphore_signal(semaphore, inc=1, device_id=peer, device_id_type=MESH)
        pl.semaphore_wait(semaphore, len(peers))


class Gather:
    def __init__(self, wire, full, rows, part, skew=1):
        self.w, self.full, self.rows, self.part = wire, full, rows, part
        self.size, self.skew = rows // GROUPS, skew
        self.hops, self.beside = {}, {}

    def region(self, c, t, group):
        return self.full.at[
            pl.ds(pl.multiple_of(c * self.rows + group * self.size, 16), self.size),
            pl.ds(pl.multiple_of(t * self.part, 128), self.part),
        ]

    def pass_on(self, device, c, t, group, when=None):
        spot = self.region(c, t, group)
        return self.w.send(spot, spot, device, when)

    def begin(self, group):
        w = self.w
        self.hops[group, 1] = self.pass_on(w.up, w.c, w.t, group, w.c < 3)
        self.hops[group, -1] = self.pass_on(w.down, w.c, w.t, group, w.c > 0)
        self.beside[group, 0] = self.pass_on(w.beside, w.c, w.t, group)
        self.cores = getattr(self, CORES, [])
        self.cores.append((self.pass_on(w.core, w.c, w.t, group), None))

    def steps(self):
        return itertools.chain(self.along(), self.around())

    def hop_order(self):
        events = [
            (group, sign * hop) for group in range(GROUPS) for hop in (1, 2, 3) for sign in (1, -1)
        ]
        return sorted(events, key=lambda event: (self.skew * event[0] + abs(event[1]), event[0]))

    def along(self):
        w = self.w
        for group, hop in self.hop_order():
            source = jnp.clip(w.c - hop, 0, 3)
            there = w.c >= hop if hop > 0 else w.c - hop <= 3
            pl.when(there)(self.hops[group, hop].wait_recv)
            if abs(hop) < 3:
                further = hop + (1 if hop > 0 else -1)
                ahead = w.c < 3 if hop > 0 else w.c > 0
                self.hops[group, further] = self.pass_on(
                    w.up if hop > 0 else w.down, source, w.t, group, jnp.logical_and(there, ahead)
                )
            self.beside[group, hop] = self.pass_on(w.beside, source, w.t, group, there)
            self.cores.append((self.pass_on(w.core, source, w.t, group, there), there))
            yield

    def around(self):
        w = self.w
        for group, hop in [(group, 0) for group in range(GROUPS)] + self.hop_order():
            source = jnp.clip(w.c - hop, 0, 3)
            there = None if hop == 0 else w.c >= hop if hop > 0 else w.c - hop <= 3
            copy = self.beside[group, hop]
            copy.wait_recv() if there is None else pl.when(there)(copy.wait_recv)
            self.cores.append((self.pass_on(w.core, source, w.t_y, group, there), there))
            yield
        for copy, there in self.cores:
            copy.wait_recv() if there is None else pl.when(there)(copy.wait_recv)


class DirectGather(Gather):
    def begin(self, group):
        w = self.w
        for step, place in w.others:
            self.hops[group, step] = self.pass_on({CTX: place}, w.c, w.t, group)
        self.beside[group, 0] = self.pass_on(w.beside, w.c, w.t, group)
        self.cores = getattr(self, CORES, [])
        self.cores.append((self.pass_on(w.core, w.c, w.t, group), None))

    def steps(self):
        w = self.w
        order = [(group, step) for group in range(GROUPS) for step in (1, 3, 2)]
        for group, step in order:
            source = (w.c + 4 - step) % 4
            self.hops[group, step].wait_recv()
            self.beside[group, step] = self.pass_on(w.beside, source, w.t, group)
            self.cores.append((self.pass_on(w.core, source, w.t, group), None))
            yield
        for group, step in [(group, 0) for group in range(GROUPS)] + order:
            self.beside[group, step].wait_recv()
            source = (w.c + 4 - step) % 4
            self.cores.append((self.pass_on(w.core, source, w.t_y, group), None))
            yield
        for copy, _ in self.cores:
            copy.wait_recv()


def scatter_scratch(rows, part):
    return [
        pltpu.VMEM((2, 4 * rows, part), BF16),
        pltpu.VMEM((2, 4 * rows, part), BF16),
        pltpu.VMEM((4 * rows, part), BF16),
        pltpu.VMEM((3, rows, part), BF16),
    ]


class Scatter:
    def __init__(self, wire, partial, scratch, rows, part):
        self.w, self.partial, self.rows, self.part = wire, partial, rows, part
        self.theirs, self.chip, self.from_y, self.from_far = scratch
        w = wire
        self.places = [(2, w.c_far), (1, w.c_up), (3, w.c_down), (0, w.c)]
        self.order = [
            (group, c, y)
            for group in (0, 1)
            for y in (1 - w.y, w.y)
            for _, c in self.places
        ]
        self.far, self.sent = {}, []

    def send(self, source, target, device):
        self.sent.append(len(self.w.copies))
        return self.w.send(source, target, device)

    def span(self, group, c):
        size = self.rows // 2
        return pl.ds(pl.multiple_of(c * self.rows + group * size, 16), size)

    def begin(self):
        w = self.w
        self.cores = []
        for group, c, y in self.order:
            columns = pl.ds(pl.multiple_of((2 * y + 1 - w.k) * self.part, 128), self.part)
            self.cores.append(
                self.send(
                    self.partial.at[self.span(group, c), columns],
                    self.theirs.at[y, self.span(group, c)],
                    w.core,
                )
            )

    def take(self, index):
        group, c, y = self.order[index]
        self.cores[index].wait_recv()
        rows = self.span(group, c)
        columns = pl.ds(pl.multiple_of((2 * y + self.w.k) * self.part, 128), self.part)
        return self.partial[rows, columns].astype(F32) + self.theirs[y, rows].astype(F32)

    def run(self):
        for _ in self.steps():
            pass

    def steps(self):
        w = self.w
        half = self.rows // 2
        beside = {}
        for group in (0, 1):
            for slot, (_, c) in enumerate(self.places):
                rows = self.span(group, c)
                self.chip[1 - w.y, rows] = self.take(8 * group + slot).astype(BF16)
                beside[group, slot] = self.send(
                    self.chip.at[1 - w.y, rows], self.from_y.at[rows], w.beside
                )
                yield
        for group in (0, 1):
            for slot, (step, c) in enumerate(self.places):
                rows = self.span(group, c)
                value = self.take(8 * group + 4 + slot)
                beside[group, slot].wait_recv()
                self.chip[w.y, rows] = (value + self.from_y[rows].astype(F32)).astype(BF16)
                if step:
                    self.far[group, step] = self.send(
                        self.chip.at[w.y, rows],
                        self.from_far.at[step - 1, pl.ds(group * half, half)],
                        {CTX: c},
                    )
                yield

    def total(self, group):
        half = self.rows // 2
        value = self.chip[self.w.y, self.span(group, self.w.c)].astype(F32)
        for step in (1, 3, 2):
            self.far[group, step].wait_recv()
            value += self.from_far[step - 1, pl.ds(group * half, half)].astype(F32)
        return value


def neighbours(w):
    return [{CTX: place} for _, place in w.others] + [w.beside, w.core]


def diagonal(w):
    return {TP: (w.t_core + 2) % 4}


def back_scratch(rows, part):
    return [
        pltpu.VMEM((rows, part), F32),
        pltpu.VMEM((GROUPS, 8, 128), F32),
        pltpu.VMEM((GROUPS, 3, 8, 128), F32),
    ]


def norm_back(w, scatter, blocks, scratch, rows, part, grad, sums, done, fill=iter(())):
    g_block, x_block, mean, inverse_std, gain = blocks
    d_normed, row_out, row_in = scratch
    half = rows // GROUPS
    width = 4 * part
    lane = lax.broadcasted_iota(jnp.int32, (128, 128), 1)
    sent = []
    gain_sum = jnp.zeros((1, part), F32)
    shift_sum = jnp.zeros((1, part), F32)
    for group in range(GROUPS):
        own = slice(group * half, (group + 1) * half)
        value = scatter.total(group)
        for _ in range(2):
            next(fill, None)
        d_normed[own] = value
        centered = (x_block[own].astype(F32) - mean[own]) * inverse_std[own]
        weighted = value * centered
        gain_sum += jnp.sum(weighted, axis=0, keepdims=True)
        shift_sum += jnp.sum(value, axis=0, keepdims=True)
        first = jnp.sum(value * gain[...], axis=1, keepdims=True)
        second = jnp.sum(weighted * gain[...], axis=1, keepdims=True)
        packed = jnp.where(lane == 0, first, jnp.where(lane == 1, second, 0.0))
        row_out[group] = packed.T[:8]
        sent.append(
            [
                w.send(row_out.at[group], row_in.at[group, slot], peer)
                for slot, peer in enumerate((w.beside, w.core, diagonal(w)))
            ]
        )
    sums[...] = jnp.concatenate(
        [gain_sum, shift_sum, jnp.zeros((6, part), F32)], axis=0
    )
    for group in range(GROUPS):
        own = slice(group * half, (group + 1) * half)
        next(fill, None)
        for copy in sent[group]:
            copy.wait_recv()
        rows_sum = row_out[group] + row_in[group, 0] + row_in[group, 1] + row_in[group, 2]
        columns = jnp.concatenate([rows_sum, jnp.zeros((half - 8, 128), F32)], axis=0).T
        centered = (x_block[own].astype(F32) - mean[own]) * inverse_std[own]
        scaled = d_normed[own] * gain[...]
        value = g_block[own].astype(F32) + inverse_std[own] * (
            scaled - columns[:, 0:1] / width - centered * (columns[:, 1:2] / width)
        )
        grad[own] = value.astype(BF16)
        done(group)


class Turn:
    def __init__(self, d_part, e_part, f_part):
        self.d, self.e, self.f = d_part, e_part, f_part

    def rows(self, name):
        return {QKV: self.d, OUT: self.e, UP: self.d, DOWN: self.f}[name]

    def inner(self, name, half):
        size = self.rows(name)
        return (0, size) if half is None else (half * size // 2, size // 2)

    def shard(self, name, ref, c, half=None):
        start, size = self.inner(name, half)
        if name == QKV:
            return ref.at[:, pl.ds(start, size), pl.ds(pl.multiple_of(c * self.e, 128), self.e)]
        if name == UP:
            return ref.at[pl.ds(start, size), pl.ds(pl.multiple_of(c * self.f, 128), self.f)]
        stride = self.e if name == OUT else self.f
        return ref.at[pl.ds(pl.multiple_of(c * stride + start, 16), size)]

    def turned(self, name, ref, c, half=None):
        start, size = self.inner(name, half)
        if name == QKV:
            return ref.at[:, pl.ds(pl.multiple_of(c * self.d + start, 16), size)]
        if name == UP:
            return ref.at[pl.ds(pl.multiple_of(c * self.d + start, 16), size)]
        return ref.at[pl.ds(start, size), pl.ds(pl.multiple_of(c * self.d, 128), self.d)]

    def piece_shape(self, name, halved=False):
        size = self.rows(name) // (2 if halved else 1)
        return {
            QKV: (3, size, self.e),
            OUT: (size, self.d),
            UP: (size, self.f),
            DOWN: (size, self.d),
        }[name]

    def turned_shape(self, name):
        return {
            QKV: (3, 4 * self.d, self.e),
            OUT: (self.e, 4 * self.d),
            UP: (4 * self.d, self.f),
            DOWN: (self.f, 4 * self.d),
        }[name]


NAMES = (QKV, OUT, UP, DOWN)


def everyone(w):
    return [
        {SECTION: (w.section + ds) % 2, CTX: (w.c + dc) % 4, TP: (w.t + dt) % 4}
        for ds in range(2)
        for dc in range(4)
        for dt in range(4)
        if (ds, dc, dt) != (0, 0, 0)
    ]


TILE = 256


def dot(a, b, contract=((1,), (0,))):
    return lax.dot_general(a, b, (contract, ((), ())), preferred_element_type=F32)


def tile(i, size=TILE):
    return pl.ds(pl.multiple_of(i * size, size), size)


def turn_heads(value, cosine, sine, sign):
    half = ROT // 2
    width = value.shape[1]
    lane = lax.broadcasted_iota(jnp.int32, value.shape, 1) % HD
    partner = jnp.where(
        lane < half, pltpu.roll(value, width - half, 1), pltpu.roll(value, half, 1)
    )
    return value * cosine + partner * (sine * sign)


def head_mask(shape, head):
    lane = lax.broadcasted_iota(jnp.int32, shape, 1)
    return jnp.logical_and(lane >= head * HD, lane < (head + 1) * HD)


def of_head(value, head):
    return jnp.where(head_mask(value.shape, head), value, jnp.zeros_like(value))


def allowed_keys(start, first_row, shape):
    row = lax.broadcasted_iota(jnp.int32, shape, 0) + first_row
    column = lax.broadcasted_iota(jnp.int32, shape, 1)
    return jnp.logical_and(column >= start, column <= row)


def forward_steps(r, lean=False):
    tokens, width = r.x.shape
    heads = r.att.shape[1] // HD

    def norm(i):
        rows = tile(i, 64)
        value = r.x[rows].astype(F32)
        mean = jnp.sum(value, axis=1, keepdims=True) / width
        variance = jnp.sum(value * value, axis=1, keepdims=True) / width - mean * mean
        inverse_std = lax.rsqrt(variance + EPS)
        r.mean[rows] = mean
        r.inverse_std[rows] = inverse_std
        r.normed[rows] = ((value - mean) * inverse_std * r.gain[...] + r.shift[...]).astype(BF16)

    def project(i):
        rows = tile(i)
        normed = r.normed[rows]
        for c in range(3):
            value = dot(normed, r.w_qkv[c]) + r.b_qkv[c : c + 1]
            if c < 2:
                value = turn_heads(value, r.cosine[rows], r.sine[rows], 1.0)
            r.qkv[c, rows] = value.astype(BF16)

    def attend(i):
        rows = pl.ds(i * TILE, TILE)
        keys = (i + 1) * TILE
        query, key, value = r.qkv[0, rows], r.qkv[1, :keys], r.qkv[2, :keys]
        allowed = allowed_keys(r.start[rows], i * TILE, (TILE, keys))
        total = jnp.zeros((TILE, heads * HD), F32)
        for head in range(heads):
            scores = dot(of_head(query, head), key, ((1,), (1,))) * HD ** (-0.5)
            sums = jnp.sum(jnp.where(allowed, jnp.exp(scores), 0.0), axis=1, keepdims=True)
            log_total = jnp.log(sums)
            r.lse[head, rows] = log_total
            probs = jnp.where(allowed, jnp.exp(scores - log_total), 0.0).astype(BF16)
            total += dot(probs, of_head(value, head))
        r.att[rows] = total.astype(BF16)

    def up(i):
        rows = tile(i)
        value = dot(r.normed[rows], r.w_up[...]) + r.b_up[...]
        inner = jnp.tanh(GELU_C * (value + GELU_K * value * value * value))
        r.hidden[rows] = (0.5 * value * (1.0 + inner)).astype(BF16)
        r.slope[rows] = 0.5 * (1.0 + inner) + 0.5 * value * (1.0 - inner * inner) * GELU_C * (
            1.0 + 3.0 * GELU_K * value * value
        )

    def down(i):
        rows = tile(i)
        r.partial[rows] = (
            dot(r.att[rows], r.w_out[...]) + dot(r.hidden[rows], r.w_down[...])
        ).astype(BF16)

    count = tokens // TILE
    return norm, project, attend, up, down, count


def each(count, step):
    lax.fori_loop(0, count, lambda i, _: (step(i), 0)[1], 0)


def some(begin, end, step):
    lax.fori_loop(begin, end, lambda i, _: (step(i), 0)[1], 0)


def run_forward(r):
    norm, project, attend, up, down, count = forward_steps(r)
    each(r.x.shape[0] // 64, norm)
    each(count, project)
    for i in range(count):
        attend(i)
    each(count, up)
    each(count, down)


def backward_steps(r):
    tokens, width = r.g.shape
    heads = r.att.shape[1] // HD
    count = tokens // TILE

    def start():
        r.d_b_up[...] = jnp.zeros_like(r.d_b_up)
        r.d_b_qkv[...] = jnp.zeros_like(r.d_b_qkv)
        r.d_kv[...] = jnp.zeros_like(r.d_kv)

    def open_branches(i):
        rows = tile(i)
        g = r.g[rows]
        d_pre = dot(g, r.w_down[...], ((1,), (1,))) * r.slope[rows]
        r.d_b_up[...] += jnp.sum(d_pre, axis=0, keepdims=True)
        r.d_hidden[rows] = d_pre.astype(BF16)
        r.d_att[rows] = dot(g, r.w_out[...], ((1,), (1,))).astype(BF16)

    def grad_rows(i):
        columns = tile(i)
        g = r.g[:, columns]
        r.d_w_down[:, columns] = dot(r.hidden[...], g, ((0,), (0,))).astype(BF16)
        r.d_w_out[:, columns] = dot(r.att[...], g, ((0,), (0,))).astype(BF16)

    def grad_up(i):
        rows = tile(i)
        r.d_w_up[rows] = dot(r.normed[:, rows], r.d_hidden[...], ((0,), (0,))).astype(BF16)

    def attend(i):
        rows = pl.ds(i * TILE, TILE)
        keys = (i + 1) * TILE
        query, key, value = r.qkv[0, rows], r.qkv[1, :keys], r.qkv[2, :keys]
        d_att = r.d_att[rows]
        product = d_att.astype(F32) * r.att[rows].astype(F32)
        allowed = allowed_keys(r.start[rows], i * TILE, (TILE, keys))
        d_query = jnp.zeros((TILE, heads * HD), F32)
        d_key = jnp.zeros((keys, heads * HD), F32)
        d_value = jnp.zeros((keys, heads * HD), F32)
        for head in range(heads):
            q_head, d_head = of_head(query, head), of_head(d_att, head)
            scores = dot(q_head, key, ((1,), (1,))) * HD ** (-0.5)
            probs = jnp.where(allowed, jnp.exp(scores - r.lse[head, rows]), 0.0)
            delta = jnp.sum(of_head(product, head), axis=1, keepdims=True)
            d_probs = dot(d_head, value, ((1,), (1,)))
            d_scores = (probs * (d_probs - delta) * HD ** (-0.5)).astype(BF16)
            d_query += dot(d_scores, of_head(key, head))
            d_key += dot(d_scores, q_head, ((0,), (0,)))
            d_value += dot(probs.astype(BF16), d_head, ((0,), (0,)))
        r.d_query[rows] = d_query
        r.d_kv[0, :keys] += d_key
        r.d_kv[1, :keys] += d_value

    def unrotate(i):
        rows = tile(i)
        cosine, sine = r.cosine[rows], r.sine[rows]
        parts = (
            turn_heads(r.d_query[rows], cosine, sine, -1.0),
            turn_heads(r.d_kv[0, rows], cosine, sine, -1.0),
            r.d_kv[1, rows],
        )
        for c, value in enumerate(parts):
            r.d_b_qkv[c : c + 1] += jnp.sum(value, axis=0, keepdims=True)
            r.d_qkv[c, rows] = value.astype(BF16)

    def grad_qkv(i):
        rows = tile(i)
        normed = r.normed[:, rows]
        for c in range(3):
            r.d_w_qkv[c, rows] = dot(normed, r.d_qkv[c], ((0,), (0,))).astype(BF16)

    def close(i):
        rows = tile(i)
        total = dot(r.d_hidden[rows], r.w_up[...], ((1,), (1,)))
        for c in range(3):
            total += dot(r.d_qkv[c, rows], r.w_qkv[c], ((1,), (1,)))
        r.partial[rows] = total.astype(BF16)

    return start, open_branches, grad_rows, grad_up, attend, unrotate, grad_qkv, close, count


def run_backward(r):
    start, open_branches, grad_rows, grad_up, attend, unrotate, grad_qkv, close, count = backward_steps(r)
    wide = r.g.shape[1] // TILE
    start()
    each(count, open_branches)
    each(wide, grad_rows)
    each(wide, grad_up)
    for i in range(count):
        attend(i)
    each(count, unrotate)
    each(wide, grad_qkv)
    each(count, close)


class Refs:
    def __init__(self, **refs):
        self.__dict__.update(refs)


WEIGHTS = ("w_qkv", "w_out", "w_up", "w_down", B_QKV, B_UP, GAIN, SHIFT)
TABLES = (N_START, COSINE, SINE)
SAVED = (NORMED, QKV, ATT, LSE, SLOPE, HIDDEN)


def saved_shapes(tokens, width, e, f):
    return {
        NORMED: ((tokens, width), BF16),
        QKV: ((3, tokens, e), BF16),
        ATT: ((tokens, e), BF16),
        LSE: ((e // HD, tokens, 1), F32),
        SLOPE: ((tokens, f), F32),
        HIDDEN: ((tokens, f), BF16),
    }


def scratch_shapes_back(tokens, e, f):
    return {
        "d_hidden": ((tokens, f), BF16),
        "d_att": ((tokens, e), BF16),
        "d_query": ((tokens, e), F32),
        "d_kv": ((2, tokens, e), F32),
        "d_qkv": ((3, tokens, e), BF16),
    }


def grad_shapes(width, e, f):
    return {
        "d_w_qkv": ((3, width, e), BF16),
        "d_w_out": ((e, width), BF16),
        "d_w_up": ((width, f), BF16),
        "d_w_down": ((f, width), BF16),
        "d_b_qkv": ((3, e), F32),
        "d_b_up": ((1, f), F32),
    }


def remote_call(body, name, key, inputs, outputs, scratch, copies, in_hbm=(), out_hbm=()):
    vmem = pl.BlockSpec(memory_space=pltpu.VMEM)
    hbm = pl.BlockSpec(memory_space=pl.ANY)
    keys = list(inputs) + list(outputs) + list(scratch) + ["free_sem", "local_sems", "send_sems", "recv_sems"]

    def kernel(*refs):
        body(Refs(**dict(zip(keys, refs))))

    outs = pl.pallas_call(
        kernel,
        out_shape=tuple(jax.ShapeDtypeStruct(shape, kind) for shape, kind in outputs.values()),
        in_specs=[hbm if each_in in in_hbm else vmem for each_in in inputs],
        out_specs=tuple(hbm if each_out in out_hbm else vmem for each_out in outputs),
        scratch_shapes=[pltpu.VMEM(shape, kind) for shape, kind in scratch.values()]
        + [
            pltpu.SemaphoreType.REGULAR,
            pltpu.SemaphoreType.DMA((32,)),
            pltpu.SemaphoreType.DMA((copies,)),
            pltpu.SemaphoreType.DMA((copies,)),
        ],
        compiler_params=pltpu.CompilerParams(
            collective_id=key, has_side_effects=True, vmem_limit_bytes=63 << 20
        ),
        name=name,
    )(*inputs.values())
    return dict(zip(outputs, outs))


def weight_scratch(turn):
    shapes = {W + name: (turn.turned_shape(name), BF16) for name in NAMES}
    width = 4 * turn.d
    return shapes | {
        B_QKV: ((3, turn.e), F32),
        B_UP: ((1, turn.f), F32),
        GAIN: ((1, width), F32),
        SHIFT: ((1, width), F32),
    }


def scatter_dict(rows, part):
    return {
        "theirs": ((2, 4 * rows, part), BF16),
        "chip": ((2, 4 * rows, part), BF16),
        "from_y": ((4 * rows, part), BF16),
        "from_far": ((3, rows, part), BF16),
    }


def back_dict(rows, part):
    return {
        "d_normed": ((rows, part), F32),
        "row_out": ((GROUPS, 8, 128), F32),
        "row_in": ((GROUPS, 3, 8, 128), F32),
    }


def scatter_of(w, r, partial, rows, part):
    return Scatter(w, partial, (r.theirs, r.chip, r.from_y, r.from_far), rows, part)


def small_params(w, r, layer):
    part = r.gain.shape[1] // 4
    slab = part // 4
    for t in range(4):
        for c in range(4):
            lanes = slice(t * part + c * slab, t * part + (c + 1) * slab)
            r.gain[:, lanes] = r.vectors[layer, c, t, 1:2]
            r.shift[:, lanes] = r.vectors[layer, c, t, 2:3]
    r.b_qkv[...] = r.vectors[layer, w.c, w.t, 3:6]
    for i in range(r.b_up.shape[1] // slab):
        r.b_up[:, i * slab : (i + 1) * slab] = r.vectors[layer, w.c, w.t, 6 + i : 7 + i]


def own_bias(w, r, layer):
    return jnp.concatenate([r.vectors[layer, c, w.t, 0:1] for c in range(4)], axis=1)


def own_gain(w, r, layer):
    return jnp.concatenate([r.vectors[layer, c, w.t, 1:2] for c in range(4)], axis=1)


FIRST = (OUT, QKV, UP, DOWN)
HALVES = {OUT: (None,), QKV: (None,), UP: (0, 1), DOWN: (0, 1)}


def pull(*generators, times=1):
    for _ in range(times):
        for generator in generators:
            next(generator, None)


def first_body(turn, rows, part, r):
    w = Wire(r.send_sems, r.recv_sems)
    s = w.section
    peers = everyone(w)
    w.greet(peers)
    shards = {name: getattr(r, SHARD + name) for name in NAMES}
    mine = {name: getattr(r, TURNED + name).at[s] for name in NAMES}
    bounce = {name: getattr(r, BOUNCE + name) for name in NAMES}
    swap = w.send(r.own.at[1 - s], r.other, w.across)
    r.vectors[s, w.c, w.t] = r.vector[...]
    told = [w.send(r.vector, r.vectors.at[s, w.c, w.t], peer) for peer in peers]
    local, far, across, puts = {}, {}, {name: [] for name in NAMES}, {}

    def send_along(name):
        for half in HALVES[name]:
            for step, place in w.others:
                far[name, step, half] = w.send(
                    turn.shard(name, shards[name], place, half),
                    turn.turned(name, mine[name], w.c, half),
                    {CTX: place},
                )
                yield

    def pass_across(name):
        for half in HALVES[name]:
            for step in (1, 3, 2):
                far[name, step, half].wait_recv()
                spot = turn.turned(name, mine[name], (w.c + 4 - step) % 4, half)
                across[name].append(w.send(spot, spot, w.across))
                yield

    def fetch(name):
        for copy in across[name]:
            copy.wait_recv()
        puts[name].wait()
        i = FIRST.index(name)
        copy = pltpu.make_async_copy(
            getattr(r, TURNED + name).at[0], getattr(r, W + name), r.local_sems.at[8 + i]
        )
        copy.start()
        return copy

    sending = itertools.chain(*(send_along(name) for name in FIRST))
    passing = itertools.chain(*(pass_across(name) for name in FIRST))
    pull(sending, times=6)
    for i, name in enumerate(FIRST):
        own_piece = turn.shard(name, shards[name], w.c)
        across[name].append(w.send(own_piece, turn.turned(name, mine[name], w.c), w.across))
        local[name] = pltpu.make_async_copy(own_piece, bounce[name], r.local_sems.at[i])
        local[name].start()
    swap.wait_recv()
    mine_block = r.own[s]
    r.x_block[...] = jnp.where(s == 0, mine_block, r.other[...])
    r.g_block[...] = jnp.where(s == 0, r.other[...], mine_block)
    half = rows // GROUPS
    gather_x = DirectGather(w, r.x, rows, part)
    for group in range(GROUPS):
        gather_x.region(w.c, w.t, group)[...] = r.x_block[group * half : (group + 1) * half]
        gather_x.begin(group)
    for i, name in enumerate(FIRST):
        local[name].wait()
        puts[name] = pltpu.make_async_copy(
            bounce[name], turn.turned(name, mine[name], w.c), r.local_sems.at[4 + i]
        )
        puts[name].start()
    pull(passing, times=6)
    pull(sending, times=3)
    for i, _ in enumerate(gather_x.steps()):
        if i == 5:
            pull(sending, times=3)
    for copy in told:
        copy.wait_recv()
    small_params(w, r, 0)
    norm, project, attend, up, down, count = forward_steps(r)
    each(4 * rows // 64, norm)
    ready = [fetch(OUT), fetch(QKV)]
    for copy in ready:
        copy.wait()
    each(count, project)
    pull(passing, times=3)
    pull(sending, times=3)
    attend(0)
    attend(1)
    pull(passing, times=3)
    pull(sending, times=3)
    for i in range(2, count):
        attend(i)
    fetch(UP).wait()
    each(count, up)
    for _ in passing:
        pass
    fetch(DOWN).wait()
    each(count, down)
    scatter = scatter_of(w, r, r.partial, rows, part)
    scatter.begin()
    scatter.run()
    gather = Gather(w, r.x1, rows, part)
    bias = own_bias(w, r, 0)
    for group in range(GROUPS):
        own = slice(group * half, (group + 1) * half)
        value = (r.x_block[own].astype(F32) + scatter.total(group) + bias).astype(BF16)
        r.act[own] = value
        gather.region(w.c, w.t, group)[...] = value
        gather.begin(group)
    for _ in gather.steps():
        pass
    w.drain()


def first(own, vector, tables, shards):
    _, rows, part = own.shape
    turn = Turn(shards[QKV].shape[1], shards[QKV].shape[2] // 4, shards[UP].shape[1] // 4)
    tokens, width = 4 * rows, 4 * part
    full = ((tokens, width), BF16)
    block = ((rows, part), BF16)
    outputs = {TURNED + name: ((2,) + turn.turned_shape(name), BF16) for name in NAMES}
    outputs |= {X1: full, X_BLOCK: block, G_BLOCK: block, ACT: block}
    outputs |= {VECTORS: ((2, 4, 4) + vector.shape, F32)}
    outputs |= saved_shapes(tokens, width, turn.e, turn.f)
    outputs |= {MEAN: ((tokens, 1), F32), INVERSE_STD: ((tokens, 1), F32)}
    scratch = {BOUNCE + name: (turn.piece_shape(name), BF16) for name in NAMES}
    scratch |= {"other": block, X: full, PARTIAL: full}
    scratch |= weight_scratch(turn) | scatter_dict(rows, part)
    return remote_call(
        functools.partial(first_body, turn, rows, part),
        "first",
        START,
        {"own": own, VECTOR: vector}
        | tables
        | {SHARD + name: shards[name] for name in NAMES},
        outputs,
        scratch,
        320,
        in_hbm=[SHARD + name for name in NAMES],
        out_hbm=[TURNED + name for name in NAMES],
    )


def middle_body(turn, rows, part, r):
    w = Wire(r.send_sems, r.recv_sems)
    loads = {}
    for i, name in enumerate(FIRST):
        loads[name] = pltpu.make_async_copy(
            getattr(r, TURNED + name).at[1], getattr(r, W + name), r.local_sems.at[i]
        )
        loads[name].start()
    w.greet(neighbours(w) + [diagonal(w)])
    half = rows // GROUPS
    gather_g = Gather(w, r.g, rows, part, skew=0)
    for group in range(GROUPS):
        gather_g.region(w.c, w.t, group)[...] = r.g_block[group * half : (group + 1) * half]
        gather_g.begin(group)
    arriving = gather_g.steps()
    small_params(w, r, 1)
    norm, project, attend, up, down, count = forward_steps(r)
    each(4 * rows // 64, norm)
    pull(arriving, times=4)
    loads[QKV].wait()
    each(count, project)
    attend(0)
    pull(arriving, times=4)
    attend(1)
    attend(2)
    pull(arriving, times=4)
    attend(3)
    pull(arriving, times=6)
    loads[UP].wait()
    each(count, up)
    loads[DOWN].wait()
    loads[OUT].wait()
    each(count, down)
    for _ in arriving:
        pass
    b = Refs(**dict(r.__dict__, partial=r.partial_g))
    start, open_branches, grad_rows, grad_up, attend_back, unrotate, grad_qkv, close, _ = (
        backward_steps(b)
    )
    start()
    each(count, open_branches)
    for i in range(count):
        attend_back(i)
    each(count, unrotate)
    each(count, close)

    def leftover():
        wide = 4 * part // TILE
        for step, times in ((grad_rows, wide), (grad_up, wide), (grad_qkv, wide)):
            for i in range(0, times, 2):
                some(i, i + 2, step)
                yield

    fill = leftover()
    scatter = scatter_of(w, r, r.partial_g, rows, part)
    scatter.begin()
    for i, _ in enumerate(scatter.steps()):
        if i % 2 == 1:
            pull(fill)
    gather = Gather(w, r.g1, rows, part)
    r.mean_block[...] = r.mean[pl.ds(pl.multiple_of(w.c * rows, rows), rows)]
    r.std_block[...] = r.inverse_std[pl.ds(pl.multiple_of(w.c * rows, rows), rows)]
    r.gain_block[...] = own_gain(w, r, 1)

    def done(group):
        gather.region(w.c, w.t, group)[...] = r.grad[group * half : (group + 1) * half]
        gather.begin(group)

    norm_back(
        w,
        scatter,
        (r.g_block, r.act, r.mean_block, r.std_block, r.gain_block),
        (r.d_normed, r.row_out, r.row_in),
        rows,
        part,
        r.grad,
        r.sums,
        done,
        fill,
    )
    for _ in gather.steps():
        pull(fill)
    for _ in fill:
        pass
    slab = part // 4
    columns = pl.ds(pl.multiple_of(w.t * part + w.c * slab, 128), slab)
    r.d_b_out[...] = jnp.sum(r.g[:, columns].astype(F32), axis=0, keepdims=True)
    w.drain()


def middle(made, tables, turn, rows, part):
    tokens, width = 4 * rows, 4 * part
    full = ((tokens, width), BF16)
    inputs = {X: made[X1], ACT: made[ACT], G_BLOCK: made[G_BLOCK]}
    inputs |= {VECTORS: made[VECTORS]} | tables
    inputs |= {TURNED + name: made[TURNED + name] for name in NAMES}
    outputs = grad_shapes(width, turn.e, turn.f)
    outputs |= {"d_b_out": ((1, part // 4), F32), PARTIAL: full}
    outputs |= {GRAD: ((rows, part), BF16), G1: full, SUMS: ((8, part), F32)}
    scratch = saved_shapes(tokens, width, turn.e, turn.f)
    scratch |= {MEAN: ((tokens, 1), F32), INVERSE_STD: ((tokens, 1), F32)}
    scratch |= scratch_shapes_back(tokens, turn.e, turn.f) | {"partial_g": full, G: full}
    scratch |= {MEAN_BLOCK: ((rows, 1), F32), STD_BLOCK: ((rows, 1), F32)}
    scratch |= {GAIN_BLOCK: ((1, part), F32)}
    scratch |= weight_scratch(turn) | scatter_dict(rows, part) | back_dict(rows, part)
    return remote_call(
        functools.partial(middle_body, turn, rows, part),
        "middle",
        BWD,
        inputs,
        outputs,
        scratch,
        200,
        in_hbm=[TURNED + name for name in NAMES],
    )


LATER = (DOWN, OUT, UP, QKV)


def last_body(turn, rows, part, r):
    w = Wire(r.send_sems, r.recv_sems)
    s = w.section
    half = rows // GROUPS
    loads = {}
    for i, name in enumerate(FIRST):
        loads[name] = pltpu.make_async_copy(
            getattr(r, TURNED + name).at[0], getattr(r, W + name), r.local_sems.at[i]
        )
        loads[name].start()
    moves = [(ds, dc) for ds in (0, 1) for dc in range(4) if (ds, dc) != (0, 0)]

    def away(ds, dc):
        return {SECTION: (s + ds) % 2, CTX: (w.c + dc) % 4}

    w.greet([away(*move) for move in moves] + [w.beside, w.core, diagonal(w)])
    places = [(2, w.c_far), (1, w.c_up), (3, w.c_down), (0, w.c)]
    grads0 = {name: getattr(r, D_W + name) for name in NAMES}
    grads1 = {name: getattr(r, ONE + name) for name in NAMES}
    arrived = {name: getattr(r, ARRIVED + name) for name in NAMES}
    outs = {name: getattr(r, HOME + name) for name in NAMES}
    kept = {name: getattr(r, KEPT + name) for name in NAMES}
    across, home, keeps = {}, {}, {}

    def send_across(name):
        for step, c in places:
            across[name, step] = w.send_one_of(
                s == 0,
                turn.turned(name, grads1[name], c),
                turn.turned(name, grads0[name], c),
                turn.turned(name, arrived[name], c),
                w.across,
            )

    def keep(name, c, slot):
        copy = pltpu.make_async_copy(
            turn.turned(name, grads1[name], c), kept[name].at[slot], r.local_sems.at[8 + 2 * NAMES.index(name) + slot]
        )
        copy.start()
        return copy

    def settle():
        for name in LATER:
            waiting = keep(name, places[0][1], 0)
            for i, (step, c) in enumerate(places):
                waiting.wait()
                if i < 3:
                    waiting = keep(name, places[i + 1][1], (i + 1) % 2)
                across[name, step].wait_recv()
                theirs = turn.turned(name, arrived[name], c)
                mine = jnp.where(
                    s == 0,
                    turn.turned(name, grads0[name], c)[...].astype(F32),
                    kept[name][i % 2].astype(F32),
                )
                theirs[...] = (mine + theirs[...].astype(F32)).astype(BF16)
                spot = turn.shard(name, outs[name], w.c)
                if step:
                    home[name, step] = w.send(theirs, spot, {CTX: c})
                else:
                    home[name, 0] = pltpu.make_async_copy(
                        theirs, spot, r.local_sems.at[16 + NAMES.index(name)]
                    )
                    home[name, 0].start()
                yield

    start, open_branches, grad_rows, grad_up, attend_back, unrotate, grad_qkv, close, count = (
        backward_steps(r)
    )
    wide = 4 * part // TILE
    start()
    other = scatter_of(w, r, r.partial_x, rows, part)
    other.begin()
    summing = other.steps()
    for i in range(0, wide, 2):
        some(i, i + 2, grad_rows)
        pull(summing, times=2)
    send_across(DOWN)
    send_across(OUT)
    loads[DOWN].wait()
    loads[OUT].wait()
    for i in range(count):
        some(i, i + 1, open_branches)
        pull(summing)
    for i in range(0, wide, 2):
        some(i, i + 2, grad_up)
        pull(summing)
    send_across(UP)
    settling = settle()
    for _ in summing:
        pass
    for i in range(count):
        attend_back(i)
        pull(settling)
    bias = own_bias(w, r, 1)
    r.all_acts[0] = r.act[...]
    for group in range(GROUPS):
        own = slice(group * half, (group + 1) * half)
        value = r.act[own].astype(F32) + other.total(group) + bias
        r.all_acts[1, own] = value.astype(BF16)
    r.acts[s] = r.all_acts[s]
    pairs = [w.send(r.all_acts.at[1 - s], r.acts.at[s], w.across)]
    each(count, unrotate)
    each(wide, grad_qkv)
    send_across(QKV)
    pull(settling)
    loads[QKV].wait()
    loads[UP].wait()
    each(count, close)
    slab = part // 4
    columns = pl.ds(pl.multiple_of(w.t * part + w.c * slab, 128), slab)
    n_up = r.d_b_up.shape[1] // slab
    r.small[0, 0:3] = r.d_b_qkv[...]
    r.small[1, 0:3] = r.one_b_qkv[...]
    for i in range(n_up):
        lanes = slice(i * slab, (i + 1) * slab)
        r.small[0, 3 + i : 4 + i] = r.d_b_up[:, lanes]
        r.small[1, 3 + i : 4 + i] = r.one_b_up[:, lanes]
    r.small[0, 3 + n_up : 4 + n_up] = jnp.sum(r.g[:, columns].astype(F32), axis=0, keepdims=True)
    r.small[1, 3 + n_up : 4 + n_up] = r.one_b_out[...]
    small_copy = w.send(r.small.at[1 - s], r.small_in, w.across)
    w.flush(other.sent)
    w.meet(r.free_sem, neighbours(w))
    scatter = scatter_of(w, r, r.partial, rows, part)
    scatter.begin()
    for i, _ in enumerate(scatter.steps()):
        if i % 4 == 3:
            pull(settling)
    r.mean_block[...] = r.mean[pl.ds(pl.multiple_of(w.c * rows, rows), rows)]
    r.std_block[...] = r.inverse_std[pl.ds(pl.multiple_of(w.c * rows, rows), rows)]
    r.gain_block[...] = own_gain(w, r, 0)
    norm_back(
        w,
        scatter,
        (r.grad1, r.x_block, r.mean_block, r.std_block, r.gain_block),
        (r.d_normed, r.row_out, r.row_in),
        rows,
        part,
        r.all_grads.at[0],
        r.sums0,
        lambda group: None,
        settling,
    )
    r.all_grads[1] = r.grad1[...]
    r.grads[s] = r.all_grads[s]
    pairs.append(w.send(r.all_grads.at[1 - s], r.grads.at[s], w.across))
    for layer, sums in ((0, r.sums0), (1, r.sums1)):
        for c in range(4):
            r.norm_out[layer, c] = sums[:, c * slab : (c + 1) * slab]
    told = [
        w.send(r.norm_out.at[(s + ds) % 2, (w.c + dc) % 4], r.norm_in.at[slot], away(ds, dc))
        for slot, (ds, dc) in enumerate(moves)
    ]
    for _ in settling:
        pass
    small_copy.wait_recv()
    r.small_sum[...] = r.small[s] + r.small_in[...]
    total = r.norm_out[s, w.c]
    for slot, copy in enumerate(told):
        copy.wait_recv()
        total += r.norm_in[slot]
    r.norm_sum[...] = total
    for name in LATER:
        home[name, 0].wait()
        for step in (1, 3, 2):
            home[name, step].wait_recv()
    for copy in pairs:
        copy.wait_recv()
    w.drain()


def last(made, mid, tables, turn, rows, part):
    tokens, width = 4 * rows, 4 * part
    full = ((tokens, width), BF16)
    e, f = 4 * turn.e, 4 * turn.f
    homes = {
        QKV: (3, turn.d, e),
        OUT: (e, turn.d),
        UP: (turn.d, f),
        DOWN: (f, turn.d),
    }
    inputs = {G: mid[G1], "grad1": mid[GRAD], "partial_x": mid[PARTIAL], "sums1": mid[SUMS]}
    inputs |= {key: made[key] for key in SAVED + (MEAN, INVERSE_STD, VECTORS, ACT, X_BLOCK)}
    inputs |= {ONE + name: mid[D_W + name] for name in NAMES}
    inputs |= {ONE + name: mid["d_" + name] for name in (B_QKV, B_UP, "b_out")}
    inputs |= {TURNED + name: made[TURNED + name] for name in NAMES} | tables
    pairs = ((2, rows, part), BF16)
    outputs = {HOME + name: (homes[name], BF16) for name in NAMES}
    outputs |= {ACTS: pairs, GRADS: pairs}
    outputs |= {SMALL_SUM: ((8, part // 4), F32), NORM_SUM: ((8, part // 4), F32)}
    scratch = grad_shapes(width, turn.e, turn.f) | {PARTIAL: full}
    scratch |= {ARRIVED + name: (turn.turned_shape(name), BF16) for name in NAMES}
    scratch |= {KEPT + name: ((2,) + turn.piece_shape(name), BF16) for name in NAMES}
    scratch |= scratch_shapes_back(tokens, turn.e, turn.f)
    scratch |= {W + name: (turn.turned_shape(name), BF16) for name in NAMES}
    scratch |= scatter_dict(rows, part) | back_dict(rows, part)
    scratch |= {
        MEAN_BLOCK: ((rows, 1), F32),
        STD_BLOCK: ((rows, 1), F32),
        GAIN_BLOCK: ((1, part), F32),
        "small": ((2, 8, part // 4), F32),
        "small_in": ((8, part // 4), F32),
        "sums0": ((8, part), F32),
        "norm_out": ((2, 4, 8, part // 4), F32),
        "norm_in": ((7, 8, part // 4), F32),
        "all_acts": pairs,
        "all_grads": pairs,
    }
    return remote_call(
        functools.partial(last_body, turn, rows, part),
        "last",
        LAST,
        inputs,
        outputs,
        scratch,
        140,
        in_hbm=[TURNED + name for name in NAMES] + [ONE + name for name in NAMES],
        out_hbm=[HOME + name for name in NAMES],
    )


def shards(
    boundary,
    doc_ids,
    qkv_weight,
    qkv_bias,
    out_weight,
    out_bias,
    fc1_weight,
    fc1_bias,
    fc2_weight,
    fc2_bias,
    norm_gain,
    norm_shift,
):
    section = lax.axis_index(SECTION)
    rows, part = boundary.shape[2:]
    slab = out_bias.shape[1]
    n_up = fc1_bias.shape[1] // slab
    tables = doc_tables(
        lax.dynamic_index_in_dim(doc_ids, section, 0, keepdims=False), slab // HD
    )
    vector = jnp.concatenate(
        [
            out_bias.astype(F32) + fc2_bias.astype(F32),
            norm_gain.astype(F32),
            norm_shift.astype(F32),
            qkv_bias[0].astype(F32),
            fc1_bias.astype(F32).reshape(n_up, slab),
        ]
    )
    vector = jnp.pad(vector, ((0, 16 - vector.shape[0]), (0, 0)))
    shard_of = {QKV: qkv_weight[0], OUT: out_weight[0], UP: fc1_weight[0], DOWN: fc2_weight[0]}
    turn = Turn(shard_of[QKV].shape[1], slab, shard_of[UP].shape[1] // 4)
    made = first(boundary[0], vector, tables, shard_of)
    mid = middle(made, tables, turn, rows, part)
    out = last(made, mid, tables, turn, rows, part)
    small, norms = out[SMALL_SUM], out[NORM_SUM]
    bias_out = small[3 + n_up][None]
    home = {name: out[HOME + name].astype(F32)[None] for name in NAMES}
    return (
        out[ACTS][None],
        out[GRADS][None],
        home[QKV],
        small[None, :3],
        home[OUT],
        bias_out,
        home[UP],
        small[3 : 3 + n_up].reshape(1, -1),
        home[DOWN],
        bias_out,
        norms[0:1],
        norms[1:2],
    )


def from_behind(value, axis, steps):
    count = lax.axis_size(axis)
    leading, last = (max(0, -steps), min(count, count - steps))
    return lax.ppermute(value, axis, [(source, source + steps) for source in range(leading, last)])


def gelu(value):
    inner = jnp.tanh(GELU_C * (value + GELU_K * value * value * value))
    return 0.5 * value * (1.0 + inner)


def gelu_slope(value):
    inner = jnp.tanh(GELU_C * (value + GELU_K * value * value * value))
    return 0.5 * (1.0 + inner) + 0.5 * value * (1.0 - inner * inner) * GELU_C * (
        1.0 + 3.0 * GELU_K * value * value
    )


def local_layout(ids_full, ctx_index, tokens):
    length = ids_full.shape[0]
    local_ids = lax.dynamic_slice_in_dim(ids_full, ctx_index * tokens, tokens)
    start = jnp.sum((ids_full[None, :] < local_ids[:, None]).astype(jnp.int32), axis=1)
    query_at = ctx_index * tokens + jnp.arange(tokens, dtype=jnp.int32)
    key_at = jnp.arange(length, dtype=jnp.int32)
    allowed = (key_at[None, :] <= query_at[:, None]) & (ids_full[None, :] == local_ids[:, None])
    return (query_at - start, allowed)


def score_block(query, keys):
    return jnp.einsum(SCORES_EQ, query, keys, preferred_element_type=jnp.float32) * HD ** (
        -0.5
    )


def forward_layer(layer_in, ids_full, params, ctx_index):
    w_qkv, b_qkv, w_out, b_out, w_up, b_up, w_down, b_down, gain, shift = params
    tokens = layer_in.shape[0]
    heads = w_qkv.shape[2] // HD
    wide_in = layer_in.astype(jnp.float32)
    row_sums = lax.psum((jnp.sum(wide_in, axis=1), jnp.sum(wide_in * wide_in, axis=1)), TP)
    row_mean = row_sums[0] / D
    variance = row_sums[1] / D - row_mean * row_mean
    inverse_std = lax.rsqrt(variance + EPS)
    centered = (wide_in - row_mean[:, None]) * inverse_std[:, None]
    normed_part = (centered * gain.astype(jnp.float32) + shift.astype(jnp.float32)).astype(
        jnp.bfloat16
    )
    normed = lax.all_gather(normed_part, TP, axis=1, tiled=True)
    positions, allowed = local_layout(ids_full, ctx_index, tokens)
    cosine, sine = rope_tables(positions)
    projected = (
        jnp.einsum("td,cde->cte", normed, w_qkv, preferred_element_type=jnp.float32)
        + b_qkv.astype(jnp.float32)[:, None, :]
    )
    query = rotate(projected[0].reshape(tokens, heads, HD), cosine, sine, 1.0).astype(jnp.bfloat16)
    key_rot = rotate(projected[1].reshape(tokens, heads, HD), cosine, sine, 1.0).astype(
        jnp.bfloat16
    )
    value_part = projected[2].reshape(tokens, heads, HD).astype(jnp.bfloat16)
    key_all, value_all = (
        lax.all_gather(key_rot, CTX, axis=0, tiled=True),
        lax.all_gather(value_part, CTX, axis=0, tiled=True),
    )
    scores = score_block(query, key_all)
    totals = jnp.sum(jnp.where(allowed[None], jnp.exp(scores), 0.0), axis=2)
    log_total = jnp.log(totals)
    probs = jnp.where(allowed[None], jnp.exp(scores - log_total[:, :, None]), 0.0).astype(
        jnp.bfloat16
    )
    attended = (
        jnp.einsum(HEADS_EQ, probs, value_all, preferred_element_type=jnp.float32)
        .astype(jnp.bfloat16)
        .reshape(tokens, heads * HD)
    )
    hidden_pre = jnp.dot(normed, w_up, preferred_element_type=jnp.float32) + b_up.astype(
        jnp.float32
    )
    hidden = gelu(hidden_pre).astype(jnp.bfloat16)
    summands = jnp.dot(attended, w_out, preferred_element_type=jnp.float32) + jnp.dot(
        hidden, w_down, preferred_element_type=jnp.float32
    )
    mixed = lax.psum_scatter(summands, TP, scatter_dimension=1, tiled=True)
    layer_out = (wide_in + mixed + b_out.astype(jnp.float32) + b_down.astype(jnp.float32)).astype(
        jnp.bfloat16
    )
    kept = (key_rot, value_part)
    return (
        layer_out,
        (centered, inverse_std, normed, query, kept, attended, log_total, hidden_pre, hidden),
    )


def backward_layer(incoming, saved, ids_full, params, ctx_index):
    w_qkv, b_qkv, w_out, b_out, w_up, b_up, w_down, b_down, gain, shift = params
    centered, inverse_std, normed, query, kept, attended, log_total, hidden_pre, hidden = saved
    tokens = query.shape[0]
    heads = query.shape[1]
    wide_grad = incoming.astype(jnp.float32)
    grad_rows = lax.all_gather(incoming, TP, axis=1, tiled=True)
    grad_out_bias = jnp.sum(wide_grad, axis=0)
    grad_out = jnp.einsum("tk,te->ke", attended, grad_rows, preferred_element_type=jnp.float32)
    d_attended = jnp.einsum(
        "te,ke->tk", grad_rows, w_out, preferred_element_type=jnp.float32
    ).astype(jnp.bfloat16)
    grad_down = jnp.einsum("tf,te->fe", hidden, grad_rows, preferred_element_type=jnp.float32)
    d_pre = jnp.einsum(
        "te,fe->tf", grad_rows, w_down, preferred_element_type=jnp.float32
    ) * gelu_slope(hidden_pre)
    grad_up_bias = jnp.sum(d_pre, axis=0)
    d_hidden = d_pre.astype(jnp.bfloat16)
    grad_up = jnp.einsum("td,tf->df", normed, d_hidden, preferred_element_type=jnp.float32)
    key_all, value_all = (
        lax.all_gather(kept[0], CTX, axis=0, tiled=True),
        lax.all_gather(kept[1], CTX, axis=0, tiled=True),
    )
    positions, allowed = local_layout(ids_full, ctx_index, tokens)
    cosine, sine = rope_tables(positions)
    d_heads = d_attended.reshape(tokens, heads, HD)
    out_heads = attended.reshape(tokens, heads, HD)
    delta = jnp.sum(d_heads.astype(jnp.float32) * out_heads.astype(jnp.float32), axis=2)
    scores = score_block(query, key_all)
    probs = jnp.where(allowed[None], jnp.exp(scores - log_total[:, :, None]), 0.0)
    d_probs = jnp.einsum(SCORES_EQ, d_heads, value_all, preferred_element_type=jnp.float32)
    d_scores = (probs * (d_probs - delta.T[:, :, None]) * HD ** (-0.5)).astype(jnp.bfloat16)
    d_query = jnp.einsum(HEADS_EQ, d_scores, key_all, preferred_element_type=jnp.float32)
    key_terms = jnp.einsum(KEYS_EQ, d_scores, query, preferred_element_type=jnp.float32)
    value_terms = jnp.einsum(
        KEYS_EQ, probs.astype(jnp.bfloat16), d_heads, preferred_element_type=jnp.float32
    )
    d_key, d_value = (
        lax.psum_scatter(
            key_terms.astype(jnp.bfloat16), CTX, scatter_dimension=0, tiled=True
        ).astype(jnp.float32),
        lax.psum_scatter(
            value_terms.astype(jnp.bfloat16), CTX, scatter_dimension=0, tiled=True
        ).astype(jnp.float32),
    )
    d_projected = jnp.stack(
        [rotate(d_query, cosine, sine, -1.0), rotate(d_key, cosine, sine, -1.0), d_value]
    ).reshape(3, tokens, heads * HD)
    grad_qkv_bias = jnp.sum(d_projected, axis=1)
    d_qkv = d_projected.astype(jnp.bfloat16)
    grad_qkv = jnp.einsum("td,cte->cde", normed, d_qkv, preferred_element_type=jnp.float32)
    normed_terms = jnp.einsum("cte,cde->td", d_qkv, w_qkv, preferred_element_type=jnp.float32)
    normed_terms = normed_terms + jnp.einsum(
        "tf,df->td", d_hidden, w_up, preferred_element_type=jnp.float32
    )
    d_normed = lax.psum_scatter(
        normed_terms.astype(jnp.bfloat16), TP, scatter_dimension=1, tiled=True
    ).astype(jnp.float32)
    grad_gain = jnp.sum(d_normed * centered, axis=0)
    grad_shift = jnp.sum(d_normed, axis=0)
    scaled = d_normed * gain.astype(jnp.float32)
    row_terms = lax.psum((jnp.sum(scaled, axis=1), jnp.sum(scaled * centered, axis=1)), TP)
    grad_in = wide_grad + inverse_std[:, None] * (
        scaled - row_terms[0][:, None] / D - centered * (row_terms[1][:, None] / D)
    )
    grads = (
        grad_qkv,
        grad_qkv_bias,
        grad_out,
        grad_out_bias,
        grad_up,
        grad_up_bias,
        grad_down,
        grad_out_bias,
        grad_gain,
        grad_shift,
    )
    return (grad_in.astype(jnp.bfloat16), grads)


def base_shards(
    boundary,
    doc_ids,
    qkv_weight,
    qkv_bias,
    out_weight,
    out_bias,
    fc1_weight,
    fc1_bias,
    fc2_weight,
    fc2_bias,
    norm_gain,
    norm_shift,
):
    section = lax.axis_index(SECTION)
    ctx_index = lax.axis_index(CTX)
    micro = boundary.shape[1]
    tokens = boundary.shape[2]
    width_part = boundary.shape[3]
    params = (
        lax.all_gather(qkv_weight[0], CTX, axis=1, tiled=True),
        lax.all_gather(qkv_bias[0], CTX, axis=1, tiled=True),
        lax.all_gather(out_weight[0], CTX, axis=1, tiled=True),
        lax.all_gather(out_bias[0], CTX, axis=0, tiled=True),
        lax.all_gather(fc1_weight[0], CTX, axis=0, tiled=True),
        lax.all_gather(fc1_bias[0], CTX, axis=0, tiled=True),
        lax.all_gather(fc2_weight[0], CTX, axis=1, tiled=True),
        lax.all_gather(fc2_bias[0], CTX, axis=0, tiled=True),
        lax.all_gather(norm_gain[0], CTX, axis=0, tiled=True),
        lax.all_gather(norm_shift[0], CTX, axis=0, tiled=True),
    )
    inputs = boundary[0]
    ticks = jnp.arange(micro + 1, dtype=jnp.int32)

    def forward_tick(received, tick):
        index = jnp.clip(tick - section, 0, micro - 1)
        first = lax.dynamic_index_in_dim(inputs, index, 0, keepdims=False)
        layer_in = jnp.where(section == 0, first, received)
        ids_full = lax.dynamic_index_in_dim(doc_ids, index, 0, keepdims=False)
        layer_out, saved = forward_layer(layer_in, ids_full, params, ctx_index)
        passed = from_behind(layer_out, SECTION, 1)
        return (passed, (layer_out, saved))

    start_zero = jnp.zeros((tokens, width_part), jnp.bfloat16)
    leftover, (outs_all, saved_all) = lax.scan(forward_tick, start_zero, ticks)
    held = lax.optimization_barrier(
        (
            (
                qkv_weight[0],
                qkv_bias[0],
                out_weight[0],
                out_bias[0],
                fc1_weight[0],
                fc1_bias[0],
                fc2_weight[0],
                fc2_bias[0],
                norm_gain[0],
                norm_shift[0],
            ),
            outs_all,
        )
    )[0]
    back_params = (
        lax.all_gather(held[0], CTX, axis=1, tiled=True),
        lax.all_gather(held[1], CTX, axis=1, tiled=True),
        lax.all_gather(held[2], CTX, axis=1, tiled=True),
        lax.all_gather(held[3], CTX, axis=0, tiled=True),
        lax.all_gather(held[4], CTX, axis=0, tiled=True),
        lax.all_gather(held[5], CTX, axis=0, tiled=True),
        lax.all_gather(held[6], CTX, axis=1, tiled=True),
        lax.all_gather(held[7], CTX, axis=0, tiled=True),
        lax.all_gather(held[8], CTX, axis=0, tiled=True),
        lax.all_gather(held[9], CTX, axis=0, tiled=True),
    )
    zero_grads = tuple((jnp.zeros(weight.shape, jnp.float32) for weight in params))

    def backward_tick(carry, tick):
        received, totals = carry
        raw_index = tick - (1 - section)
        valid = (raw_index >= 0) & (raw_index < micro)
        index = jnp.clip(raw_index, 0, micro - 1)
        cotangent = lax.dynamic_index_in_dim(inputs, index, 0, keepdims=False)
        incoming = jnp.where(section == 1, cotangent, received)
        incoming = jnp.where(valid, incoming, jnp.zeros_like(incoming))
        position_slot = index + section
        saved = jax.tree.map(
            lambda stacked: lax.dynamic_index_in_dim(stacked, position_slot, 0, keepdims=False),
            saved_all,
        )
        ids_full = lax.dynamic_index_in_dim(doc_ids, index, 0, keepdims=False)
        grad_in, terms = backward_layer(incoming, saved, ids_full, back_params, ctx_index)
        totals = tuple((total + term for total, term in zip(totals, terms)))
        passed = from_behind(grad_in, SECTION, -1)
        return ((passed, totals), grad_in)

    (leftover_grad, totals), grads_all = lax.scan(backward_tick, (start_zero, zero_grads), ticks)
    acts = lax.dynamic_slice_in_dim(outs_all, section, micro, 0)[None]
    input_grads = lax.dynamic_slice_in_dim(grads_all, 1 - section, micro, 0)[None]
    shares = (
        lax.psum_scatter(
            totals[0].astype(jnp.bfloat16), CTX, scatter_dimension=1, tiled=True
        ).astype(jnp.float32),
        lax.psum_scatter(
            totals[1].astype(jnp.bfloat16), CTX, scatter_dimension=1, tiled=True
        ).astype(jnp.float32),
        lax.psum_scatter(
            totals[2].astype(jnp.bfloat16), CTX, scatter_dimension=1, tiled=True
        ).astype(jnp.float32),
        lax.psum_scatter(
            totals[3].astype(jnp.bfloat16), CTX, scatter_dimension=0, tiled=True
        ).astype(jnp.float32),
        lax.psum_scatter(
            totals[4].astype(jnp.bfloat16), CTX, scatter_dimension=0, tiled=True
        ).astype(jnp.float32),
        lax.psum_scatter(
            totals[5].astype(jnp.bfloat16), CTX, scatter_dimension=0, tiled=True
        ).astype(jnp.float32),
        lax.psum_scatter(
            totals[6].astype(jnp.bfloat16), CTX, scatter_dimension=1, tiled=True
        ).astype(jnp.float32),
        lax.psum_scatter(
            totals[7].astype(jnp.bfloat16), CTX, scatter_dimension=0, tiled=True
        ).astype(jnp.float32),
        lax.psum_scatter(
            totals[8].astype(jnp.bfloat16), CTX, scatter_dimension=0, tiled=True
        ).astype(jnp.float32),
        lax.psum_scatter(
            totals[9].astype(jnp.bfloat16), CTX, scatter_dimension=0, tiled=True
        ).astype(jnp.float32),
    )
    return (
        acts,
        input_grads,
        shares[0][None],
        shares[1][None],
        shares[2][None],
        shares[3][None],
        shares[4][None],
        shares[5][None],
        shares[6][None],
        shares[7][None],
        shares[8][None],
        shares[9][None],
    )


def solution(mesh):
    specs = {
        TOKEN: P(SECTION, None, CTX, TP),
        ROWS: P(SECTION, TP, CTX),
        COLUMNS: P(SECTION, CTX, TP),
        VECTOR: P(SECTION, (TP, CTX)),
        VECTORS: P(SECTION, None, (TP, CTX)),
    }
    weights = (TOKEN, VECTORS, ROWS, VECTOR, COLUMNS, VECTOR, ROWS, VECTOR, VECTOR, VECTOR)
    placed = tuple(specs[name] for name in weights)
    heads = D // HD
    place = {SECTION: 2, CTX: 4, TP: 4}
    whole_heads = heads % (mesh.shape[TP] * mesh.shape[CTX]) == 0
    return jax.shard_map(
        shards if whole_heads and dict(mesh.shape) == place else base_shards,
        mesh=mesh,
        in_specs=(specs[TOKEN], P(), *placed),
        out_specs=(specs[TOKEN], specs[TOKEN], *placed),
        check_vma=False,
    )
```

```python
import functools
import itertools

import jax
import jax.numpy as jnp
from jax import lax
from jax.experimental import pallas as pl
from jax.experimental.pallas import tpu as pltpu
from jax.sharding import PartitionSpec as P

D = 2048
HD = 64
ROT = 32
EPS = 1e-05
GELU_C = 0.7978845608028654
GELU_K = 0.044715
ACT = "act"
ACT1 = "act1"
ACTS = "acts"
ARRIVED = "arrived_"
ATT = "att"
BOUNCE = "bounce_"
B_QKV = "b_qkv"
B_UP = "b_up"
COLUMNS = "columns"
CORES = "cores"
COSINE = "cosine"
CTX = "ctx"
DOWN = "down"
D_W = "d_w_"
D_W_DOWN = "d_w_down"
D_W_OUT = "d_w_out"
D_W_QKV = "d_w_qkv"
D_W_UP = "d_w_up"
G = "g"
G1 = "g1"
GAIN = "gain"
GAIN_BLOCK = "gain_block"
GRAD = "grad"
GRADS = "grads"
G_BLOCK = "g_block"
HBM = "hbm_"
HEADS_EQ = "hts,shd->thd"
HIDDEN = "hidden"
HOME = "home_"
INVERSE_STD = "inverse_std"
KEPT = "kept_"
KEYS_EQ = "hts,thd->shd"
LSE = "lse"
MEAN = "mean"
MEAN_BLOCK = "mean_block"
NORMED = "normed"
NORM_SUM = "norm_sum"
N_START = "start"
ONE = "one_"
OUT = "out"
PARTIAL = "partial"
QKV = "qkv"
ROWS = "rows"
SCORES_EQ = "thd,shd->hts"
SECTION = "section"
SHARD = "shard_"
SHIFT = "shift"
SINE = "sine"
SLOPE = "slope"
SMALL_SUM = "small_sum"
STD_BLOCK = "std_block"
SUMS = "sums"
TOKEN = "token"
TP = "tp"
TURNED = "turned_"
UP = "up"
VECTOR = "vector"
VECTORS = "vectors"
W = "w_"
X1 = "x1"
X_BLOCK = "x_block"
BF16 = jnp.bfloat16
F32 = jnp.float32


def rope_tables(positions):
    half = ROT // 2
    freq = 10000.0 ** (-(jnp.arange(half).astype(F32) * 2.0 / ROT))
    angle = positions.astype(F32)[:, None] * freq[None, :]
    return (jnp.cos(angle), jnp.sin(angle))


def rotate(field, cosine, sine, sign):
    half = ROT // 2
    first = field[..., :half]
    second = field[..., half:ROT]
    cosine = cosine[:, None, :]
    sine = sine[:, None, :] * sign
    return jnp.concatenate(
        [first * cosine - second * sine, second * cosine + first * sine, field[..., ROT:]], axis=-1
    )


def doc_tables(ids, heads):
    length = ids.shape[0]
    start = jnp.sum((ids[None, :] < ids[:, None]).astype(jnp.int32), axis=1)
    cosine, sine = rope_tables(jnp.arange(length, dtype=jnp.int32) - start)
    still = jnp.ones((length, HD - ROT), F32)
    cosine = jnp.tile(jnp.concatenate([cosine, cosine, still], axis=1), (1, heads))
    sine = jnp.tile(jnp.concatenate([-sine, sine, 0.0 * still], axis=1), (1, heads))
    return {N_START: start[:, None], COSINE: cosine, SINE: sine}


MESH = pl.DeviceIdType.MESH
FWD, BWD, LAST, START = 0, 1, 2, 3
GROUPS = 2


class Wire:
    def __init__(self, send_sems, recv_sems):
        self.send_sems, self.recv_sems = send_sems, recv_sems
        self.copies = []
        self.section = lax.axis_index(SECTION)
        self.c = lax.axis_index(CTX)
        self.t = lax.axis_index(TP)
        self.y = self.t // 2
        self.k = self.t % 2
        self.c_up = (self.c + 1) % 4
        self.c_far = (self.c + 2) % 4
        self.c_down = (self.c + 3) % 4
        self.t_y = (self.t + 2) % 4
        self.t_core = self.t + 1 - 2 * self.k
        self.up = {CTX: jnp.minimum(self.c + 1, 3)}
        self.down = {CTX: jnp.maximum(self.c - 1, 0)}
        self.beside = {TP: self.t_y}
        self.core = {TP: self.t_core}
        self.across = {SECTION: 1 - self.section}
        self.others = [(2, self.c_far), (1, self.c_up), (3, self.c_down)]

    def greet(self, targets):
        barrier = pltpu.get_barrier_semaphore()
        for target in targets:
            pl.semaphore_signal(barrier, inc=1, device_id=target, device_id_type=MESH)
        pl.semaphore_wait(barrier, len(targets))

    def send(self, source, target, device, when=None):
        index = len(self.copies)
        copy = pltpu.make_async_remote_copy(
            src_ref=source,
            dst_ref=target,
            send_sem=self.send_sems.at[index],
            recv_sem=self.recv_sems.at[index],
            device_id=device,
            device_id_type=MESH,
        )
        if when is None:
            copy.start()
        else:
            pl.when(when)(copy.start)
        self.copies.append((copy, when))
        return copy

    def pick(self, *values):
        chosen = values[3]
        for c in (2, 1, 0):
            chosen = jnp.where(self.c == c, values[c], chosen)
        return chosen

    def step_copy(self, base, step, source, target):
        return pltpu.make_async_remote_copy(
            src_ref=source,
            dst_ref=target,
            send_sem=self.send_sems.at[base + step - 1],
            recv_sem=self.recv_sems.at[base + step - 1],
            device_id={CTX: (self.c + step) % 4},
            device_id_type=MESH,
        )

    def send_one_of(self, first, source, other_source, target, device):
        index = len(self.copies)
        copies = [
            pltpu.make_async_remote_copy(
                src_ref=ref,
                dst_ref=target,
                send_sem=self.send_sems.at[index],
                recv_sem=self.recv_sems.at[index],
                device_id=device,
                device_id_type=MESH,
            )
            for ref in (source, other_source)
        ]
        pl.when(first)(copies[0].start)
        pl.when(jnp.logical_not(first))(copies[1].start)
        self.copies.append((copies[0], None))
        return copies[0]

    def flush(self, indices):
        for index in indices:
            if self.copies[index] is not None:
                copy, when = self.copies[index]
                self.copies[index] = None
                if when is None:
                    copy.wait_send()
                else:
                    pl.when(when)(copy.wait_send)

    def drain(self):
        self.flush(range(len(self.copies)))

    def meet(self, semaphore, peers):
        for peer in peers:
            pl.semaphore_signal(semaphore, inc=1, device_id=peer, device_id_type=MESH)
        pl.semaphore_wait(semaphore, len(peers))


class Gather:
    def __init__(self, wire, full, rows, part, skew=1):
        self.w, self.full, self.rows, self.part = wire, full, rows, part
        self.size, self.skew = rows // GROUPS, skew
        self.hops, self.beside = {}, {}

    def region(self, c, t, group):
        return self.full.at[
            pl.ds(pl.multiple_of(c * self.rows + group * self.size, 16), self.size),
            pl.ds(pl.multiple_of(t * self.part, 128), self.part),
        ]

    def pass_on(self, device, c, t, group, when=None):
        spot = self.region(c, t, group)
        return self.w.send(spot, spot, device, when)

    def begin(self, group):
        w = self.w
        self.hops[group, 1] = self.pass_on(w.up, w.c, w.t, group, w.c < 3)
        self.hops[group, -1] = self.pass_on(w.down, w.c, w.t, group, w.c > 0)
        self.beside[group, 0] = self.pass_on(w.beside, w.c, w.t, group)
        self.cores = getattr(self, CORES, [])
        self.cores.append((self.pass_on(w.core, w.c, w.t, group), None))

    def steps(self):
        return itertools.chain(self.along(), self.around())

    def hop_order(self):
        events = [
            (group, sign * hop) for group in range(GROUPS) for hop in (1, 2, 3) for sign in (1, -1)
        ]
        return sorted(events, key=lambda event: (self.skew * event[0] + abs(event[1]), event[0]))

    def along(self):
        w = self.w
        for group, hop in self.hop_order():
            source = jnp.clip(w.c - hop, 0, 3)
            there = w.c >= hop if hop > 0 else w.c - hop <= 3
            pl.when(there)(self.hops[group, hop].wait_recv)
            if abs(hop) < 3:
                further = hop + (1 if hop > 0 else -1)
                ahead = w.c < 3 if hop > 0 else w.c > 0
                self.hops[group, further] = self.pass_on(
                    w.up if hop > 0 else w.down, source, w.t, group, jnp.logical_and(there, ahead)
                )
            self.beside[group, hop] = self.pass_on(w.beside, source, w.t, group, there)
            self.cores.append((self.pass_on(w.core, source, w.t, group, there), there))
            yield

    def around(self):
        w = self.w
        for group, hop in [(group, 0) for group in range(GROUPS)] + self.hop_order():
            source = jnp.clip(w.c - hop, 0, 3)
            there = None if hop == 0 else w.c >= hop if hop > 0 else w.c - hop <= 3
            copy = self.beside[group, hop]
            copy.wait_recv() if there is None else pl.when(there)(copy.wait_recv)
            self.cores.append((self.pass_on(w.core, source, w.t_y, group, there), there))
            yield
        for copy, there in self.cores:
            copy.wait_recv() if there is None else pl.when(there)(copy.wait_recv)


class DirectGather(Gather):
    def begin(self, group):
        w = self.w
        for step, place in w.others:
            self.hops[group, step] = self.pass_on({CTX: place}, w.c, w.t, group)
        self.beside[group, 0] = self.pass_on(w.beside, w.c, w.t, group)
        self.cores = getattr(self, CORES, [])
        self.cores.append((self.pass_on(w.core, w.c, w.t, group), None))

    def steps(self):
        w = self.w
        order = [(group, step) for group in range(GROUPS) for step in (1, 3, 2)]
        for group, step in order:
            source = (w.c + 4 - step) % 4
            self.hops[group, step].wait_recv()
            self.beside[group, step] = self.pass_on(w.beside, source, w.t, group)
            self.cores.append((self.pass_on(w.core, source, w.t, group), None))
            yield
        for group, step in [(group, 0) for group in range(GROUPS)] + order:
            self.beside[group, step].wait_recv()
            source = (w.c + 4 - step) % 4
            self.cores.append((self.pass_on(w.core, source, w.t_y, group), None))
            yield
        for copy, _ in self.cores:
            copy.wait_recv()


def scatter_scratch(rows, part):
    return [
        pltpu.VMEM((2, 4 * rows, part), BF16),
        pltpu.VMEM((2, 4 * rows, part), BF16),
        pltpu.VMEM((4 * rows, part), BF16),
        pltpu.VMEM((3, rows, part), BF16),
    ]


class Scatter:
    def __init__(self, wire, partial, scratch, rows, part):
        self.w, self.partial, self.rows, self.part = wire, partial, rows, part
        self.theirs, self.chip, self.from_y, self.from_far = scratch
        w = wire
        self.places = [(2, w.c_far), (1, w.c_up), (3, w.c_down), (0, w.c)]
        self.order = [
            (group, c, y)
            for group in (0, 1)
            for y in (1 - w.y, w.y)
            for _, c in self.places
        ]
        self.far, self.sent = {}, []

    def send(self, source, target, device):
        self.sent.append(len(self.w.copies))
        return self.w.send(source, target, device)

    def span(self, group, c):
        size = self.rows // 2
        return pl.ds(pl.multiple_of(c * self.rows + group * size, 16), size)

    def begin(self, compute):
        w = self.w
        self.cores = [None] * len(self.order)
        for _, place in self.places:
            compute(place)
            for index, (group, c, y) in enumerate(self.order):
                if c is place:
                    columns = pl.ds(pl.multiple_of((2 * y + 1 - w.k) * self.part, 128), self.part)
                    self.cores[index] = self.send(
                        self.partial.at[self.span(group, c), columns],
                        self.theirs.at[y, self.span(group, c)],
                        w.core,
                    )

    def take(self, index):
        group, c, y = self.order[index]
        self.cores[index].wait_recv()
        rows = self.span(group, c)
        columns = pl.ds(pl.multiple_of((2 * y + self.w.k) * self.part, 128), self.part)
        return self.partial[rows, columns].astype(F32) + self.theirs[y, rows].astype(F32)

    def run(self):
        for _ in self.steps():
            pass

    def steps(self):
        w = self.w
        half = self.rows // 2
        beside = {}
        for group in (0, 1):
            for slot, (_, c) in enumerate(self.places):
                rows = self.span(group, c)
                self.chip[1 - w.y, rows] = self.take(8 * group + slot).astype(BF16)
                beside[group, slot] = self.send(
                    self.chip.at[1 - w.y, rows], self.from_y.at[rows], w.beside
                )
                yield
        for group in (0, 1):
            for slot, (step, c) in enumerate(self.places):
                rows = self.span(group, c)
                value = self.take(8 * group + 4 + slot)
                beside[group, slot].wait_recv()
                self.chip[w.y, rows] = (value + self.from_y[rows].astype(F32)).astype(BF16)
                if step:
                    self.far[group, step] = self.send(
                        self.chip.at[w.y, rows],
                        self.from_far.at[step - 1, pl.ds(group * half, half)],
                        {CTX: c},
                    )
                yield

    def total(self, group):
        half = self.rows // 2
        value = self.chip[self.w.y, self.span(group, self.w.c)].astype(F32)
        for step in (1, 3, 2):
            self.far[group, step].wait_recv()
            value += self.from_far[step - 1, pl.ds(group * half, half)].astype(F32)
        return value


def neighbours(w):
    return [{CTX: place} for _, place in w.others] + [w.beside, w.core]


def diagonal(w):
    return {TP: (w.t_core + 2) % 4}


def back_scratch(rows, part):
    return [
        pltpu.VMEM((rows, part), F32),
        pltpu.VMEM((GROUPS, 8, 128), F32),
        pltpu.VMEM((GROUPS, 3, 8, 128), F32),
    ]


def norm_back(w, scatter, blocks, scratch, rows, part, grad, sums, done, fill=iter(())):
    g_block, x_block, mean, inverse_std, gain = blocks
    d_normed, row_out, row_in = scratch
    half = rows // GROUPS
    width = 4 * part
    lane = lax.broadcasted_iota(jnp.int32, (128, 128), 1)
    sent = []
    gain_sum = jnp.zeros((1, part), F32)
    shift_sum = jnp.zeros((1, part), F32)
    for group in range(GROUPS):
        own = slice(group * half, (group + 1) * half)
        value = scatter.total(group)
        for _ in range(2):
            next(fill, None)
        d_normed[own] = value
        centered = (x_block[own].astype(F32) - mean[own]) * inverse_std[own]
        weighted = value * centered
        gain_sum += jnp.sum(weighted, axis=0, keepdims=True)
        shift_sum += jnp.sum(value, axis=0, keepdims=True)
        first = jnp.sum(value * gain[...], axis=1, keepdims=True)
        second = jnp.sum(weighted * gain[...], axis=1, keepdims=True)
        packed = jnp.where(lane == 0, first, jnp.where(lane == 1, second, 0.0))
        row_out[group] = packed.T[:8]
        sent.append(
            [
                w.send(row_out.at[group], row_in.at[group, slot], peer)
                for slot, peer in enumerate((w.beside, w.core, diagonal(w)))
            ]
        )
    sums[...] = jnp.concatenate(
        [gain_sum, shift_sum, jnp.zeros((6, part), F32)], axis=0
    )
    for group in range(GROUPS):
        own = slice(group * half, (group + 1) * half)
        next(fill, None)
        for copy in sent[group]:
            copy.wait_recv()
        rows_sum = row_out[group] + row_in[group, 0] + row_in[group, 1] + row_in[group, 2]
        columns = jnp.concatenate([rows_sum, jnp.zeros((half - 8, 128), F32)], axis=0).T
        centered = (x_block[own].astype(F32) - mean[own]) * inverse_std[own]
        scaled = d_normed[own] * gain[...]
        value = g_block[own].astype(F32) + inverse_std[own] * (
            scaled - columns[:, 0:1] / width - centered * (columns[:, 1:2] / width)
        )
        grad[own] = value.astype(BF16)
        done(group)


class Turn:
    def __init__(self, d_part, e_part, f_part):
        self.d, self.e, self.f = d_part, e_part, f_part

    def rows(self, name):
        return {QKV: self.d, OUT: self.e, UP: self.d, DOWN: self.f}[name]

    def inner(self, name, half):
        size = self.rows(name)
        return (0, size) if half is None else (half * size // 2, size // 2)

    def shard(self, name, ref, c, half=None):
        start, size = self.inner(name, half)
        if name == QKV:
            return ref.at[:, pl.ds(start, size), pl.ds(pl.multiple_of(c * self.e, 128), self.e)]
        if name == UP:
            return ref.at[pl.ds(start, size), pl.ds(pl.multiple_of(c * self.f, 128), self.f)]
        stride = self.e if name == OUT else self.f
        return ref.at[pl.ds(pl.multiple_of(c * stride + start, 16), size)]

    def turned(self, name, ref, c, half=None):
        start, size = self.inner(name, half)
        if name == QKV:
            return ref.at[:, pl.ds(pl.multiple_of(c * self.d + start, 16), size)]
        if name == UP:
            return ref.at[pl.ds(pl.multiple_of(c * self.d + start, 16), size)]
        return ref.at[pl.ds(start, size), pl.ds(pl.multiple_of(c * self.d, 128), self.d)]

    def piece_shape(self, name, halved=False):
        size = self.rows(name) // (2 if halved else 1)
        return {
            QKV: (3, size, self.e),
            OUT: (size, self.d),
            UP: (size, self.f),
            DOWN: (size, self.d),
        }[name]

    def turned_shape(self, name):
        return {
            QKV: (3, 4 * self.d, self.e),
            OUT: (self.e, 4 * self.d),
            UP: (4 * self.d, self.f),
            DOWN: (self.f, 4 * self.d),
        }[name]


NAMES = (QKV, OUT, UP, DOWN)


def everyone(w):
    return [
        {SECTION: (w.section + ds) % 2, CTX: (w.c + dc) % 4, TP: (w.t + dt) % 4}
        for ds in range(2)
        for dc in range(4)
        for dt in range(4)
        if (ds, dc, dt) != (0, 0, 0)
    ]


TILE = 256


def dot(a, b, contract=((1,), (0,))):
    return lax.dot_general(a, b, (contract, ((), ())), preferred_element_type=F32)


def tile(i, size=TILE):
    return pl.ds(pl.multiple_of(i * size, size), size)


def turn_heads(value, cosine, sine, sign):
    half = ROT // 2
    width = value.shape[1]
    lane = lax.broadcasted_iota(jnp.int32, value.shape, 1) % HD
    partner = jnp.where(
        lane < half, pltpu.roll(value, width - half, 1), pltpu.roll(value, half, 1)
    )
    return value * cosine + partner * (sine * sign)


def head_mask(shape, head):
    lane = lax.broadcasted_iota(jnp.int32, shape, 1)
    return jnp.logical_and(lane >= head * HD, lane < (head + 1) * HD)


def of_head(value, head):
    return jnp.where(head_mask(value.shape, head), value, jnp.zeros_like(value))


def allowed_keys(start, first_row, shape):
    row = lax.broadcasted_iota(jnp.int32, shape, 0) + first_row
    column = lax.broadcasted_iota(jnp.int32, shape, 1)
    return jnp.logical_and(column >= start, column <= row)


def forward_steps(r, lean=False):
    tokens, width = r.x.shape
    heads = r.att.shape[1] // HD

    def norm(i):
        rows = tile(i, 64)
        value = r.x[rows].astype(F32)
        mean = jnp.sum(value, axis=1, keepdims=True) / width
        variance = jnp.sum(value * value, axis=1, keepdims=True) / width - mean * mean
        inverse_std = lax.rsqrt(variance + EPS)
        r.mean[rows] = mean
        r.inverse_std[rows] = inverse_std
        r.normed[rows] = ((value - mean) * inverse_std * r.gain[...] + r.shift[...]).astype(BF16)

    def project(i):
        rows = tile(i)
        normed = r.normed[rows]
        for c in range(3):
            value = dot(normed, r.w_qkv[c]) + r.b_qkv[c : c + 1]
            if c < 2:
                value = turn_heads(value, r.cosine[rows], r.sine[rows], 1.0)
            r.qkv[c, rows] = value.astype(BF16)

    def attend(i):
        rows = pl.ds(i * TILE, TILE)
        keys = (i + 1) * TILE
        query, key, value = r.qkv[0, rows], r.qkv[1, :keys], r.qkv[2, :keys]
        allowed = allowed_keys(r.start[rows], i * TILE, (TILE, keys))
        total = jnp.zeros((TILE, heads * HD), F32)
        for head in range(heads):
            scores = dot(of_head(query, head), key, ((1,), (1,))) * HD ** (-0.5)
            sums = jnp.sum(jnp.where(allowed, jnp.exp(scores), 0.0), axis=1, keepdims=True)
            log_total = jnp.log(sums)
            r.lse[head, rows] = log_total
            probs = jnp.where(allowed, jnp.exp(scores - log_total), 0.0).astype(BF16)
            total += dot(probs, of_head(value, head))
        r.att[rows] = total.astype(BF16)

    def up(i):
        rows = tile(i)
        value = dot(r.normed[rows], r.w_up[...]) + r.b_up[...]
        inner = jnp.tanh(GELU_C * (value + GELU_K * value * value * value))
        r.hidden[rows] = (0.5 * value * (1.0 + inner)).astype(BF16)
        r.slope[rows] = 0.5 * (1.0 + inner) + 0.5 * value * (1.0 - inner * inner) * GELU_C * (
            1.0 + 3.0 * GELU_K * value * value
        )

    def down(i):
        rows = tile(i)
        r.partial[rows] = (
            dot(r.att[rows], r.w_out[...]) + dot(r.hidden[rows], r.w_down[...])
        ).astype(BF16)

    count = tokens // TILE
    return norm, project, attend, up, down, count


def each(count, step):
    lax.fori_loop(0, count, lambda i, _: (step(i), 0)[1], 0)


def some(begin, end, step):
    lax.fori_loop(begin, end, lambda i, _: (step(i), 0)[1], 0)


def run_forward(r):
    norm, project, attend, up, down, count = forward_steps(r)
    each(r.x.shape[0] // 64, norm)
    each(count, project)
    for i in range(count):
        attend(i)
    each(count, up)
    each(count, down)


def backward_steps(r):
    tokens, width = r.g.shape
    heads = r.att.shape[1] // HD
    count = tokens // TILE

    def start():
        r.d_b_up[...] = jnp.zeros_like(r.d_b_up)
        r.d_b_qkv[...] = jnp.zeros_like(r.d_b_qkv)
        r.d_kv[...] = jnp.zeros_like(r.d_kv)

    def open_branches(i):
        rows = tile(i)
        g = r.g[rows]
        d_pre = dot(g, r.w_down[...], ((1,), (1,))) * r.slope[rows]
        r.d_b_up[...] += jnp.sum(d_pre, axis=0, keepdims=True)
        r.d_hidden[rows] = d_pre.astype(BF16)
        r.d_att[rows] = dot(g, r.w_out[...], ((1,), (1,))).astype(BF16)

    def grad_rows(i):
        columns = tile(i)
        g = r.g[:, columns]
        r.d_w_down[:, columns] = dot(r.hidden[...], g, ((0,), (0,))).astype(BF16)
        r.d_w_out[:, columns] = dot(r.att[...], g, ((0,), (0,))).astype(BF16)

    def grad_up(i):
        rows = tile(i)
        r.d_w_up[rows] = dot(r.normed[:, rows], r.d_hidden[...], ((0,), (0,))).astype(BF16)

    def attend(i):
        rows = pl.ds(i * TILE, TILE)
        keys = (i + 1) * TILE
        query, key, value = r.qkv[0, rows], r.qkv[1, :keys], r.qkv[2, :keys]
        d_att = r.d_att[rows]
        product = d_att.astype(F32) * r.att[rows].astype(F32)
        allowed = allowed_keys(r.start[rows], i * TILE, (TILE, keys))
        d_query = jnp.zeros((TILE, heads * HD), F32)
        d_key = jnp.zeros((keys, heads * HD), F32)
        d_value = jnp.zeros((keys, heads * HD), F32)
        for head in range(heads):
            q_head, d_head = of_head(query, head), of_head(d_att, head)
            scores = dot(q_head, key, ((1,), (1,))) * HD ** (-0.5)
            probs = jnp.where(allowed, jnp.exp(scores - r.lse[head, rows]), 0.0)
            delta = jnp.sum(of_head(product, head), axis=1, keepdims=True)
            d_probs = dot(d_head, value, ((1,), (1,)))
            d_scores = (probs * (d_probs - delta) * HD ** (-0.5)).astype(BF16)
            d_query += dot(d_scores, of_head(key, head))
            d_key += dot(d_scores, q_head, ((0,), (0,)))
            d_value += dot(probs.astype(BF16), d_head, ((0,), (0,)))
        r.d_query[rows] = d_query
        r.d_kv[0, :keys] += d_key
        r.d_kv[1, :keys] += d_value

    def unrotate(i):
        rows = tile(i)
        cosine, sine = r.cosine[rows], r.sine[rows]
        parts = (
            turn_heads(r.d_query[rows], cosine, sine, -1.0),
            turn_heads(r.d_kv[0, rows], cosine, sine, -1.0),
            r.d_kv[1, rows],
        )
        for c, value in enumerate(parts):
            r.d_b_qkv[c : c + 1] += jnp.sum(value, axis=0, keepdims=True)
            r.d_qkv[c, rows] = value.astype(BF16)

    def grad_qkv(i):
        rows = tile(i)
        normed = r.normed[:, rows]
        for c in range(3):
            r.d_w_qkv[c, rows] = dot(normed, r.d_qkv[c], ((0,), (0,))).astype(BF16)

    def close(i):
        rows = tile(i)
        total = dot(r.d_hidden[rows], r.w_up[...], ((1,), (1,)))
        for c in range(3):
            total += dot(r.d_qkv[c, rows], r.w_qkv[c], ((1,), (1,)))
        r.partial[rows] = total.astype(BF16)

    return start, open_branches, grad_rows, grad_up, attend, unrotate, grad_qkv, close, count


def run_backward(r):
    start, open_branches, grad_rows, grad_up, attend, unrotate, grad_qkv, close, count = backward_steps(r)
    wide = r.g.shape[1] // TILE
    start()
    each(count, open_branches)
    each(wide, grad_rows)
    each(wide, grad_up)
    for i in range(count):
        attend(i)
    each(count, unrotate)
    each(wide, grad_qkv)
    each(count, close)


class Refs:
    def __init__(self, **refs):
        self.__dict__.update(refs)


WEIGHTS = ("w_qkv", "w_out", "w_up", "w_down", B_QKV, B_UP, GAIN, SHIFT)
TABLES = (N_START, COSINE, SINE)
SAVED = (NORMED, QKV, ATT, LSE, SLOPE, HIDDEN)


def saved_shapes(tokens, width, e, f):
    return {
        NORMED: ((tokens, width), BF16),
        QKV: ((3, tokens, e), BF16),
        ATT: ((tokens, e), BF16),
        LSE: ((e // HD, tokens, 1), F32),
        SLOPE: ((tokens, f), F32),
        HIDDEN: ((tokens, f), BF16),
    }


def scratch_shapes_back(tokens, e, f):
    return {
        "d_hidden": ((tokens, f), BF16),
        "d_att": ((tokens, e), BF16),
        "d_query": ((tokens, e), F32),
        "d_kv": ((2, tokens, e), F32),
        "d_qkv": ((3, tokens, e), BF16),
    }


def grad_shapes(width, e, f):
    return {
        D_W_QKV: ((3, width, e), BF16),
        D_W_OUT: ((e, width), BF16),
        D_W_UP: ((width, f), BF16),
        D_W_DOWN: ((f, width), BF16),
        "d_b_qkv": ((3, e), F32),
        "d_b_up": ((1, f), F32),
    }


STAGED = (NORMED, QKV, ATT, SLOPE, HIDDEN)


def remote_call(
    body, name, key, inputs, outputs, scratch, copies, in_hbm=(), out_hbm=(), staged=()
):
    scratch = scratch | {each_in: (inputs[each_in].shape, inputs[each_in].dtype) for each_in in staged if each_in in inputs}
    scratch |= {each_out: outputs[each_out] for each_out in staged if each_out in outputs}
    in_hbm, out_hbm = (*in_hbm, *staged), (*out_hbm, *staged)
    vmem = pl.BlockSpec(memory_space=pltpu.VMEM)
    hbm = pl.BlockSpec(memory_space=pl.ANY)
    given = [HBM + ref if ref in staged else ref for ref in (*inputs, *outputs)]
    keys = given + list(scratch) + ["free_sem", "local_sems", "send_sems", "recv_sems"]

    def kernel(*refs):
        body(Refs(**dict(zip(keys, refs))))

    outs = pl.pallas_call(
        kernel,
        out_shape=tuple(jax.ShapeDtypeStruct(shape, kind) for shape, kind in outputs.values()),
        in_specs=[hbm if each_in in in_hbm else vmem for each_in in inputs],
        out_specs=tuple(hbm if each_out in out_hbm else vmem for each_out in outputs),
        scratch_shapes=[pltpu.VMEM(shape, kind) for shape, kind in scratch.values()]
        + [
            pltpu.SemaphoreType.REGULAR,
            pltpu.SemaphoreType.DMA((32,)),
            pltpu.SemaphoreType.DMA((copies,)),
            pltpu.SemaphoreType.DMA((copies,)),
        ],
        compiler_params=pltpu.CompilerParams(
            collective_id=key, has_side_effects=True, vmem_limit_bytes=63 << 20
        ),
        name=name,
    )(*inputs.values())
    return dict(zip(outputs, outs))


def stage(r, names, first_sem, out=False):
    copies = {}
    for i, name in enumerate(names):
        ends = (getattr(r, HBM + name), getattr(r, name))
        copies[name] = pltpu.make_async_copy(
            *(ends[::-1] if out else ends), r.local_sems.at[first_sem + i]
        )
        copies[name].start()
    return copies


def weight_scratch(turn):
    shapes = {W + name: (turn.turned_shape(name), BF16) for name in NAMES}
    width = 4 * turn.d
    return shapes | {
        B_QKV: ((3, turn.e), F32),
        B_UP: ((1, turn.f), F32),
        GAIN: ((1, width), F32),
        SHIFT: ((1, width), F32),
    }


def scatter_dict(rows, part):
    return {
        "theirs": ((2, 4 * rows, part), BF16),
        "chip": ((2, 4 * rows, part), BF16),
        "from_y": ((4 * rows, part), BF16),
        "from_far": ((3, rows, part), BF16),
    }


def back_dict(rows, part):
    return {
        "d_normed": ((rows, part), F32),
        "row_out": ((GROUPS, 8, 128), F32),
        "row_in": ((GROUPS, 3, 8, 128), F32),
    }


def scatter_of(w, r, partial, rows, part):
    return Scatter(w, partial, (r.theirs, r.chip, r.from_y, r.from_far), rows, part)


def small_params(w, r, layer):
    part = r.gain.shape[1] // 4
    slab = part // 4
    for t in range(4):
        for c in range(4):
            lanes = slice(t * part + c * slab, t * part + (c + 1) * slab)
            r.gain[:, lanes] = r.vectors[layer, c, t, 1:2]
            r.shift[:, lanes] = r.vectors[layer, c, t, 2:3]
    r.b_qkv[...] = r.vectors[layer, w.c, w.t, 3:6]
    for i in range(r.b_up.shape[1] // slab):
        r.b_up[:, i * slab : (i + 1) * slab] = r.vectors[layer, w.c, w.t, 6 + i : 7 + i]


def own_bias(w, r, layer):
    return jnp.concatenate([r.vectors[layer, c, w.t, 0:1] for c in range(4)], axis=1)


def own_gain(w, r, layer):
    return jnp.concatenate([r.vectors[layer, c, w.t, 1:2] for c in range(4)], axis=1)


FIRST = (OUT, QKV, UP, DOWN)
HALVES = {OUT: (None,), QKV: (None,), UP: (0, 1), DOWN: (0, 1)}


def pull(*generators, times=1):
    for _ in range(times):
        for generator in generators:
            next(generator, None)


def first_body(turn, rows, part, r):
    w = Wire(r.send_sems, r.recv_sems)
    s = w.section
    peers = everyone(w)
    w.greet(peers)
    shards = {name: getattr(r, SHARD + name) for name in NAMES}
    mine = {name: getattr(r, TURNED + name).at[s] for name in NAMES}
    bounce = {name: getattr(r, BOUNCE + name) for name in NAMES}
    swap = w.send(r.own.at[1 - s], r.other, w.across)
    r.vectors[s, w.c, w.t] = r.vector[...]
    told = [w.send(r.vector, r.vectors.at[s, w.c, w.t], peer) for peer in peers]
    local, far, across, puts = {}, {}, {name: [] for name in NAMES}, {}

    leave = (w.pick(3, 2, 2, 1), w.pick(2, 3, 1, 2), w.pick(1, 1, 3, 3))
    enter = (w.pick(1, 2, 2, 3), w.pick(2, 1, 3, 2), w.pick(3, 3, 1, 1))

    def along_copy(name, half, base, step):
        place = (w.c + step) % 4
        return w.step_copy(
            base,
            step,
            turn.shard(name, shards[name], place, half),
            turn.turned(name, mine[name], w.c, half),
        )

    def send_along(name):
        for half in HALVES[name]:
            base = far[name, half] = len(w.copies)
            for step in leave:
                copy = along_copy(name, half, base, step)
                copy.start()
                w.copies.append((copy, None))
                yield

    def pass_across(name):
        for half in HALVES[name]:
            for step in enter:
                along_copy(name, half, far[name, half], step).wait_recv()
                spot = turn.turned(name, mine[name], (w.c + 4 - step) % 4, half)
                across[name].append(w.send(spot, spot, w.across))
                yield

    def fetch(name):
        for copy in across[name]:
            copy.wait_recv()
        puts[name].wait()
        i = FIRST.index(name)
        copy = pltpu.make_async_copy(
            getattr(r, TURNED + name).at[0], getattr(r, W + name), r.local_sems.at[8 + i]
        )
        copy.start()
        return copy

    sending = itertools.chain(*(send_along(name) for name in FIRST))
    passing = itertools.chain(*(pass_across(name) for name in FIRST))
    pull(sending, times=6)
    for i, name in enumerate(FIRST):
        own_piece = turn.shard(name, shards[name], w.c)
        across[name].append(w.send(own_piece, turn.turned(name, mine[name], w.c), w.across))
        local[name] = pltpu.make_async_copy(own_piece, bounce[name], r.local_sems.at[i])
        local[name].start()
    swap.wait_recv()
    mine_block = r.own[s]
    r.x_block[...] = jnp.where(s == 0, mine_block, r.other[...])
    r.g_block[...] = jnp.where(s == 0, r.other[...], mine_block)
    half = rows // GROUPS
    gather_x = DirectGather(w, r.x, rows, part)
    for group in range(GROUPS):
        gather_x.region(w.c, w.t, group)[...] = r.x_block[group * half : (group + 1) * half]
        gather_x.begin(group)
    for i, name in enumerate(FIRST):
        local[name].wait()
        puts[name] = pltpu.make_async_copy(
            bounce[name], turn.turned(name, mine[name], w.c), r.local_sems.at[4 + i]
        )
        puts[name].start()
    pull(passing, times=6)
    pull(sending, times=3)
    for i, _ in enumerate(gather_x.steps()):
        if i == 5:
            pull(sending, times=3)
    for copy in told:
        copy.wait_recv()
    small_params(w, r, 0)
    norm, project, attend, up, down, count = forward_steps(r)
    each(4 * rows // 64, norm)
    ready = [fetch(OUT), fetch(QKV)]
    for copy in ready:
        copy.wait()
    each(count, project)
    pull(passing, times=3)
    pull(sending, times=3)
    attend(0)
    attend(1)
    pull(passing, times=3)
    pull(sending, times=3)
    for i in range(2, count):
        attend(i)
    fetch(UP).wait()
    each(count, up)
    stores = stage(r, STAGED, 12, True)
    for _ in passing:
        pass
    fetch(DOWN).wait()
    scatter = scatter_of(w, r, r.partial, rows, part)
    scatter.begin(down)
    scatter.run()
    gather = Gather(w, r.x1, rows, part)
    bias = own_bias(w, r, 0)
    for group in range(GROUPS):
        own = slice(group * half, (group + 1) * half)
        value = (r.x_block[own].astype(F32) + scatter.total(group) + bias).astype(BF16)
        r.act[own] = value
        gather.region(w.c, w.t, group)[...] = value
        gather.begin(group)
    for _ in gather.steps():
        pass
    for copy in stores.values():
        copy.wait()
    w.drain()


def first(own, vector, tables, shards):
    _, rows, part = own.shape
    turn = Turn(shards[QKV].shape[1], shards[QKV].shape[2] // 4, shards[UP].shape[1] // 4)
    tokens, width = 4 * rows, 4 * part
    full = ((tokens, width), BF16)
    block = ((rows, part), BF16)
    outputs = {TURNED + name: ((2,) + turn.turned_shape(name), BF16) for name in NAMES}
    outputs |= {X1: full, X_BLOCK: block, G_BLOCK: block, ACT: block}
    outputs |= {VECTORS: ((2, 4, 4) + vector.shape, F32)}
    outputs |= saved_shapes(tokens, width, turn.e, turn.f)
    outputs |= {MEAN: ((tokens, 1), F32), INVERSE_STD: ((tokens, 1), F32)}
    scratch = {BOUNCE + name: (turn.piece_shape(name), BF16) for name in NAMES}
    scratch |= {"other": block, "x": full, PARTIAL: full}
    scratch |= weight_scratch(turn) | scatter_dict(rows, part)
    return remote_call(
        functools.partial(first_body, turn, rows, part),
        "first",
        START,
        {"own": own, VECTOR: vector}
        | tables
        | {SHARD + name: shards[name] for name in NAMES},
        outputs,
        scratch,
        320,
        in_hbm=[SHARD + name for name in NAMES],
        out_hbm=[TURNED + name for name in NAMES],
        staged=STAGED,
    )


def middle_body(turn, rows, part, r):
    w = Wire(r.send_sems, r.recv_sems)
    load_x = pltpu.make_async_copy(r.x1, r.normed, r.local_sems.at[4])
    load_x.start()
    r.x = r.normed
    loads = {}
    for i, name in enumerate(FIRST):
        loads[name] = pltpu.make_async_copy(
            getattr(r, TURNED + name).at[1], getattr(r, W + name), r.local_sems.at[i]
        )
        loads[name].start()
    w.greet(neighbours(w) + [diagonal(w)])
    half = rows // GROUPS
    gather_g = Gather(w, r.g, rows, part, skew=0)
    for group in range(GROUPS):
        gather_g.region(w.c, w.t, group)[...] = r.g_block[group * half : (group + 1) * half]
        gather_g.begin(group)
    arriving = gather_g.steps()
    small_params(w, r, 1)
    norm, project, attend, up, down, count = forward_steps(r)
    load_x.wait()
    each(4 * rows // 64, norm)
    pull(arriving, times=4)
    loads[QKV].wait()
    each(count, project)
    attend(0)
    pull(arriving, times=4)
    attend(1)
    attend(2)
    pull(arriving, times=4)
    attend(3)
    pull(arriving, times=6)
    loads[UP].wait()
    each(count, up)
    loads[DOWN].wait()
    loads[OUT].wait()
    other = Scatter(w, r.partial, (r.theirs_x, r.chip_x, r.from_y_x, r.from_far_x), rows, part)
    other.begin(down)
    summing = other.steps()
    for _ in arriving:
        pass
    b = Refs(**dict(r.__dict__, partial=r.partial_g))
    start, open_branches, grad_rows, grad_up, attend_back, unrotate, grad_qkv, close, _ = (
        backward_steps(b)
    )
    start()
    pull(summing, times=2)
    some(0, 2, open_branches)
    pull(summing, times=2)
    some(2, count, open_branches)
    pull(summing, times=4)
    for i in range(count):
        attend_back(i)
        pull(summing)
    each(count, unrotate)

    def leftover():
        wide = 4 * part // TILE
        for slot, step, made in (
            (8, grad_rows, (D_W_DOWN, D_W_OUT)),
            (10, grad_up, (D_W_UP,)),
            (11, grad_qkv, (D_W_QKV,)),
        ):
            for i in range(0, wide, 2):
                some(i, i + 2, step)
                yield
            stores.update(stage(r, made, slot, True))

    stores = {}
    fill = leftover()
    scatter = scatter_of(w, r, r.partial_g, rows, part)
    scatter.begin(close)
    for _ in summing:
        pass
    for i, _ in enumerate(scatter.steps()):
        if i % 2 == 1:
            pull(fill)
    gather = Gather(w, r.g1, rows, part)
    r.mean_block[...] = r.mean[pl.ds(pl.multiple_of(w.c * rows, rows), rows)]
    r.std_block[...] = r.inverse_std[pl.ds(pl.multiple_of(w.c * rows, rows), rows)]
    r.gain_block[...] = own_gain(w, r, 1)

    def done(group):
        gather.region(w.c, w.t, group)[...] = r.grad[group * half : (group + 1) * half]
        gather.begin(group)

    norm_back(
        w,
        scatter,
        (r.g_block, r.act, r.mean_block, r.std_block, r.gain_block),
        (r.d_normed, r.row_out, r.row_in),
        rows,
        part,
        r.grad,
        r.sums,
        done,
        fill,
    )
    for _ in gather.steps():
        pull(fill)
    for _ in fill:
        pass
    bias = own_bias(w, r, 1)
    for group in range(GROUPS):
        own = slice(group * half, (group + 1) * half)
        value = r.act[own].astype(F32) + other.total(group) + bias
        r.act1[own] = value.astype(BF16)
    slab = part // 4
    columns = pl.ds(pl.multiple_of(w.t * part + w.c * slab, 128), slab)
    r.d_b_out[...] = jnp.sum(r.g[:, columns].astype(F32), axis=0, keepdims=True)
    for copy in stores.values():
        copy.wait()
    w.drain()


def middle(made, tables, turn, rows, part):
    tokens, width = 4 * rows, 4 * part
    full = ((tokens, width), BF16)
    inputs = {X1: made[X1], ACT: made[ACT], G_BLOCK: made[G_BLOCK]}
    inputs |= {VECTORS: made[VECTORS]} | tables
    inputs |= {TURNED + name: made[TURNED + name] for name in NAMES}
    outputs = grad_shapes(width, turn.e, turn.f)
    outputs |= {"d_b_out": ((1, part // 4), F32), ACT1: ((rows, part), BF16)}
    outputs |= {GRAD: ((rows, part), BF16), G1: full, SUMS: ((8, part), F32)}
    scratch = saved_shapes(tokens, width, turn.e, turn.f)
    scratch |= {MEAN: ((tokens, 1), F32), INVERSE_STD: ((tokens, 1), F32)}
    scratch |= scratch_shapes_back(tokens, turn.e, turn.f) | {"partial_g": full, G: full, PARTIAL: full}
    scratch |= {key + "_x": value for key, value in scatter_dict(rows, part).items()}
    scratch |= {MEAN_BLOCK: ((rows, 1), F32), STD_BLOCK: ((rows, 1), F32)}
    scratch |= {GAIN_BLOCK: ((1, part), F32)}
    scratch |= weight_scratch(turn) | scatter_dict(rows, part) | back_dict(rows, part)
    return remote_call(
        functools.partial(middle_body, turn, rows, part),
        "middle",
        BWD,
        inputs,
        outputs,
        scratch,
        240,
        in_hbm=[X1] + [TURNED + name for name in NAMES],
        staged=[D_W + name for name in NAMES],
    )


LATER = (OUT, DOWN, UP, QKV)


ENTERING = (G, HIDDEN, ATT, SLOPE, NORMED, QKV, COSINE, SINE)


def last_body(turn, rows, part, r):
    w = Wire(r.send_sems, r.recv_sems)
    s = w.section
    half = rows // GROUPS
    brought = stage(r, ENTERING, 20)
    loads = {}
    for i, name in enumerate(FIRST):
        loads[name] = pltpu.make_async_copy(
            getattr(r, TURNED + name).at[0], getattr(r, W + name), r.local_sems.at[i]
        )
        loads[name].start()
    moves = [(ds, dc) for ds in (0, 1) for dc in range(4) if (ds, dc) != (0, 0)]

    def away(ds, dc):
        return {SECTION: (s + ds) % 2, CTX: (w.c + dc) % 4}

    w.greet([away(*move) for move in moves] + [w.beside, w.core, diagonal(w)])
    places = [(2, w.c_far), (1, w.c_up), (3, w.c_down), (0, w.c)]
    grads0 = {name: getattr(r, D_W + name) for name in NAMES}
    grads1 = {name: getattr(r, ONE + name) for name in NAMES}
    arrived = {name: getattr(r, ARRIVED + name) for name in NAMES}
    outs = {name: getattr(r, HOME + name) for name in NAMES}
    kept = {name: getattr(r, KEPT + name) for name in NAMES}
    across, home, keeps = {}, {}, {}

    def send_across(name):
        for step, c in places:
            across[name, step] = w.send_one_of(
                s == 0,
                turn.turned(name, grads1[name], c),
                turn.turned(name, grads0[name], c),
                turn.turned(name, arrived[name], c),
                w.across,
            )

    def keep(name, c, slot):
        copy = pltpu.make_async_copy(
            turn.turned(name, grads1[name], c), kept[name].at[slot], r.local_sems.at[8 + 2 * NAMES.index(name) + slot]
        )
        copy.start()
        return copy

    def settle():
        for name in LATER:
            waiting = keep(name, places[0][1], 0)
            for i, (step, c) in enumerate(places):
                waiting.wait()
                if i < 3:
                    waiting = keep(name, places[i + 1][1], (i + 1) % 2)
                across[name, step].wait_recv()
                theirs = turn.turned(name, arrived[name], c)
                mine = jnp.where(
                    s == 0,
                    turn.turned(name, grads0[name], c)[...].astype(F32),
                    kept[name][i % 2].astype(F32),
                )
                theirs[...] = (mine + theirs[...].astype(F32)).astype(BF16)
                spot = turn.shard(name, outs[name], w.c)
                if step:
                    home[name, step] = w.send(theirs, spot, {CTX: c})
                else:
                    home[name, 0] = pltpu.make_async_copy(
                        theirs, spot, r.local_sems.at[16 + NAMES.index(name)]
                    )
                    home[name, 0].start()
                yield

    start, open_branches, grad_rows, grad_up, attend_back, unrotate, grad_qkv, close, count = (
        backward_steps(r)
    )
    wide = 4 * part // TILE
    start()
    for name in ENTERING[:3]:
        brought[name].wait()
    each(wide, grad_rows)
    for name in ENTERING[3:]:
        brought[name].wait()
    send_across(OUT)
    send_across(DOWN)
    settling = settle()
    loads[DOWN].wait()
    loads[OUT].wait()
    each(count, open_branches)
    pull(settling)
    each(wide, grad_up)
    send_across(UP)
    pull(settling)
    for i in range(count):
        attend_back(i)
        pull(settling)
    r.all_acts[0] = r.act[...]
    r.all_acts[1] = r.act1[...]
    r.acts[s] = r.all_acts[s]
    pairs = [w.send(r.all_acts.at[1 - s], r.acts.at[s], w.across)]
    each(count, unrotate)
    each(wide, grad_qkv)
    send_across(QKV)
    pull(settling)
    loads[QKV].wait()
    loads[UP].wait()
    scatter = scatter_of(w, r, r.partial, rows, part)
    scatter.begin(close)
    slab = part // 4
    columns = pl.ds(pl.multiple_of(w.t * part + w.c * slab, 128), slab)
    n_up = r.d_b_up.shape[1] // slab
    r.small[0, 0:3] = r.d_b_qkv[...]
    r.small[1, 0:3] = r.one_b_qkv[...]
    for i in range(n_up):
        lanes = slice(i * slab, (i + 1) * slab)
        r.small[0, 3 + i : 4 + i] = r.d_b_up[:, lanes]
        r.small[1, 3 + i : 4 + i] = r.one_b_up[:, lanes]
    r.small[0, 3 + n_up : 4 + n_up] = jnp.sum(r.g[:, columns].astype(F32), axis=0, keepdims=True)
    r.small[1, 3 + n_up : 4 + n_up] = r.one_b_out[...]
    small_copy = w.send(r.small.at[1 - s], r.small_in, w.across)
    for i, _ in enumerate(scatter.steps()):
        if i % 4 == 3:
            pull(settling)
    r.mean_block[...] = r.mean[pl.ds(pl.multiple_of(w.c * rows, rows), rows)]
    r.std_block[...] = r.inverse_std[pl.ds(pl.multiple_of(w.c * rows, rows), rows)]
    r.gain_block[...] = own_gain(w, r, 0)
    norm_back(
        w,
        scatter,
        (r.grad1, r.x_block, r.mean_block, r.std_block, r.gain_block),
        (r.d_normed, r.row_out, r.row_in),
        rows,
        part,
        r.all_grads.at[0],
        r.sums0,
        lambda group: None,
        settling,
    )
    r.all_grads[1] = r.grad1[...]
    r.grads[s] = r.all_grads[s]
    pairs.append(w.send(r.all_grads.at[1 - s], r.grads.at[s], w.across))
    for layer, sums in ((0, r.sums0), (1, r.sums1)):
        for c in range(4):
            r.norm_out[layer, c] = sums[:, c * slab : (c + 1) * slab]
    told = [
        w.send(r.norm_out.at[(s + ds) % 2, (w.c + dc) % 4], r.norm_in.at[slot], away(ds, dc))
        for slot, (ds, dc) in enumerate(moves)
    ]
    for _ in settling:
        pass
    small_copy.wait_recv()
    r.small_sum[...] = r.small[s] + r.small_in[...]
    total = r.norm_out[s, w.c]
    for slot, copy in enumerate(told):
        copy.wait_recv()
        total += r.norm_in[slot]
    r.norm_sum[...] = total
    for name in LATER:
        home[name, 0].wait()
        for step in (1, 3, 2):
            home[name, step].wait_recv()
    for copy in pairs:
        copy.wait_recv()
    w.drain()


def last(made, mid, tables, turn, rows, part):
    tokens, width = 4 * rows, 4 * part
    full = ((tokens, width), BF16)
    e, f = 4 * turn.e, 4 * turn.f
    homes = {
        QKV: (3, turn.d, e),
        OUT: (e, turn.d),
        UP: (turn.d, f),
        DOWN: (f, turn.d),
    }
    inputs = {G: mid[G1], "grad1": mid[GRAD], ACT1: mid[ACT1], "sums1": mid[SUMS]}
    inputs |= {key: made[key] for key in SAVED + (MEAN, INVERSE_STD, VECTORS, ACT, X_BLOCK)}
    inputs |= {ONE + name: mid[D_W + name] for name in NAMES}
    inputs |= {ONE + name: mid["d_" + name] for name in (B_QKV, B_UP, "b_out")}
    inputs |= {TURNED + name: made[TURNED + name] for name in NAMES} | tables
    pairs = ((2, rows, part), BF16)
    outputs = {HOME + name: (homes[name], BF16) for name in NAMES}
    outputs |= {ACTS: pairs, GRADS: pairs}
    outputs |= {SMALL_SUM: ((8, part // 4), F32), NORM_SUM: ((8, part // 4), F32)}
    scratch = grad_shapes(width, turn.e, turn.f) | {PARTIAL: full}
    scratch |= {ARRIVED + name: (turn.turned_shape(name), BF16) for name in NAMES}
    scratch |= {KEPT + name: ((2,) + turn.piece_shape(name), BF16) for name in NAMES}
    scratch |= scratch_shapes_back(tokens, turn.e, turn.f)
    scratch |= {W + name: (turn.turned_shape(name), BF16) for name in NAMES}
    scratch |= scatter_dict(rows, part) | back_dict(rows, part)
    scratch |= {
        MEAN_BLOCK: ((rows, 1), F32),
        STD_BLOCK: ((rows, 1), F32),
        GAIN_BLOCK: ((1, part), F32),
        "small": ((2, 8, part // 4), F32),
        "small_in": ((8, part // 4), F32),
        "sums0": ((8, part), F32),
        "norm_out": ((2, 4, 8, part // 4), F32),
        "norm_in": ((7, 8, part // 4), F32),
        "all_acts": pairs,
        "all_grads": pairs,
    }
    return remote_call(
        functools.partial(last_body, turn, rows, part),
        "last",
        LAST,
        inputs,
        outputs,
        scratch,
        140,
        in_hbm=[TURNED + name for name in NAMES] + [ONE + name for name in NAMES],
        out_hbm=[HOME + name for name in NAMES],
        staged=ENTERING,
    )


def shards(
    boundary,
    doc_ids,
    qkv_weight,
    qkv_bias,
    out_weight,
    out_bias,
    fc1_weight,
    fc1_bias,
    fc2_weight,
    fc2_bias,
    norm_gain,
    norm_shift,
):
    section = lax.axis_index(SECTION)
    rows, part = boundary.shape[2:]
    slab = out_bias.shape[1]
    n_up = fc1_bias.shape[1] // slab
    tables = doc_tables(
        lax.dynamic_index_in_dim(doc_ids, section, 0, keepdims=False), slab // HD
    )
    vector = jnp.concatenate(
        [
            out_bias.astype(F32) + fc2_bias.astype(F32),
            norm_gain.astype(F32),
            norm_shift.astype(F32),
            qkv_bias[0].astype(F32),
            fc1_bias.astype(F32).reshape(n_up, slab),
        ]
    )
    vector = jnp.pad(vector, ((0, 16 - vector.shape[0]), (0, 0)))
    shard_of = {QKV: qkv_weight[0], OUT: out_weight[0], UP: fc1_weight[0], DOWN: fc2_weight[0]}
    turn = Turn(shard_of[QKV].shape[1], slab, shard_of[UP].shape[1] // 4)
    made = first(boundary[0], vector, tables, shard_of)
    mid = middle(made, tables, turn, rows, part)
    out = last(made, mid, tables, turn, rows, part)
    small, norms = out[SMALL_SUM], out[NORM_SUM]
    bias_out = small[3 + n_up][None]
    home = {name: out[HOME + name].astype(F32)[None] for name in NAMES}
    return (
        out[ACTS][None],
        out[GRADS][None],
        home[QKV],
        small[None, :3],
        home[OUT],
        bias_out,
        home[UP],
        small[3 : 3 + n_up].reshape(1, -1),
        home[DOWN],
        bias_out,
        norms[0:1],
        norms[1:2],
    )


def from_behind(value, axis, steps):
    count = lax.axis_size(axis)
    leading, last = (max(0, -steps), min(count, count - steps))
    return lax.ppermute(value, axis, [(source, source + steps) for source in range(leading, last)])


def gelu(value):
    inner = jnp.tanh(GELU_C * (value + GELU_K * value * value * value))
    return 0.5 * value * (1.0 + inner)


def gelu_slope(value):
    inner = jnp.tanh(GELU_C * (value + GELU_K * value * value * value))
    return 0.5 * (1.0 + inner) + 0.5 * value * (1.0 - inner * inner) * GELU_C * (
        1.0 + 3.0 * GELU_K * value * value
    )


def local_layout(ids_full, ctx_index, tokens):
    length = ids_full.shape[0]
    local_ids = lax.dynamic_slice_in_dim(ids_full, ctx_index * tokens, tokens)
    start = jnp.sum((ids_full[None, :] < local_ids[:, None]).astype(jnp.int32), axis=1)
    query_at = ctx_index * tokens + jnp.arange(tokens, dtype=jnp.int32)
    key_at = jnp.arange(length, dtype=jnp.int32)
    allowed = (key_at[None, :] <= query_at[:, None]) & (ids_full[None, :] == local_ids[:, None])
    return (query_at - start, allowed)


def score_block(query, keys):
    return jnp.einsum(SCORES_EQ, query, keys, preferred_element_type=jnp.float32) * HD ** (
        -0.5
    )


def forward_layer(layer_in, ids_full, params, ctx_index):
    w_qkv, b_qkv, w_out, b_out, w_up, b_up, w_down, b_down, gain, shift = params
    tokens = layer_in.shape[0]
    heads = w_qkv.shape[2] // HD
    wide_in = layer_in.astype(jnp.float32)
    row_sums = lax.psum((jnp.sum(wide_in, axis=1), jnp.sum(wide_in * wide_in, axis=1)), TP)
    row_mean = row_sums[0] / D
    variance = row_sums[1] / D - row_mean * row_mean
    inverse_std = lax.rsqrt(variance + EPS)
    centered = (wide_in - row_mean[:, None]) * inverse_std[:, None]
    normed_part = (centered * gain.astype(jnp.float32) + shift.astype(jnp.float32)).astype(
        jnp.bfloat16
    )
    normed = lax.all_gather(normed_part, TP, axis=1, tiled=True)
    positions, allowed = local_layout(ids_full, ctx_index, tokens)
    cosine, sine = rope_tables(positions)
    projected = (
        jnp.einsum("td,cde->cte", normed, w_qkv, preferred_element_type=jnp.float32)
        + b_qkv.astype(jnp.float32)[:, None, :]
    )
    query = rotate(projected[0].reshape(tokens, heads, HD), cosine, sine, 1.0).astype(jnp.bfloat16)
    key_rot = rotate(projected[1].reshape(tokens, heads, HD), cosine, sine, 1.0).astype(
        jnp.bfloat16
    )
    value_part = projected[2].reshape(tokens, heads, HD).astype(jnp.bfloat16)
    key_all, value_all = (
        lax.all_gather(key_rot, CTX, axis=0, tiled=True),
        lax.all_gather(value_part, CTX, axis=0, tiled=True),
    )
    scores = score_block(query, key_all)
    totals = jnp.sum(jnp.where(allowed[None], jnp.exp(scores), 0.0), axis=2)
    log_total = jnp.log(totals)
    probs = jnp.where(allowed[None], jnp.exp(scores - log_total[:, :, None]), 0.0).astype(
        jnp.bfloat16
    )
    attended = (
        jnp.einsum(HEADS_EQ, probs, value_all, preferred_element_type=jnp.float32)
        .astype(jnp.bfloat16)
        .reshape(tokens, heads * HD)
    )
    hidden_pre = jnp.dot(normed, w_up, preferred_element_type=jnp.float32) + b_up.astype(
        jnp.float32
    )
    hidden = gelu(hidden_pre).astype(jnp.bfloat16)
    summands = jnp.dot(attended, w_out, preferred_element_type=jnp.float32) + jnp.dot(
        hidden, w_down, preferred_element_type=jnp.float32
    )
    mixed = lax.psum_scatter(summands, TP, scatter_dimension=1, tiled=True)
    layer_out = (wide_in + mixed + b_out.astype(jnp.float32) + b_down.astype(jnp.float32)).astype(
        jnp.bfloat16
    )
    kept = (key_rot, value_part)
    return (
        layer_out,
        (centered, inverse_std, normed, query, kept, attended, log_total, hidden_pre, hidden),
    )


def backward_layer(incoming, saved, ids_full, params, ctx_index):
    w_qkv, b_qkv, w_out, b_out, w_up, b_up, w_down, b_down, gain, shift = params
    centered, inverse_std, normed, query, kept, attended, log_total, hidden_pre, hidden = saved
    tokens = query.shape[0]
    heads = query.shape[1]
    wide_grad = incoming.astype(jnp.float32)
    grad_rows = lax.all_gather(incoming, TP, axis=1, tiled=True)
    grad_out_bias = jnp.sum(wide_grad, axis=0)
    grad_out = jnp.einsum("tk,te->ke", attended, grad_rows, preferred_element_type=jnp.float32)
    d_attended = jnp.einsum(
        "te,ke->tk", grad_rows, w_out, preferred_element_type=jnp.float32
    ).astype(jnp.bfloat16)
    grad_down = jnp.einsum("tf,te->fe", hidden, grad_rows, preferred_element_type=jnp.float32)
    d_pre = jnp.einsum(
        "te,fe->tf", grad_rows, w_down, preferred_element_type=jnp.float32
    ) * gelu_slope(hidden_pre)
    grad_up_bias = jnp.sum(d_pre, axis=0)
    d_hidden = d_pre.astype(jnp.bfloat16)
    grad_up = jnp.einsum("td,tf->df", normed, d_hidden, preferred_element_type=jnp.float32)
    key_all, value_all = (
        lax.all_gather(kept[0], CTX, axis=0, tiled=True),
        lax.all_gather(kept[1], CTX, axis=0, tiled=True),
    )
    positions, allowed = local_layout(ids_full, ctx_index, tokens)
    cosine, sine = rope_tables(positions)
    d_heads = d_attended.reshape(tokens, heads, HD)
    out_heads = attended.reshape(tokens, heads, HD)
    delta = jnp.sum(d_heads.astype(jnp.float32) * out_heads.astype(jnp.float32), axis=2)
    scores = score_block(query, key_all)
    probs = jnp.where(allowed[None], jnp.exp(scores - log_total[:, :, None]), 0.0)
    d_probs = jnp.einsum(SCORES_EQ, d_heads, value_all, preferred_element_type=jnp.float32)
    d_scores = (probs * (d_probs - delta.T[:, :, None]) * HD ** (-0.5)).astype(jnp.bfloat16)
    d_query = jnp.einsum(HEADS_EQ, d_scores, key_all, preferred_element_type=jnp.float32)
    key_terms = jnp.einsum(KEYS_EQ, d_scores, query, preferred_element_type=jnp.float32)
    value_terms = jnp.einsum(
        KEYS_EQ, probs.astype(jnp.bfloat16), d_heads, preferred_element_type=jnp.float32
    )
    d_key, d_value = (
        lax.psum_scatter(
            key_terms.astype(jnp.bfloat16), CTX, scatter_dimension=0, tiled=True
        ).astype(jnp.float32),
        lax.psum_scatter(
            value_terms.astype(jnp.bfloat16), CTX, scatter_dimension=0, tiled=True
        ).astype(jnp.float32),
    )
    d_projected = jnp.stack(
        [rotate(d_query, cosine, sine, -1.0), rotate(d_key, cosine, sine, -1.0), d_value]
    ).reshape(3, tokens, heads * HD)
    grad_qkv_bias = jnp.sum(d_projected, axis=1)
    d_qkv = d_projected.astype(jnp.bfloat16)
    grad_qkv = jnp.einsum("td,cte->cde", normed, d_qkv, preferred_element_type=jnp.float32)
    normed_terms = jnp.einsum("cte,cde->td", d_qkv, w_qkv, preferred_element_type=jnp.float32)
    normed_terms = normed_terms + jnp.einsum(
        "tf,df->td", d_hidden, w_up, preferred_element_type=jnp.float32
    )
    d_normed = lax.psum_scatter(
        normed_terms.astype(jnp.bfloat16), TP, scatter_dimension=1, tiled=True
    ).astype(jnp.float32)
    grad_gain = jnp.sum(d_normed * centered, axis=0)
    grad_shift = jnp.sum(d_normed, axis=0)
    scaled = d_normed * gain.astype(jnp.float32)
    row_terms = lax.psum((jnp.sum(scaled, axis=1), jnp.sum(scaled * centered, axis=1)), TP)
    grad_in = wide_grad + inverse_std[:, None] * (
        scaled - row_terms[0][:, None] / D - centered * (row_terms[1][:, None] / D)
    )
    grads = (
        grad_qkv,
        grad_qkv_bias,
        grad_out,
        grad_out_bias,
        grad_up,
        grad_up_bias,
        grad_down,
        grad_out_bias,
        grad_gain,
        grad_shift,
    )
    return (grad_in.astype(jnp.bfloat16), grads)


def base_shards(
    boundary,
    doc_ids,
    qkv_weight,
    qkv_bias,
    out_weight,
    out_bias,
    fc1_weight,
    fc1_bias,
    fc2_weight,
    fc2_bias,
    norm_gain,
    norm_shift,
):
    section = lax.axis_index(SECTION)
    ctx_index = lax.axis_index(CTX)
    micro = boundary.shape[1]
    tokens = boundary.shape[2]
    width_part = boundary.shape[3]
    params = (
        lax.all_gather(qkv_weight[0], CTX, axis=1, tiled=True),
        lax.all_gather(qkv_bias[0], CTX, axis=1, tiled=True),
        lax.all_gather(out_weight[0], CTX, axis=1, tiled=True),
        lax.all_gather(out_bias[0], CTX, axis=0, tiled=True),
        lax.all_gather(fc1_weight[0], CTX, axis=0, tiled=True),
        lax.all_gather(fc1_bias[0], CTX, axis=0, tiled=True),
        lax.all_gather(fc2_weight[0], CTX, axis=1, tiled=True),
        lax.all_gather(fc2_bias[0], CTX, axis=0, tiled=True),
        lax.all_gather(norm_gain[0], CTX, axis=0, tiled=True),
        lax.all_gather(norm_shift[0], CTX, axis=0, tiled=True),
    )
    inputs = boundary[0]
    ticks = jnp.arange(micro + 1, dtype=jnp.int32)

    def forward_tick(received, tick):
        index = jnp.clip(tick - section, 0, micro - 1)
        first = lax.dynamic_index_in_dim(inputs, index, 0, keepdims=False)
        layer_in = jnp.where(section == 0, first, received)
        ids_full = lax.dynamic_index_in_dim(doc_ids, index, 0, keepdims=False)
        layer_out, saved = forward_layer(layer_in, ids_full, params, ctx_index)
        passed = from_behind(layer_out, SECTION, 1)
        return (passed, (layer_out, saved))

    start_zero = jnp.zeros((tokens, width_part), jnp.bfloat16)
    leftover, (outs_all, saved_all) = lax.scan(forward_tick, start_zero, ticks)
    held = lax.optimization_barrier(
        (
            (
                qkv_weight[0],
                qkv_bias[0],
                out_weight[0],
                out_bias[0],
                fc1_weight[0],
                fc1_bias[0],
                fc2_weight[0],
                fc2_bias[0],
                norm_gain[0],
                norm_shift[0],
            ),
            outs_all,
        )
    )[0]
    back_params = (
        lax.all_gather(held[0], CTX, axis=1, tiled=True),
        lax.all_gather(held[1], CTX, axis=1, tiled=True),
        lax.all_gather(held[2], CTX, axis=1, tiled=True),
        lax.all_gather(held[3], CTX, axis=0, tiled=True),
        lax.all_gather(held[4], CTX, axis=0, tiled=True),
        lax.all_gather(held[5], CTX, axis=0, tiled=True),
        lax.all_gather(held[6], CTX, axis=1, tiled=True),
        lax.all_gather(held[7], CTX, axis=0, tiled=True),
        lax.all_gather(held[8], CTX, axis=0, tiled=True),
        lax.all_gather(held[9], CTX, axis=0, tiled=True),
    )
    zero_grads = tuple((jnp.zeros(weight.shape, jnp.float32) for weight in params))

    def backward_tick(carry, tick):
        received, totals = carry
        raw_index = tick - (1 - section)
        valid = (raw_index >= 0) & (raw_index < micro)
        index = jnp.clip(raw_index, 0, micro - 1)
        cotangent = lax.dynamic_index_in_dim(inputs, index, 0, keepdims=False)
        incoming = jnp.where(section == 1, cotangent, received)
        incoming = jnp.where(valid, incoming, jnp.zeros_like(incoming))
        position_slot = index + section
        saved = jax.tree.map(
            lambda stacked: lax.dynamic_index_in_dim(stacked, position_slot, 0, keepdims=False),
            saved_all,
        )
        ids_full = lax.dynamic_index_in_dim(doc_ids, index, 0, keepdims=False)
        grad_in, terms = backward_layer(incoming, saved, ids_full, back_params, ctx_index)
        totals = tuple((total + term for total, term in zip(totals, terms)))
        passed = from_behind(grad_in, SECTION, -1)
        return ((passed, totals), grad_in)

    (leftover_grad, totals), grads_all = lax.scan(backward_tick, (start_zero, zero_grads), ticks)
    acts = lax.dynamic_slice_in_dim(outs_all, section, micro, 0)[None]
    input_grads = lax.dynamic_slice_in_dim(grads_all, 1 - section, micro, 0)[None]
    shares = (
        lax.psum_scatter(
            totals[0].astype(jnp.bfloat16), CTX, scatter_dimension=1, tiled=True
        ).astype(jnp.float32),
        lax.psum_scatter(
            totals[1].astype(jnp.bfloat16), CTX, scatter_dimension=1, tiled=True
        ).astype(jnp.float32),
        lax.psum_scatter(
            totals[2].astype(jnp.bfloat16), CTX, scatter_dimension=1, tiled=True
        ).astype(jnp.float32),
        lax.psum_scatter(
            totals[3].astype(jnp.bfloat16), CTX, scatter_dimension=0, tiled=True
        ).astype(jnp.float32),
        lax.psum_scatter(
            totals[4].astype(jnp.bfloat16), CTX, scatter_dimension=0, tiled=True
        ).astype(jnp.float32),
        lax.psum_scatter(
            totals[5].astype(jnp.bfloat16), CTX, scatter_dimension=0, tiled=True
        ).astype(jnp.float32),
        lax.psum_scatter(
            totals[6].astype(jnp.bfloat16), CTX, scatter_dimension=1, tiled=True
        ).astype(jnp.float32),
        lax.psum_scatter(
            totals[7].astype(jnp.bfloat16), CTX, scatter_dimension=0, tiled=True
        ).astype(jnp.float32),
        lax.psum_scatter(
            totals[8].astype(jnp.bfloat16), CTX, scatter_dimension=0, tiled=True
        ).astype(jnp.float32),
        lax.psum_scatter(
            totals[9].astype(jnp.bfloat16), CTX, scatter_dimension=0, tiled=True
        ).astype(jnp.float32),
    )
    return (
        acts,
        input_grads,
        shares[0][None],
        shares[1][None],
        shares[2][None],
        shares[3][None],
        shares[4][None],
        shares[5][None],
        shares[6][None],
        shares[7][None],
        shares[8][None],
        shares[9][None],
    )


def solution(mesh):
    specs = {
        TOKEN: P(SECTION, None, CTX, TP),
        ROWS: P(SECTION, TP, CTX),
        COLUMNS: P(SECTION, CTX, TP),
        VECTOR: P(SECTION, (TP, CTX)),
        VECTORS: P(SECTION, None, (TP, CTX)),
    }
    weights = (TOKEN, VECTORS, ROWS, VECTOR, COLUMNS, VECTOR, ROWS, VECTOR, VECTOR, VECTOR)
    placed = tuple(specs[name] for name in weights)
    heads = D // HD
    place = {SECTION: 2, CTX: 4, TP: 4}
    whole_heads = heads % (mesh.shape[TP] * mesh.shape[CTX]) == 0
    return jax.shard_map(
        shards if whole_heads and dict(mesh.shape) == place else base_shards,
        mesh=mesh,
        in_specs=(specs[TOKEN], P(), *placed),
        out_specs=(specs[TOKEN], specs[TOKEN], *placed),
        check_vma=False,
    )
```

```python
import functools
import itertools

import jax
import jax.numpy as jnp
from jax import lax
from jax.experimental import pallas as pl
from jax.experimental.pallas import tpu as pltpu
from jax.sharding import PartitionSpec as P

D = 2048
HD = 64
ROT = 32
EPS = 1e-05
GELU_C = 0.7978845608028654
GELU_K = 0.044715
ACT = "act"
ACT1 = "act1"
ACTS = "acts"
ARRIVED = "arrived_"
ATT = "att"
BOUNCE = "bounce_"
B_OUT = "b_out"
B_QKV = "b_qkv"
B_UP = "b_up"
COLUMNS = "columns"
CORES = "cores"
COSINE = "cosine"
CTX = "ctx"
DOWN = "down"
D_W = "d_w_"
D_W_DOWN = "d_w_down"
D_W_OUT = "d_w_out"
D_W_QKV = "d_w_qkv"
D_W_UP = "d_w_up"
G = "g"
G1 = "g1"
GAIN = "gain"
GAIN_BLOCK = "gain_block"
GRAD = "grad"
GRADS = "grads"
G_BLOCK = "g_block"
HBM = "hbm_"
HEADS_EQ = "hts,shd->thd"
HIDDEN = "hidden"
HOME = "home_"
INVERSE_STD = "inverse_std"
KEPT = "kept_"
KEYS_EQ = "hts,thd->shd"
LSE = "lse"
MEAN = "mean"
MEAN_BLOCK = "mean_block"
NORMED = "normed"
NORM_SUM = "norm_sum"
N_RAW = "raw_"
N_START = "start"
ONE = "one_"
OUT = "out"
PARTIAL = "partial"
QKV = "qkv"
ROWS = "rows"
SCORES_EQ = "thd,shd->hts"
SECTION = "section"
SHARD = "shard_"
SHIFT = "shift"
SINE = "sine"
SLOPE = "slope"
SMALL_SUM = "small_sum"
STD_BLOCK = "std_block"
SUMS = "sums"
TOKEN = "token"
TP = "tp"
TURNED = "turned_"
UP = "up"
VECTOR = "vector"
VECTORS = "vectors"
W = "w_"
X1 = "x1"
X_BLOCK = "x_block"
BF16 = jnp.bfloat16
F32 = jnp.float32


def rope_tables(positions):
    half = ROT // 2
    freq = 10000.0 ** (-(jnp.arange(half).astype(F32) * 2.0 / ROT))
    angle = positions.astype(F32)[:, None] * freq[None, :]
    return (jnp.cos(angle), jnp.sin(angle))


def rotate(field, cosine, sine, sign):
    half = ROT // 2
    first = field[..., :half]
    second = field[..., half:ROT]
    cosine = cosine[:, None, :]
    sine = sine[:, None, :] * sign
    return jnp.concatenate(
        [first * cosine - second * sine, second * cosine + first * sine, field[..., ROT:]], axis=-1
    )


def doc_tables(ids, heads):
    length = ids.shape[0]
    start = jnp.sum((ids[None, :] < ids[:, None]).astype(jnp.int32), axis=1)
    cosine, sine = rope_tables(jnp.arange(length, dtype=jnp.int32) - start)
    still = jnp.ones((length, HD - ROT), F32)
    cosine = jnp.tile(jnp.concatenate([cosine, cosine, still], axis=1), (1, heads))
    sine = jnp.tile(jnp.concatenate([-sine, sine, 0.0 * still], axis=1), (1, heads))
    return {N_START: start[:, None], COSINE: cosine, SINE: sine}


MESH = pl.DeviceIdType.MESH
FWD, BWD, LAST, START = 0, 1, 2, 3
GROUPS = 2


class Wire:
    def __init__(self, send_sems, recv_sems):
        self.send_sems, self.recv_sems = send_sems, recv_sems
        self.copies = []
        self.section = lax.axis_index(SECTION)
        self.c = lax.axis_index(CTX)
        self.t = lax.axis_index(TP)
        self.y = self.t // 2
        self.k = self.t % 2
        self.c_up = (self.c + 1) % 4
        self.c_far = (self.c + 2) % 4
        self.c_down = (self.c + 3) % 4
        self.t_y = (self.t + 2) % 4
        self.t_core = self.t + 1 - 2 * self.k
        self.up = {CTX: jnp.minimum(self.c + 1, 3)}
        self.down = {CTX: jnp.maximum(self.c - 1, 0)}
        self.beside = {TP: self.t_y}
        self.core = {TP: self.t_core}
        self.across = {SECTION: 1 - self.section}
        self.others = [(2, self.c_far), (1, self.c_up), (3, self.c_down)]

    def greet(self, targets):
        barrier = pltpu.get_barrier_semaphore()
        for target in targets:
            pl.semaphore_signal(barrier, inc=1, device_id=target, device_id_type=MESH)
        pl.semaphore_wait(barrier, len(targets))

    def send(self, source, target, device, when=None):
        index = len(self.copies)
        copy = pltpu.make_async_remote_copy(
            src_ref=source,
            dst_ref=target,
            send_sem=self.send_sems.at[index],
            recv_sem=self.recv_sems.at[index],
            device_id=device,
            device_id_type=MESH,
        )
        if when is None:
            copy.start()
        else:
            pl.when(when)(copy.start)
        self.copies.append((copy, when))
        return copy

    def pick(self, *values):
        chosen = values[3]
        for c in (2, 1, 0):
            chosen = jnp.where(self.c == c, values[c], chosen)
        return chosen

    def step_copy(self, base, step, source, target):
        return pltpu.make_async_remote_copy(
            src_ref=source,
            dst_ref=target,
            send_sem=self.send_sems.at[base + step - 1],
            recv_sem=self.recv_sems.at[base + step - 1],
            device_id={CTX: (self.c + step) % 4},
            device_id_type=MESH,
        )

    def send_one_of(self, first, source, other_source, target, device):
        index = len(self.copies)
        copies = [
            pltpu.make_async_remote_copy(
                src_ref=ref,
                dst_ref=target,
                send_sem=self.send_sems.at[index],
                recv_sem=self.recv_sems.at[index],
                device_id=device,
                device_id_type=MESH,
            )
            for ref in (source, other_source)
        ]
        pl.when(first)(copies[0].start)
        pl.when(jnp.logical_not(first))(copies[1].start)
        self.copies.append((copies[0], None))
        return copies[0]

    def flush(self, indices):
        for index in indices:
            if self.copies[index] is not None:
                copy, when = self.copies[index]
                self.copies[index] = None
                if when is None:
                    copy.wait_send()
                else:
                    pl.when(when)(copy.wait_send)

    def drain(self):
        self.flush(range(len(self.copies)))

    def meet(self, semaphore, peers):
        for peer in peers:
            pl.semaphore_signal(semaphore, inc=1, device_id=peer, device_id_type=MESH)
        pl.semaphore_wait(semaphore, len(peers))


class Gather:
    def __init__(self, wire, full, rows, part, skew=1):
        self.w, self.full, self.rows, self.part = wire, full, rows, part
        self.size, self.skew = rows // GROUPS, skew
        self.hops, self.beside = {}, {}

    def region(self, c, t, group):
        return self.full.at[
            pl.ds(pl.multiple_of(c * self.rows + group * self.size, 16), self.size),
            pl.ds(pl.multiple_of(t * self.part, 128), self.part),
        ]

    def pass_on(self, device, c, t, group, when=None):
        spot = self.region(c, t, group)
        return self.w.send(spot, spot, device, when)

    def begin(self, group):
        w = self.w
        self.hops[group, 1] = self.pass_on(w.up, w.c, w.t, group, w.c < 3)
        self.hops[group, -1] = self.pass_on(w.down, w.c, w.t, group, w.c > 0)
        self.beside[group, 0] = self.pass_on(w.beside, w.c, w.t, group)
        self.cores = getattr(self, CORES, [])
        self.cores.append((self.pass_on(w.core, w.c, w.t, group), None))

    def steps(self):
        return itertools.chain(self.along(), self.around())

    def hop_order(self):
        events = [
            (group, sign * hop) for group in range(GROUPS) for hop in (1, 2, 3) for sign in (1, -1)
        ]
        return sorted(events, key=lambda event: (self.skew * event[0] + abs(event[1]), event[0]))

    def along(self):
        w = self.w
        for group, hop in self.hop_order():
            source = jnp.clip(w.c - hop, 0, 3)
            there = w.c >= hop if hop > 0 else w.c - hop <= 3
            pl.when(there)(self.hops[group, hop].wait_recv)
            if abs(hop) < 3:
                further = hop + (1 if hop > 0 else -1)
                ahead = w.c < 3 if hop > 0 else w.c > 0
                self.hops[group, further] = self.pass_on(
                    w.up if hop > 0 else w.down, source, w.t, group, jnp.logical_and(there, ahead)
                )
            self.beside[group, hop] = self.pass_on(w.beside, source, w.t, group, there)
            self.cores.append((self.pass_on(w.core, source, w.t, group, there), there))
            yield

    def around(self):
        w = self.w
        for group, hop in [(group, 0) for group in range(GROUPS)] + self.hop_order():
            source = jnp.clip(w.c - hop, 0, 3)
            there = None if hop == 0 else w.c >= hop if hop > 0 else w.c - hop <= 3
            copy = self.beside[group, hop]
            copy.wait_recv() if there is None else pl.when(there)(copy.wait_recv)
            self.cores.append((self.pass_on(w.core, source, w.t_y, group, there), there))
            yield
        for copy, there in self.cores:
            copy.wait_recv() if there is None else pl.when(there)(copy.wait_recv)


class DirectGather(Gather):
    def begin(self, group):
        w = self.w
        for step, place in w.others:
            self.hops[group, step] = self.pass_on({CTX: place}, w.c, w.t, group)
        self.beside[group, 0] = self.pass_on(w.beside, w.c, w.t, group)
        self.cores = getattr(self, CORES, [])
        self.cores.append((self.pass_on(w.core, w.c, w.t, group), None))

    def steps(self):
        w = self.w
        order = [(group, step) for group in range(GROUPS) for step in (1, 3, 2)]
        for group, step in order:
            source = (w.c + 4 - step) % 4
            self.hops[group, step].wait_recv()
            self.beside[group, step] = self.pass_on(w.beside, source, w.t, group)
            self.cores.append((self.pass_on(w.core, source, w.t, group), None))
            yield
        for group, step in [(group, 0) for group in range(GROUPS)] + order:
            self.beside[group, step].wait_recv()
            source = (w.c + 4 - step) % 4
            self.cores.append((self.pass_on(w.core, source, w.t_y, group), None))
            yield
        for copy, _ in self.cores:
            copy.wait_recv()


def scatter_scratch(rows, part):
    return [
        pltpu.VMEM((2, 4 * rows, part), BF16),
        pltpu.VMEM((2, 4 * rows, part), BF16),
        pltpu.VMEM((4 * rows, part), BF16),
        pltpu.VMEM((3, rows, part), BF16),
    ]


class Scatter:
    def __init__(self, wire, partial, scratch, rows, part):
        self.w, self.partial, self.rows, self.part = wire, partial, rows, part
        self.theirs, self.chip, self.from_y, self.from_far = scratch
        w = wire
        self.places = [(2, w.c_far), (1, w.c_up), (3, w.c_down), (0, w.c)]
        self.order = [
            (group, c, y)
            for group in (0, 1)
            for y in (1 - w.y, w.y)
            for _, c in self.places
        ]
        self.far, self.sent = {}, []

    def send(self, source, target, device):
        self.sent.append(len(self.w.copies))
        return self.w.send(source, target, device)

    def span(self, group, c):
        size = self.rows // 2
        return pl.ds(pl.multiple_of(c * self.rows + group * size, 16), size)

    def begin(self, compute):
        w = self.w
        self.cores = [None] * len(self.order)
        for _, place in self.places:
            compute(place)
            for index, (group, c, y) in enumerate(self.order):
                if c is place:
                    columns = pl.ds(pl.multiple_of((2 * y + 1 - w.k) * self.part, 128), self.part)
                    self.cores[index] = self.send(
                        self.partial.at[self.span(group, c), columns],
                        self.theirs.at[y, self.span(group, c)],
                        w.core,
                    )

    def take(self, index):
        group, c, y = self.order[index]
        self.cores[index].wait_recv()
        rows = self.span(group, c)
        columns = pl.ds(pl.multiple_of((2 * y + self.w.k) * self.part, 128), self.part)
        return self.partial[rows, columns].astype(F32) + self.theirs[y, rows].astype(F32)

    def run(self):
        for _ in self.steps():
            pass

    def steps(self):
        w = self.w
        half = self.rows // 2
        beside = {}
        for group in (0, 1):
            for slot, (_, c) in enumerate(self.places):
                rows = self.span(group, c)
                self.chip[1 - w.y, rows] = self.take(8 * group + slot).astype(BF16)
                beside[group, slot] = self.send(
                    self.chip.at[1 - w.y, rows], self.from_y.at[rows], w.beside
                )
                yield
        for group in (0, 1):
            for slot, (step, c) in enumerate(self.places):
                rows = self.span(group, c)
                value = self.take(8 * group + 4 + slot)
                beside[group, slot].wait_recv()
                self.chip[w.y, rows] = (value + self.from_y[rows].astype(F32)).astype(BF16)
                if step:
                    self.far[group, step] = self.send(
                        self.chip.at[w.y, rows],
                        self.from_far.at[step - 1, pl.ds(group * half, half)],
                        {CTX: c},
                    )
                yield

    def total(self, group):
        half = self.rows // 2
        value = self.chip[self.w.y, self.span(group, self.w.c)].astype(F32)
        for step in (1, 3, 2):
            self.far[group, step].wait_recv()
            value += self.from_far[step - 1, pl.ds(group * half, half)].astype(F32)
        return value


def neighbours(w):
    return [{CTX: place} for _, place in w.others] + [w.beside, w.core]


def diagonal(w):
    return {TP: (w.t_core + 2) % 4}


def back_scratch(rows, part):
    return [
        pltpu.VMEM((rows, part), F32),
        pltpu.VMEM((GROUPS, 8, 128), F32),
        pltpu.VMEM((GROUPS, 3, 8, 128), F32),
    ]


def norm_back(w, scatter, blocks, scratch, rows, part, grad, sums, done, fill=iter(())):
    g_block, x_block, mean, inverse_std, gain = blocks
    d_normed, row_out, row_in = scratch
    half = rows // GROUPS
    width = 4 * part
    lane = lax.broadcasted_iota(jnp.int32, (128, 128), 1)
    sent = []
    gain_sum = jnp.zeros((1, part), F32)
    shift_sum = jnp.zeros((1, part), F32)
    for group in range(GROUPS):
        own = slice(group * half, (group + 1) * half)
        value = scatter.total(group)
        for _ in range(2):
            next(fill, None)
        d_normed[own] = value
        centered = (x_block[own].astype(F32) - mean[own]) * inverse_std[own]
        weighted = value * centered
        gain_sum += jnp.sum(weighted, axis=0, keepdims=True)
        shift_sum += jnp.sum(value, axis=0, keepdims=True)
        first = jnp.sum(value * gain[...], axis=1, keepdims=True)
        second = jnp.sum(weighted * gain[...], axis=1, keepdims=True)
        packed = jnp.where(lane == 0, first, jnp.where(lane == 1, second, 0.0))
        row_out[group] = packed.T[:8]
        sent.append(
            [
                w.send(row_out.at[group], row_in.at[group, slot], peer)
                for slot, peer in enumerate((w.beside, w.core, diagonal(w)))
            ]
        )
    sums[...] = jnp.concatenate(
        [gain_sum, shift_sum, jnp.zeros((6, part), F32)], axis=0
    )
    for group in range(GROUPS):
        own = slice(group * half, (group + 1) * half)
        next(fill, None)
        for copy in sent[group]:
            copy.wait_recv()
        rows_sum = row_out[group] + row_in[group, 0] + row_in[group, 1] + row_in[group, 2]
        columns = jnp.concatenate([rows_sum, jnp.zeros((half - 8, 128), F32)], axis=0).T
        centered = (x_block[own].astype(F32) - mean[own]) * inverse_std[own]
        scaled = d_normed[own] * gain[...]
        value = g_block[own].astype(F32) + inverse_std[own] * (
            scaled - columns[:, 0:1] / width - centered * (columns[:, 1:2] / width)
        )
        grad[own] = value.astype(BF16)
        done(group)


class Turn:
    def __init__(self, d_part, e_part, f_part):
        self.d, self.e, self.f = d_part, e_part, f_part

    def rows(self, name):
        return {QKV: self.d, OUT: self.e, UP: self.d, DOWN: self.f}[name]

    def inner(self, name, half):
        size = self.rows(name)
        if half is None:
            return (0, size)
        index, count = half
        return (index * size // count, size // count)

    def shard(self, name, ref, c, half=None):
        start, size = self.inner(name, half)
        if name == QKV:
            return ref.at[:, pl.ds(start, size), pl.ds(pl.multiple_of(c * self.e, 128), self.e)]
        if name == UP:
            return ref.at[pl.ds(start, size), pl.ds(pl.multiple_of(c * self.f, 128), self.f)]
        stride = self.e if name == OUT else self.f
        return ref.at[pl.ds(pl.multiple_of(c * stride + start, 16), size)]

    def turned(self, name, ref, c, half=None):
        start, size = self.inner(name, half)
        if name == QKV:
            return ref.at[:, pl.ds(pl.multiple_of(c * self.d + start, 16), size)]
        if name == UP:
            return ref.at[pl.ds(pl.multiple_of(c * self.d + start, 16), size)]
        return ref.at[pl.ds(start, size), pl.ds(pl.multiple_of(c * self.d, 128), self.d)]

    def piece_shape(self, name, halved=False):
        size = self.rows(name) // (2 if halved else 1)
        return {
            QKV: (3, size, self.e),
            OUT: (size, self.d),
            UP: (size, self.f),
            DOWN: (size, self.d),
        }[name]

    def turned_shape(self, name):
        return {
            QKV: (3, 4 * self.d, self.e),
            OUT: (self.e, 4 * self.d),
            UP: (4 * self.d, self.f),
            DOWN: (self.f, 4 * self.d),
        }[name]


NAMES = (QKV, OUT, UP, DOWN)


def everyone(w):
    return [
        {SECTION: (w.section + ds) % 2, CTX: (w.c + dc) % 4, TP: (w.t + dt) % 4}
        for ds in range(2)
        for dc in range(4)
        for dt in range(4)
        if (ds, dc, dt) != (0, 0, 0)
    ]


TILE = 256


def dot(a, b, contract=((1,), (0,))):
    return lax.dot_general(a, b, (contract, ((), ())), preferred_element_type=F32)


def tile(i, size=TILE):
    return pl.ds(pl.multiple_of(i * size, size), size)


def turn_heads(value, cosine, sine, sign):
    half = ROT // 2
    width = value.shape[1]
    lane = lax.broadcasted_iota(jnp.int32, value.shape, 1) % HD
    partner = jnp.where(
        lane < half, pltpu.roll(value, width - half, 1), pltpu.roll(value, half, 1)
    )
    return value * cosine + partner * (sine * sign)


def head_mask(shape, head):
    lane = lax.broadcasted_iota(jnp.int32, shape, 1)
    return jnp.logical_and(lane >= head * HD, lane < (head + 1) * HD)


def of_head(value, head):
    return jnp.where(head_mask(value.shape, head), value, jnp.zeros_like(value))


def allowed_keys(start, first_row, shape):
    row = lax.broadcasted_iota(jnp.int32, shape, 0) + first_row
    column = lax.broadcasted_iota(jnp.int32, shape, 1)
    return jnp.logical_and(column >= start, column <= row)


def forward_steps(r, lean=False):
    tokens, width = r.x.shape
    heads = r.att.shape[1] // HD

    def norm(i):
        rows = tile(i, 64)
        value = r.x[rows].astype(F32)
        mean = jnp.sum(value, axis=1, keepdims=True) / width
        variance = jnp.sum(value * value, axis=1, keepdims=True) / width - mean * mean
        inverse_std = lax.rsqrt(variance + EPS)
        r.mean[rows] = mean
        r.inverse_std[rows] = inverse_std
        r.normed[rows] = ((value - mean) * inverse_std * r.gain[...] + r.shift[...]).astype(BF16)

    def project(i):
        rows = tile(i)
        normed = r.normed[rows]
        for c in range(3):
            value = dot(normed, r.w_qkv[c]) + r.b_qkv[c : c + 1]
            if c < 2:
                value = turn_heads(value, r.cosine[rows], r.sine[rows], 1.0)
            r.qkv[c, rows] = value.astype(BF16)

    def attend(i):
        rows = pl.ds(i * TILE, TILE)
        keys = (i + 1) * TILE
        query, key, value = r.qkv[0, rows], r.qkv[1, :keys], r.qkv[2, :keys]
        allowed = allowed_keys(r.start[rows], i * TILE, (TILE, keys))
        total = jnp.zeros((TILE, heads * HD), F32)
        for head in range(heads):
            scores = dot(of_head(query, head), key, ((1,), (1,))) * HD ** (-0.5)
            sums = jnp.sum(jnp.where(allowed, jnp.exp(scores), 0.0), axis=1, keepdims=True)
            log_total = jnp.log(sums)
            r.lse[head, rows] = log_total
            probs = jnp.where(allowed, jnp.exp(scores - log_total), 0.0).astype(BF16)
            total += dot(probs, of_head(value, head))
        r.att[rows] = total.astype(BF16)

    def up(i):
        rows = tile(i)
        value = dot(r.normed[rows], r.w_up[...]) + r.b_up[...]
        inner = jnp.tanh(GELU_C * (value + GELU_K * value * value * value))
        r.hidden[rows] = (0.5 * value * (1.0 + inner)).astype(BF16)
        r.slope[rows] = 0.5 * (1.0 + inner) + 0.5 * value * (1.0 - inner * inner) * GELU_C * (
            1.0 + 3.0 * GELU_K * value * value
        )

    def down(i):
        rows = tile(i)
        r.partial[rows] = (
            dot(r.att[rows], r.w_out[...]) + dot(r.hidden[rows], r.w_down[...])
        ).astype(BF16)

    count = tokens // TILE
    return norm, project, attend, up, down, count


def each(count, step):
    lax.fori_loop(0, count, lambda i, _: (step(i), 0)[1], 0)


def some(begin, end, step):
    lax.fori_loop(begin, end, lambda i, _: (step(i), 0)[1], 0)


def run_forward(r):
    norm, project, attend, up, down, count = forward_steps(r)
    each(r.x.shape[0] // 64, norm)
    each(count, project)
    for i in range(count):
        attend(i)
    each(count, up)
    each(count, down)


def backward_steps(r):
    tokens, width = r.g.shape
    heads = r.att.shape[1] // HD
    count = tokens // TILE

    def start():
        r.d_b_up[...] = jnp.zeros_like(r.d_b_up)
        r.d_b_qkv[...] = jnp.zeros_like(r.d_b_qkv)
        r.d_kv[...] = jnp.zeros_like(r.d_kv)

    def open_branches(i):
        rows = tile(i)
        g = r.g[rows]
        d_pre = dot(g, r.w_down[...], ((1,), (1,))) * r.slope[rows]
        r.d_b_up[...] += jnp.sum(d_pre, axis=0, keepdims=True)
        r.d_hidden[rows] = d_pre.astype(BF16)
        r.d_att[rows] = dot(g, r.w_out[...], ((1,), (1,))).astype(BF16)

    def grad_rows(i):
        columns = tile(i)
        g = r.g[:, columns]
        r.d_w_down[:, columns] = dot(r.hidden[...], g, ((0,), (0,))).astype(BF16)
        r.d_w_out[:, columns] = dot(r.att[...], g, ((0,), (0,))).astype(BF16)

    def grad_up(i):
        rows = tile(i)
        r.d_w_up[rows] = dot(r.normed[:, rows], r.d_hidden[...], ((0,), (0,))).astype(BF16)

    def attend(i):
        rows = pl.ds(i * TILE, TILE)
        keys = (i + 1) * TILE
        query, key, value = r.qkv[0, rows], r.qkv[1, :keys], r.qkv[2, :keys]
        d_att = r.d_att[rows]
        product = d_att.astype(F32) * r.att[rows].astype(F32)
        allowed = allowed_keys(r.start[rows], i * TILE, (TILE, keys))
        d_query = jnp.zeros((TILE, heads * HD), F32)
        d_key = jnp.zeros((keys, heads * HD), F32)
        d_value = jnp.zeros((keys, heads * HD), F32)
        for head in range(heads):
            q_head, d_head = of_head(query, head), of_head(d_att, head)
            scores = dot(q_head, key, ((1,), (1,))) * HD ** (-0.5)
            probs = jnp.where(allowed, jnp.exp(scores - r.lse[head, rows]), 0.0)
            delta = jnp.sum(of_head(product, head), axis=1, keepdims=True)
            d_probs = dot(d_head, value, ((1,), (1,)))
            d_scores = (probs * (d_probs - delta) * HD ** (-0.5)).astype(BF16)
            d_query += dot(d_scores, of_head(key, head))
            d_key += dot(d_scores, q_head, ((0,), (0,)))
            d_value += dot(probs.astype(BF16), d_head, ((0,), (0,)))
        r.d_query[rows] = d_query
        r.d_kv[0, :keys] += d_key
        r.d_kv[1, :keys] += d_value

    def unrotate(i):
        rows = tile(i)
        cosine, sine = r.cosine[rows], r.sine[rows]
        parts = (
            turn_heads(r.d_query[rows], cosine, sine, -1.0),
            turn_heads(r.d_kv[0, rows], cosine, sine, -1.0),
            r.d_kv[1, rows],
        )
        for c, value in enumerate(parts):
            r.d_b_qkv[c : c + 1] += jnp.sum(value, axis=0, keepdims=True)
            r.d_qkv[c, rows] = value.astype(BF16)

    def grad_qkv(i):
        rows = tile(i)
        normed = r.normed[:, rows]
        for c in range(3):
            r.d_w_qkv[c, rows] = dot(normed, r.d_qkv[c], ((0,), (0,))).astype(BF16)

    def close(i):
        rows = tile(i)
        total = dot(r.d_hidden[rows], r.w_up[...], ((1,), (1,)))
        for c in range(3):
            total += dot(r.d_qkv[c, rows], r.w_qkv[c], ((1,), (1,)))
        r.partial[rows] = total.astype(BF16)

    return start, open_branches, grad_rows, grad_up, attend, unrotate, grad_qkv, close, count


def run_backward(r):
    start, open_branches, grad_rows, grad_up, attend, unrotate, grad_qkv, close, count = backward_steps(r)
    wide = r.g.shape[1] // TILE
    start()
    each(count, open_branches)
    each(wide, grad_rows)
    each(wide, grad_up)
    for i in range(count):
        attend(i)
    each(count, unrotate)
    each(wide, grad_qkv)
    each(count, close)


class Refs:
    def __init__(self, **refs):
        self.__dict__.update(refs)


WEIGHTS = ("w_qkv", "w_out", "w_up", "w_down", B_QKV, B_UP, GAIN, SHIFT)
TABLES = (N_START, COSINE, SINE)
SAVED = (NORMED, QKV, ATT, LSE, SLOPE, HIDDEN)


def saved_shapes(tokens, width, e, f):
    return {
        NORMED: ((tokens, width), BF16),
        QKV: ((3, tokens, e), BF16),
        ATT: ((tokens, e), BF16),
        LSE: ((e // HD, tokens, 1), F32),
        SLOPE: ((tokens, f), F32),
        HIDDEN: ((tokens, f), BF16),
    }


def scratch_shapes_back(tokens, e, f):
    return {
        "d_hidden": ((tokens, f), BF16),
        "d_att": ((tokens, e), BF16),
        "d_query": ((tokens, e), F32),
        "d_kv": ((2, tokens, e), F32),
        "d_qkv": ((3, tokens, e), BF16),
    }


def grad_shapes(width, e, f):
    return {
        D_W_QKV: ((3, width, e), BF16),
        D_W_OUT: ((e, width), BF16),
        D_W_UP: ((width, f), BF16),
        D_W_DOWN: ((f, width), BF16),
        "d_b_qkv": ((3, e), F32),
        "d_b_up": ((1, f), F32),
    }


STAGED = (NORMED, QKV, ATT, SLOPE, HIDDEN)


def remote_call(
    body, name, key, inputs, outputs, scratch, copies, in_hbm=(), out_hbm=(), staged=()
):
    scratch = scratch | {each_in: (inputs[each_in].shape, inputs[each_in].dtype) for each_in in staged if each_in in inputs}
    scratch |= {each_out: outputs[each_out] for each_out in staged if each_out in outputs}
    in_hbm, out_hbm = (*in_hbm, *staged), (*out_hbm, *staged)
    vmem = pl.BlockSpec(memory_space=pltpu.VMEM)
    hbm = pl.BlockSpec(memory_space=pl.ANY)
    given = [HBM + ref if ref in staged else ref for ref in (*inputs, *outputs)]
    keys = given + list(scratch) + ["free_sem", "local_sems", "send_sems", "recv_sems"]

    def kernel(*refs):
        body(Refs(**dict(zip(keys, refs))))

    outs = pl.pallas_call(
        kernel,
        out_shape=tuple(jax.ShapeDtypeStruct(shape, kind) for shape, kind in outputs.values()),
        in_specs=[hbm if each_in in in_hbm else vmem for each_in in inputs],
        out_specs=tuple(hbm if each_out in out_hbm else vmem for each_out in outputs),
        scratch_shapes=[pltpu.VMEM(shape, kind) for shape, kind in scratch.values()]
        + [
            pltpu.SemaphoreType.REGULAR,
            pltpu.SemaphoreType.DMA((32,)),
            pltpu.SemaphoreType.DMA((copies,)),
            pltpu.SemaphoreType.DMA((copies,)),
        ],
        compiler_params=pltpu.CompilerParams(
            collective_id=key, has_side_effects=True, vmem_limit_bytes=63 << 20
        ),
        name=name,
    )(*inputs.values())
    return dict(zip(outputs, outs))


def stage(r, names, first_sem, out=False):
    copies = {}
    for i, name in enumerate(names):
        ends = (getattr(r, HBM + name), getattr(r, name))
        copies[name] = pltpu.make_async_copy(
            *(ends[::-1] if out else ends), r.local_sems.at[first_sem + i]
        )
        copies[name].start()
    return copies


def weight_scratch(turn):
    shapes = {W + name: (turn.turned_shape(name), BF16) for name in NAMES}
    width = 4 * turn.d
    return shapes | {
        B_QKV: ((3, turn.e), F32),
        B_UP: ((1, turn.f), F32),
        GAIN: ((1, width), F32),
        SHIFT: ((1, width), F32),
    }


def scatter_dict(rows, part):
    return {
        "theirs": ((2, 4 * rows, part), BF16),
        "chip": ((2, 4 * rows, part), BF16),
        "from_y": ((4 * rows, part), BF16),
        "from_far": ((3, rows, part), BF16),
    }


def back_dict(rows, part):
    return {
        "d_normed": ((rows, part), F32),
        "row_out": ((GROUPS, 8, 128), F32),
        "row_in": ((GROUPS, 3, 8, 128), F32),
    }


def scatter_of(w, r, partial, rows, part):
    return Scatter(w, partial, (r.theirs, r.chip, r.from_y, r.from_far), rows, part)


def small_params(w, r, layer):
    part = r.gain.shape[1] // 4
    slab = part // 4
    for t in range(4):
        for c in range(4):
            lanes = slice(t * part + c * slab, t * part + (c + 1) * slab)
            r.gain[:, lanes] = r.vectors[layer, c, t, 1:2]
            r.shift[:, lanes] = r.vectors[layer, c, t, 2:3]
    r.b_qkv[...] = r.vectors[layer, w.c, w.t, 3:6]
    for i in range(r.b_up.shape[1] // slab):
        r.b_up[:, i * slab : (i + 1) * slab] = r.vectors[layer, w.c, w.t, 6 + i : 7 + i]


def own_bias(w, r, layer):
    return jnp.concatenate([r.vectors[layer, c, w.t, 0:1] for c in range(4)], axis=1)


def own_gain(w, r, layer):
    return jnp.concatenate([r.vectors[layer, c, w.t, 1:2] for c in range(4)], axis=1)


FIRST = (OUT, QKV, UP, DOWN)
HALVES = {
    OUT: (None,),
    QKV: (None,),
    UP: ((0, 2), (1, 2)),
    DOWN: ((0, 4), (1, 4), (2, 4), (3, 4)),
}


def pull(*generators, times=1):
    for _ in range(times):
        for generator in generators:
            next(generator, None)


def first_body(turn, rows, part, r):
    w = Wire(r.send_sems, r.recv_sems)
    s = w.section
    peers = everyone(w)
    w.greet(peers)
    shards = {name: getattr(r, SHARD + name) for name in NAMES}
    mine = {name: getattr(r, TURNED + name).at[s] for name in NAMES}
    bounce = {name: getattr(r, BOUNCE + name) for name in NAMES}
    swap = w.send(r.own.at[1 - s], r.other, w.across)
    raw = [getattr(r, N_RAW + name)[...].astype(F32) for name in RAW]
    slab = raw[0].shape[1]
    r.vector[...] = jnp.zeros_like(r.vector)
    r.vector[0:1] = raw[0] + raw[1]
    r.vector[1:2], r.vector[2:3], r.vector[3:6] = raw[2], raw[3], raw[4]
    for i in range(raw[5].shape[1] // slab):
        r.vector[6 + i : 7 + i] = raw[5][:, i * slab : (i + 1) * slab]
    r.vectors[s, w.c, w.t] = r.vector[...]
    told = [w.send(r.vector, r.vectors.at[s, w.c, w.t], peer) for peer in peers]
    local, far, across, puts = {}, {}, {name: [] for name in NAMES}, {}

    leave = (w.pick(3, 2, 2, 1), w.pick(2, 3, 1, 2), w.pick(1, 1, 3, 3))
    enter = (w.pick(1, 2, 2, 3), w.pick(2, 1, 3, 2), w.pick(3, 3, 1, 1))

    def along_copy(name, half, base, step):
        place = (w.c + step) % 4
        return w.step_copy(
            base,
            step,
            turn.shard(name, shards[name], place, half),
            turn.turned(name, mine[name], w.c, half),
        )

    def send_along(name):
        for half in HALVES[name]:
            base = far[name, half] = len(w.copies)
            for step in leave:
                copy = along_copy(name, half, base, step)
                copy.start()
                w.copies.append((copy, None))
                yield

    def pass_across(name):
        for half in HALVES[name]:
            for step in enter:
                along_copy(name, half, far[name, half], step).wait_recv()
                spot = turn.turned(name, mine[name], (w.c + 4 - step) % 4, half)
                across[name].append(w.send(spot, spot, w.across))
                yield

    def fetch(name):
        for copy in across[name]:
            copy.wait_recv()
        puts[name].wait()
        i = FIRST.index(name)
        copy = pltpu.make_async_copy(
            getattr(r, TURNED + name).at[0], getattr(r, W + name), r.local_sems.at[8 + i]
        )
        copy.start()
        return copy

    sending = itertools.chain(*(send_along(name) for name in FIRST))
    passing = itertools.chain(*(pass_across(name) for name in FIRST))
    pull(sending, times=6)
    for i, name in enumerate(FIRST):
        own_piece = turn.shard(name, shards[name], w.c)
        across[name].append(w.send(own_piece, turn.turned(name, mine[name], w.c), w.across))
        local[name] = pltpu.make_async_copy(own_piece, bounce[name], r.local_sems.at[i])
        local[name].start()
    swap.wait_recv()
    mine_block = r.own[s]
    r.x_block[...] = jnp.where(s == 0, mine_block, r.other[...])
    r.g_block[...] = jnp.where(s == 0, r.other[...], mine_block)
    half = rows // GROUPS
    gather_x = DirectGather(w, r.x, rows, part)
    for group in range(GROUPS):
        gather_x.region(w.c, w.t, group)[...] = r.x_block[group * half : (group + 1) * half]
        gather_x.begin(group)
    for i, name in enumerate(FIRST):
        local[name].wait()
        puts[name] = pltpu.make_async_copy(
            bounce[name], turn.turned(name, mine[name], w.c), r.local_sems.at[4 + i]
        )
        puts[name].start()
    pull(passing, times=6)
    pull(sending, times=3)
    for i, _ in enumerate(gather_x.steps()):
        if i == 5:
            pull(sending, times=3)
    for copy in told:
        copy.wait_recv()
    small_params(w, r, 0)
    norm, project, attend, up, down, count = forward_steps(r)
    each(4 * rows // 64, norm)
    ready = [fetch(OUT), fetch(QKV)]
    for copy in ready:
        copy.wait()
    each(count, project)
    pull(passing, times=3)
    pull(sending, times=6)
    attend(0)
    attend(1)
    pull(passing, times=3)
    pull(sending, times=6)
    for i in range(2, count):
        attend(i)
    fetch(UP).wait()
    each(count, up)
    stores = stage(r, STAGED, 12, True)
    for _ in passing:
        pass
    fetch(DOWN).wait()
    scatter = scatter_of(w, r, r.partial, rows, part)
    scatter.begin(down)
    scatter.run()
    gather = Gather(w, r.x1, rows, part)
    bias = own_bias(w, r, 0)
    for group in range(GROUPS):
        own = slice(group * half, (group + 1) * half)
        value = (r.x_block[own].astype(F32) + scatter.total(group) + bias).astype(BF16)
        r.act[own] = value
        gather.region(w.c, w.t, group)[...] = value
        gather.begin(group)
    for _ in gather.steps():
        pass
    for copy in stores.values():
        copy.wait()
    w.drain()


RAW = (B_OUT, "b_down", GAIN, SHIFT, B_QKV, B_UP)


def first(own, vectors, tables, shards):
    _, rows, part = own.shape
    turn = Turn(shards[QKV].shape[1], shards[QKV].shape[2] // 4, shards[UP].shape[1] // 4)
    tokens, width = 4 * rows, 4 * part
    full = ((tokens, width), BF16)
    block = ((rows, part), BF16)
    outputs = {TURNED + name: ((2,) + turn.turned_shape(name), BF16) for name in NAMES}
    outputs |= {X1: full, X_BLOCK: block, G_BLOCK: block, ACT: block}
    outputs |= {VECTORS: ((2, 4, 4, 16, turn.e), F32)}
    outputs |= saved_shapes(tokens, width, turn.e, turn.f)
    outputs |= {MEAN: ((tokens, 1), F32), INVERSE_STD: ((tokens, 1), F32)}
    scratch = {BOUNCE + name: (turn.piece_shape(name), BF16) for name in NAMES}
    scratch |= {"other": block, "x": full, PARTIAL: full, VECTOR: ((16, turn.e), F32)}
    scratch |= weight_scratch(turn) | scatter_dict(rows, part)
    return remote_call(
        functools.partial(first_body, turn, rows, part),
        "first",
        START,
        {"own": own}
        | {N_RAW + name: vector for name, vector in zip(RAW, vectors)}
        | tables
        | {SHARD + name: shards[name] for name in NAMES},
        outputs,
        scratch,
        320,
        in_hbm=[SHARD + name for name in NAMES],
        out_hbm=[TURNED + name for name in NAMES],
        staged=STAGED,
    )


def middle_body(turn, rows, part, r):
    w = Wire(r.send_sems, r.recv_sems)
    load_x = pltpu.make_async_copy(r.x1, r.normed, r.local_sems.at[4])
    load_x.start()
    r.x = r.normed
    loads = {}
    for i, name in enumerate(FIRST):
        loads[name] = pltpu.make_async_copy(
            getattr(r, TURNED + name).at[1], getattr(r, W + name), r.local_sems.at[i]
        )
        loads[name].start()
    w.greet(neighbours(w) + [diagonal(w)])
    half = rows // GROUPS
    gather_g = Gather(w, r.g, rows, part, skew=0)
    for group in range(GROUPS):
        gather_g.region(w.c, w.t, group)[...] = r.g_block[group * half : (group + 1) * half]
        gather_g.begin(group)
    arriving = gather_g.steps()
    small_params(w, r, 1)
    norm, project, attend, up, down, count = forward_steps(r)
    load_x.wait()
    each(4 * rows // 64, norm)
    pull(arriving, times=4)
    loads[QKV].wait()
    each(count, project)
    attend(0)
    pull(arriving, times=4)
    attend(1)
    attend(2)
    pull(arriving, times=4)
    attend(3)
    pull(arriving, times=6)
    loads[UP].wait()
    each(count, up)
    loads[DOWN].wait()
    loads[OUT].wait()
    other = Scatter(w, r.partial, (r.theirs_x, r.chip_x, r.from_y_x, r.from_far_x), rows, part)
    other.begin(down)
    summing = other.steps()
    for _ in arriving:
        pass
    b = Refs(**dict(r.__dict__, partial=r.partial_g))
    start, open_branches, grad_rows, grad_up, attend_back, unrotate, grad_qkv, close, _ = (
        backward_steps(b)
    )
    start()
    pull(summing, times=2)
    some(0, 2, open_branches)
    pull(summing, times=2)
    some(2, count, open_branches)
    pull(summing, times=4)
    for i in range(count):
        attend_back(i)
        pull(summing)
    each(count, unrotate)

    def leftover():
        wide = 4 * part // TILE
        for slot, step, made in (
            (8, grad_rows, (D_W_DOWN, D_W_OUT)),
            (10, grad_up, (D_W_UP,)),
            (11, grad_qkv, (D_W_QKV,)),
        ):
            for i in range(0, wide, 2):
                some(i, i + 2, step)
                yield
            stores.update(stage(r, made, slot, True))

    stores = {}
    fill = leftover()
    scatter = scatter_of(w, r, r.partial_g, rows, part)
    scatter.begin(close)
    for _ in summing:
        pass
    for i, _ in enumerate(scatter.steps()):
        if i % 2 == 1:
            pull(fill)
    gather = Gather(w, r.g1, rows, part)
    r.mean_block[...] = r.mean[pl.ds(pl.multiple_of(w.c * rows, rows), rows)]
    r.std_block[...] = r.inverse_std[pl.ds(pl.multiple_of(w.c * rows, rows), rows)]
    r.gain_block[...] = own_gain(w, r, 1)

    def done(group):
        gather.region(w.c, w.t, group)[...] = r.grad[group * half : (group + 1) * half]
        gather.begin(group)

    norm_back(
        w,
        scatter,
        (r.g_block, r.act, r.mean_block, r.std_block, r.gain_block),
        (r.d_normed, r.row_out, r.row_in),
        rows,
        part,
        r.grad,
        r.sums,
        done,
        fill,
    )
    for _ in gather.steps():
        pull(fill)
    for _ in fill:
        pass
    bias = own_bias(w, r, 1)
    for group in range(GROUPS):
        own = slice(group * half, (group + 1) * half)
        value = r.act[own].astype(F32) + other.total(group) + bias
        r.act1[own] = value.astype(BF16)
    slab = part // 4
    columns = pl.ds(pl.multiple_of(w.t * part + w.c * slab, 128), slab)
    r.d_b_out[...] = jnp.sum(r.g[:, columns].astype(F32), axis=0, keepdims=True)
    for copy in stores.values():
        copy.wait()
    w.drain()


def middle(made, tables, turn, rows, part):
    tokens, width = 4 * rows, 4 * part
    full = ((tokens, width), BF16)
    inputs = {X1: made[X1], ACT: made[ACT], G_BLOCK: made[G_BLOCK]}
    inputs |= {VECTORS: made[VECTORS]} | tables
    inputs |= {TURNED + name: made[TURNED + name] for name in NAMES}
    outputs = grad_shapes(width, turn.e, turn.f)
    outputs |= {"d_b_out": ((1, part // 4), F32), ACT1: ((rows, part), BF16)}
    outputs |= {GRAD: ((rows, part), BF16), G1: full, SUMS: ((8, part), F32)}
    scratch = saved_shapes(tokens, width, turn.e, turn.f)
    scratch |= {MEAN: ((tokens, 1), F32), INVERSE_STD: ((tokens, 1), F32)}
    scratch |= scratch_shapes_back(tokens, turn.e, turn.f) | {"partial_g": full, G: full, PARTIAL: full}
    scratch |= {key + "_x": value for key, value in scatter_dict(rows, part).items()}
    scratch |= {MEAN_BLOCK: ((rows, 1), F32), STD_BLOCK: ((rows, 1), F32)}
    scratch |= {GAIN_BLOCK: ((1, part), F32)}
    scratch |= weight_scratch(turn) | scatter_dict(rows, part) | back_dict(rows, part)
    return remote_call(
        functools.partial(middle_body, turn, rows, part),
        "middle",
        BWD,
        inputs,
        outputs,
        scratch,
        240,
        in_hbm=[X1] + [TURNED + name for name in NAMES],
        staged=[D_W + name for name in NAMES],
    )


LATER = (OUT, DOWN, UP, QKV)


ENTERING = (G, HIDDEN, ATT, SLOPE, NORMED, QKV, COSINE, SINE)


def last_body(turn, rows, part, r):
    w = Wire(r.send_sems, r.recv_sems)
    s = w.section
    half = rows // GROUPS
    brought = stage(r, ENTERING, 20)
    loads = {}
    for i, name in enumerate(FIRST):
        loads[name] = pltpu.make_async_copy(
            getattr(r, TURNED + name).at[0], getattr(r, W + name), r.local_sems.at[i]
        )
        loads[name].start()
    moves = [(ds, dc) for ds in (0, 1) for dc in range(4) if (ds, dc) != (0, 0)]

    def away(ds, dc):
        return {SECTION: (s + ds) % 2, CTX: (w.c + dc) % 4}

    w.greet([away(*move) for move in moves] + [w.beside, w.core, diagonal(w)])
    places = [(2, w.c_far), (1, w.c_up), (3, w.c_down), (0, w.c)]
    grads0 = {name: getattr(r, D_W + name) for name in NAMES}
    grads1 = {name: getattr(r, ONE + name) for name in NAMES}
    arrived = {name: getattr(r, ARRIVED + name) for name in NAMES}
    outs = {name: getattr(r, HOME + name) for name in NAMES}
    kept = {name: getattr(r, KEPT + name) for name in NAMES}
    across, home, keeps = {}, {}, {}

    def send_across(name):
        for step, c in places:
            across[name, step] = w.send_one_of(
                s == 0,
                turn.turned(name, grads1[name], c),
                turn.turned(name, grads0[name], c),
                turn.turned(name, arrived[name], c),
                w.across,
            )

    def keep(name, c, slot):
        copy = pltpu.make_async_copy(
            turn.turned(name, grads1[name], c), kept[name].at[slot], r.local_sems.at[8 + 2 * NAMES.index(name) + slot]
        )
        copy.start()
        return copy

    def settle():
        for name in LATER:
            waiting = keep(name, places[0][1], 0)
            for i, (step, c) in enumerate(places):
                waiting.wait()
                if i < 3:
                    waiting = keep(name, places[i + 1][1], (i + 1) % 2)
                across[name, step].wait_recv()
                theirs = turn.turned(name, arrived[name], c)
                mine = jnp.where(
                    s == 0,
                    turn.turned(name, grads0[name], c)[...].astype(F32),
                    kept[name][i % 2].astype(F32),
                )
                theirs[...] = (mine + theirs[...].astype(F32)).astype(BF16)
                spot = turn.shard(name, outs[name], w.c)
                if step:
                    home[name, step] = w.send(theirs, spot, {CTX: c})
                else:
                    home[name, 0] = pltpu.make_async_copy(
                        theirs, spot, r.local_sems.at[16 + NAMES.index(name)]
                    )
                    home[name, 0].start()
                yield

    start, open_branches, grad_rows, grad_up, attend_back, unrotate, grad_qkv, close, count = (
        backward_steps(r)
    )
    wide = 4 * part // TILE
    start()
    for name in ENTERING[:3]:
        brought[name].wait()
    each(wide, grad_rows)
    for name in ENTERING[3:]:
        brought[name].wait()
    send_across(OUT)
    send_across(DOWN)
    settling = settle()
    loads[DOWN].wait()
    loads[OUT].wait()
    each(count, open_branches)
    pull(settling)
    each(wide, grad_up)
    send_across(UP)
    pull(settling)
    for i in range(count):
        attend_back(i)
        pull(settling)
    r.all_acts[0] = r.act[...]
    r.all_acts[1] = r.act1[...]
    r.acts[s] = r.all_acts[s]
    pairs = [w.send(r.all_acts.at[1 - s], r.acts.at[s], w.across)]
    each(count, unrotate)
    each(wide, grad_qkv)
    send_across(QKV)
    pull(settling)
    loads[QKV].wait()
    loads[UP].wait()
    scatter = scatter_of(w, r, r.partial, rows, part)
    scatter.begin(close)
    slab = part // 4
    columns = pl.ds(pl.multiple_of(w.t * part + w.c * slab, 128), slab)
    n_up = r.d_b_up.shape[1] // slab
    r.small[0, 0:3] = r.d_b_qkv[...]
    r.small[1, 0:3] = r.one_b_qkv[...]
    for i in range(n_up):
        lanes = slice(i * slab, (i + 1) * slab)
        r.small[0, 3 + i : 4 + i] = r.d_b_up[:, lanes]
        r.small[1, 3 + i : 4 + i] = r.one_b_up[:, lanes]
    r.small[0, 3 + n_up : 4 + n_up] = jnp.sum(r.g[:, columns].astype(F32), axis=0, keepdims=True)
    r.small[1, 3 + n_up : 4 + n_up] = r.one_b_out[...]
    small_copy = w.send(r.small.at[1 - s], r.small_in, w.across)
    for i, _ in enumerate(scatter.steps()):
        if i % 4 == 3:
            pull(settling)
    r.mean_block[...] = r.mean[pl.ds(pl.multiple_of(w.c * rows, rows), rows)]
    r.std_block[...] = r.inverse_std[pl.ds(pl.multiple_of(w.c * rows, rows), rows)]
    r.gain_block[...] = own_gain(w, r, 0)
    norm_back(
        w,
        scatter,
        (r.grad1, r.x_block, r.mean_block, r.std_block, r.gain_block),
        (r.d_normed, r.row_out, r.row_in),
        rows,
        part,
        r.all_grads.at[0],
        r.sums0,
        lambda group: None,
        settling,
    )
    r.all_grads[1] = r.grad1[...]
    r.grads[s] = r.all_grads[s]
    pairs.append(w.send(r.all_grads.at[1 - s], r.grads.at[s], w.across))
    for layer, sums in ((0, r.sums0), (1, r.sums1)):
        for c in range(4):
            r.norm_out[layer, c] = sums[:, c * slab : (c + 1) * slab]
    told = [
        w.send(r.norm_out.at[(s + ds) % 2, (w.c + dc) % 4], r.norm_in.at[slot], away(ds, dc))
        for slot, (ds, dc) in enumerate(moves)
    ]
    for _ in settling:
        pass
    small_copy.wait_recv()
    r.small_sum[...] = r.small[s] + r.small_in[...]
    total = r.norm_out[s, w.c]
    for slot, copy in enumerate(told):
        copy.wait_recv()
        total += r.norm_in[slot]
    r.norm_sum[...] = total
    for name in LATER:
        home[name, 0].wait()
        for step in (1, 3, 2):
            home[name, step].wait_recv()
    for copy in pairs:
        copy.wait_recv()
    w.drain()


def last(made, mid, tables, turn, rows, part):
    tokens, width = 4 * rows, 4 * part
    full = ((tokens, width), BF16)
    e, f = 4 * turn.e, 4 * turn.f
    homes = {
        QKV: (3, turn.d, e),
        OUT: (e, turn.d),
        UP: (turn.d, f),
        DOWN: (f, turn.d),
    }
    inputs = {G: mid[G1], "grad1": mid[GRAD], ACT1: mid[ACT1], "sums1": mid[SUMS]}
    inputs |= {key: made[key] for key in SAVED + (MEAN, INVERSE_STD, VECTORS, ACT, X_BLOCK)}
    inputs |= {ONE + name: mid[D_W + name] for name in NAMES}
    inputs |= {ONE + name: mid["d_" + name] for name in (B_QKV, B_UP, B_OUT)}
    inputs |= {TURNED + name: made[TURNED + name] for name in NAMES} | tables
    pairs = ((2, rows, part), BF16)
    outputs = {HOME + name: (homes[name], BF16) for name in NAMES}
    outputs |= {ACTS: pairs, GRADS: pairs}
    outputs |= {SMALL_SUM: ((8, part // 4), F32), NORM_SUM: ((8, part // 4), F32)}
    scratch = grad_shapes(width, turn.e, turn.f) | {PARTIAL: full}
    scratch |= {ARRIVED + name: (turn.turned_shape(name), BF16) for name in NAMES}
    scratch |= {KEPT + name: ((2,) + turn.piece_shape(name), BF16) for name in NAMES}
    scratch |= scratch_shapes_back(tokens, turn.e, turn.f)
    scratch |= {W + name: (turn.turned_shape(name), BF16) for name in NAMES}
    scratch |= scatter_dict(rows, part) | back_dict(rows, part)
    scratch |= {
        MEAN_BLOCK: ((rows, 1), F32),
        STD_BLOCK: ((rows, 1), F32),
        GAIN_BLOCK: ((1, part), F32),
        "small": ((2, 8, part // 4), F32),
        "small_in": ((8, part // 4), F32),
        "sums0": ((8, part), F32),
        "norm_out": ((2, 4, 8, part // 4), F32),
        "norm_in": ((7, 8, part // 4), F32),
        "all_acts": pairs,
        "all_grads": pairs,
    }
    return remote_call(
        functools.partial(last_body, turn, rows, part),
        "last",
        LAST,
        inputs,
        outputs,
        scratch,
        140,
        in_hbm=[TURNED + name for name in NAMES] + [ONE + name for name in NAMES],
        out_hbm=[HOME + name for name in NAMES],
        staged=ENTERING,
    )


def shards(
    boundary,
    doc_ids,
    qkv_weight,
    qkv_bias,
    out_weight,
    out_bias,
    fc1_weight,
    fc1_bias,
    fc2_weight,
    fc2_bias,
    norm_gain,
    norm_shift,
):
    section = lax.axis_index(SECTION)
    rows, part = boundary.shape[2:]
    slab = out_bias.shape[1]
    n_up = fc1_bias.shape[1] // slab
    tables = doc_tables(
        lax.dynamic_index_in_dim(doc_ids, section, 0, keepdims=False), slab // HD
    )
    vectors = (out_bias, fc2_bias, norm_gain, norm_shift, qkv_bias[0], fc1_bias)
    shard_of = {QKV: qkv_weight[0], OUT: out_weight[0], UP: fc1_weight[0], DOWN: fc2_weight[0]}
    turn = Turn(shard_of[QKV].shape[1], slab, shard_of[UP].shape[1] // 4)
    made = first(boundary[0], vectors, tables, shard_of)
    mid = middle(made, tables, turn, rows, part)
    out = last(made, mid, tables, turn, rows, part)
    small, norms = out[SMALL_SUM], out[NORM_SUM]
    bias_out = small[3 + n_up][None]
    home = {name: out[HOME + name].astype(F32)[None] for name in NAMES}
    return (
        out[ACTS][None],
        out[GRADS][None],
        home[QKV],
        small[None, :3],
        home[OUT],
        bias_out,
        home[UP],
        small[3 : 3 + n_up].reshape(1, -1),
        home[DOWN],
        bias_out,
        norms[0:1],
        norms[1:2],
    )


def from_behind(value, axis, steps):
    count = lax.axis_size(axis)
    leading, last = (max(0, -steps), min(count, count - steps))
    return lax.ppermute(value, axis, [(source, source + steps) for source in range(leading, last)])


def gelu(value):
    inner = jnp.tanh(GELU_C * (value + GELU_K * value * value * value))
    return 0.5 * value * (1.0 + inner)


def gelu_slope(value):
    inner = jnp.tanh(GELU_C * (value + GELU_K * value * value * value))
    return 0.5 * (1.0 + inner) + 0.5 * value * (1.0 - inner * inner) * GELU_C * (
        1.0 + 3.0 * GELU_K * value * value
    )


def local_layout(ids_full, ctx_index, tokens):
    length = ids_full.shape[0]
    local_ids = lax.dynamic_slice_in_dim(ids_full, ctx_index * tokens, tokens)
    start = jnp.sum((ids_full[None, :] < local_ids[:, None]).astype(jnp.int32), axis=1)
    query_at = ctx_index * tokens + jnp.arange(tokens, dtype=jnp.int32)
    key_at = jnp.arange(length, dtype=jnp.int32)
    allowed = (key_at[None, :] <= query_at[:, None]) & (ids_full[None, :] == local_ids[:, None])
    return (query_at - start, allowed)


def score_block(query, keys):
    return jnp.einsum(SCORES_EQ, query, keys, preferred_element_type=jnp.float32) * HD ** (
        -0.5
    )


def forward_layer(layer_in, ids_full, params, ctx_index):
    w_qkv, b_qkv, w_out, b_out, w_up, b_up, w_down, b_down, gain, shift = params
    tokens = layer_in.shape[0]
    heads = w_qkv.shape[2] // HD
    wide_in = layer_in.astype(jnp.float32)
    row_sums = lax.psum((jnp.sum(wide_in, axis=1), jnp.sum(wide_in * wide_in, axis=1)), TP)
    row_mean = row_sums[0] / D
    variance = row_sums[1] / D - row_mean * row_mean
    inverse_std = lax.rsqrt(variance + EPS)
    centered = (wide_in - row_mean[:, None]) * inverse_std[:, None]
    normed_part = (centered * gain.astype(jnp.float32) + shift.astype(jnp.float32)).astype(
        jnp.bfloat16
    )
    normed = lax.all_gather(normed_part, TP, axis=1, tiled=True)
    positions, allowed = local_layout(ids_full, ctx_index, tokens)
    cosine, sine = rope_tables(positions)
    projected = (
        jnp.einsum("td,cde->cte", normed, w_qkv, preferred_element_type=jnp.float32)
        + b_qkv.astype(jnp.float32)[:, None, :]
    )
    query = rotate(projected[0].reshape(tokens, heads, HD), cosine, sine, 1.0).astype(jnp.bfloat16)
    key_rot = rotate(projected[1].reshape(tokens, heads, HD), cosine, sine, 1.0).astype(
        jnp.bfloat16
    )
    value_part = projected[2].reshape(tokens, heads, HD).astype(jnp.bfloat16)
    key_all, value_all = (
        lax.all_gather(key_rot, CTX, axis=0, tiled=True),
        lax.all_gather(value_part, CTX, axis=0, tiled=True),
    )
    scores = score_block(query, key_all)
    totals = jnp.sum(jnp.where(allowed[None], jnp.exp(scores), 0.0), axis=2)
    log_total = jnp.log(totals)
    probs = jnp.where(allowed[None], jnp.exp(scores - log_total[:, :, None]), 0.0).astype(
        jnp.bfloat16
    )
    attended = (
        jnp.einsum(HEADS_EQ, probs, value_all, preferred_element_type=jnp.float32)
        .astype(jnp.bfloat16)
        .reshape(tokens, heads * HD)
    )
    hidden_pre = jnp.dot(normed, w_up, preferred_element_type=jnp.float32) + b_up.astype(
        jnp.float32
    )
    hidden = gelu(hidden_pre).astype(jnp.bfloat16)
    summands = jnp.dot(attended, w_out, preferred_element_type=jnp.float32) + jnp.dot(
        hidden, w_down, preferred_element_type=jnp.float32
    )
    mixed = lax.psum_scatter(summands, TP, scatter_dimension=1, tiled=True)
    layer_out = (wide_in + mixed + b_out.astype(jnp.float32) + b_down.astype(jnp.float32)).astype(
        jnp.bfloat16
    )
    kept = (key_rot, value_part)
    return (
        layer_out,
        (centered, inverse_std, normed, query, kept, attended, log_total, hidden_pre, hidden),
    )


def backward_layer(incoming, saved, ids_full, params, ctx_index):
    w_qkv, b_qkv, w_out, b_out, w_up, b_up, w_down, b_down, gain, shift = params
    centered, inverse_std, normed, query, kept, attended, log_total, hidden_pre, hidden = saved
    tokens = query.shape[0]
    heads = query.shape[1]
    wide_grad = incoming.astype(jnp.float32)
    grad_rows = lax.all_gather(incoming, TP, axis=1, tiled=True)
    grad_out_bias = jnp.sum(wide_grad, axis=0)
    grad_out = jnp.einsum("tk,te->ke", attended, grad_rows, preferred_element_type=jnp.float32)
    d_attended = jnp.einsum(
        "te,ke->tk", grad_rows, w_out, preferred_element_type=jnp.float32
    ).astype(jnp.bfloat16)
    grad_down = jnp.einsum("tf,te->fe", hidden, grad_rows, preferred_element_type=jnp.float32)
    d_pre = jnp.einsum(
        "te,fe->tf", grad_rows, w_down, preferred_element_type=jnp.float32
    ) * gelu_slope(hidden_pre)
    grad_up_bias = jnp.sum(d_pre, axis=0)
    d_hidden = d_pre.astype(jnp.bfloat16)
    grad_up = jnp.einsum("td,tf->df", normed, d_hidden, preferred_element_type=jnp.float32)
    key_all, value_all = (
        lax.all_gather(kept[0], CTX, axis=0, tiled=True),
        lax.all_gather(kept[1], CTX, axis=0, tiled=True),
    )
    positions, allowed = local_layout(ids_full, ctx_index, tokens)
    cosine, sine = rope_tables(positions)
    d_heads = d_attended.reshape(tokens, heads, HD)
    out_heads = attended.reshape(tokens, heads, HD)
    delta = jnp.sum(d_heads.astype(jnp.float32) * out_heads.astype(jnp.float32), axis=2)
    scores = score_block(query, key_all)
    probs = jnp.where(allowed[None], jnp.exp(scores - log_total[:, :, None]), 0.0)
    d_probs = jnp.einsum(SCORES_EQ, d_heads, value_all, preferred_element_type=jnp.float32)
    d_scores = (probs * (d_probs - delta.T[:, :, None]) * HD ** (-0.5)).astype(jnp.bfloat16)
    d_query = jnp.einsum(HEADS_EQ, d_scores, key_all, preferred_element_type=jnp.float32)
    key_terms = jnp.einsum(KEYS_EQ, d_scores, query, preferred_element_type=jnp.float32)
    value_terms = jnp.einsum(
        KEYS_EQ, probs.astype(jnp.bfloat16), d_heads, preferred_element_type=jnp.float32
    )
    d_key, d_value = (
        lax.psum_scatter(
            key_terms.astype(jnp.bfloat16), CTX, scatter_dimension=0, tiled=True
        ).astype(jnp.float32),
        lax.psum_scatter(
            value_terms.astype(jnp.bfloat16), CTX, scatter_dimension=0, tiled=True
        ).astype(jnp.float32),
    )
    d_projected = jnp.stack(
        [rotate(d_query, cosine, sine, -1.0), rotate(d_key, cosine, sine, -1.0), d_value]
    ).reshape(3, tokens, heads * HD)
    grad_qkv_bias = jnp.sum(d_projected, axis=1)
    d_qkv = d_projected.astype(jnp.bfloat16)
    grad_qkv = jnp.einsum("td,cte->cde", normed, d_qkv, preferred_element_type=jnp.float32)
    normed_terms = jnp.einsum("cte,cde->td", d_qkv, w_qkv, preferred_element_type=jnp.float32)
    normed_terms = normed_terms + jnp.einsum(
        "tf,df->td", d_hidden, w_up, preferred_element_type=jnp.float32
    )
    d_normed = lax.psum_scatter(
        normed_terms.astype(jnp.bfloat16), TP, scatter_dimension=1, tiled=True
    ).astype(jnp.float32)
    grad_gain = jnp.sum(d_normed * centered, axis=0)
    grad_shift = jnp.sum(d_normed, axis=0)
    scaled = d_normed * gain.astype(jnp.float32)
    row_terms = lax.psum((jnp.sum(scaled, axis=1), jnp.sum(scaled * centered, axis=1)), TP)
    grad_in = wide_grad + inverse_std[:, None] * (
        scaled - row_terms[0][:, None] / D - centered * (row_terms[1][:, None] / D)
    )
    grads = (
        grad_qkv,
        grad_qkv_bias,
        grad_out,
        grad_out_bias,
        grad_up,
        grad_up_bias,
        grad_down,
        grad_out_bias,
        grad_gain,
        grad_shift,
    )
    return (grad_in.astype(jnp.bfloat16), grads)


def base_shards(
    boundary,
    doc_ids,
    qkv_weight,
    qkv_bias,
    out_weight,
    out_bias,
    fc1_weight,
    fc1_bias,
    fc2_weight,
    fc2_bias,
    norm_gain,
    norm_shift,
):
    section = lax.axis_index(SECTION)
    ctx_index = lax.axis_index(CTX)
    micro = boundary.shape[1]
    tokens = boundary.shape[2]
    width_part = boundary.shape[3]
    params = (
        lax.all_gather(qkv_weight[0], CTX, axis=1, tiled=True),
        lax.all_gather(qkv_bias[0], CTX, axis=1, tiled=True),
        lax.all_gather(out_weight[0], CTX, axis=1, tiled=True),
        lax.all_gather(out_bias[0], CTX, axis=0, tiled=True),
        lax.all_gather(fc1_weight[0], CTX, axis=0, tiled=True),
        lax.all_gather(fc1_bias[0], CTX, axis=0, tiled=True),
        lax.all_gather(fc2_weight[0], CTX, axis=1, tiled=True),
        lax.all_gather(fc2_bias[0], CTX, axis=0, tiled=True),
        lax.all_gather(norm_gain[0], CTX, axis=0, tiled=True),
        lax.all_gather(norm_shift[0], CTX, axis=0, tiled=True),
    )
    inputs = boundary[0]
    ticks = jnp.arange(micro + 1, dtype=jnp.int32)

    def forward_tick(received, tick):
        index = jnp.clip(tick - section, 0, micro - 1)
        first = lax.dynamic_index_in_dim(inputs, index, 0, keepdims=False)
        layer_in = jnp.where(section == 0, first, received)
        ids_full = lax.dynamic_index_in_dim(doc_ids, index, 0, keepdims=False)
        layer_out, saved = forward_layer(layer_in, ids_full, params, ctx_index)
        passed = from_behind(layer_out, SECTION, 1)
        return (passed, (layer_out, saved))

    start_zero = jnp.zeros((tokens, width_part), jnp.bfloat16)
    leftover, (outs_all, saved_all) = lax.scan(forward_tick, start_zero, ticks)
    held = lax.optimization_barrier(
        (
            (
                qkv_weight[0],
                qkv_bias[0],
                out_weight[0],
                out_bias[0],
                fc1_weight[0],
                fc1_bias[0],
                fc2_weight[0],
                fc2_bias[0],
                norm_gain[0],
                norm_shift[0],
            ),
            outs_all,
        )
    )[0]
    back_params = (
        lax.all_gather(held[0], CTX, axis=1, tiled=True),
        lax.all_gather(held[1], CTX, axis=1, tiled=True),
        lax.all_gather(held[2], CTX, axis=1, tiled=True),
        lax.all_gather(held[3], CTX, axis=0, tiled=True),
        lax.all_gather(held[4], CTX, axis=0, tiled=True),
        lax.all_gather(held[5], CTX, axis=0, tiled=True),
        lax.all_gather(held[6], CTX, axis=1, tiled=True),
        lax.all_gather(held[7], CTX, axis=0, tiled=True),
        lax.all_gather(held[8], CTX, axis=0, tiled=True),
        lax.all_gather(held[9], CTX, axis=0, tiled=True),
    )
    zero_grads = tuple((jnp.zeros(weight.shape, jnp.float32) for weight in params))

    def backward_tick(carry, tick):
        received, totals = carry
        raw_index = tick - (1 - section)
        valid = (raw_index >= 0) & (raw_index < micro)
        index = jnp.clip(raw_index, 0, micro - 1)
        cotangent = lax.dynamic_index_in_dim(inputs, index, 0, keepdims=False)
        incoming = jnp.where(section == 1, cotangent, received)
        incoming = jnp.where(valid, incoming, jnp.zeros_like(incoming))
        position_slot = index + section
        saved = jax.tree.map(
            lambda stacked: lax.dynamic_index_in_dim(stacked, position_slot, 0, keepdims=False),
            saved_all,
        )
        ids_full = lax.dynamic_index_in_dim(doc_ids, index, 0, keepdims=False)
        grad_in, terms = backward_layer(incoming, saved, ids_full, back_params, ctx_index)
        totals = tuple((total + term for total, term in zip(totals, terms)))
        passed = from_behind(grad_in, SECTION, -1)
        return ((passed, totals), grad_in)

    (leftover_grad, totals), grads_all = lax.scan(backward_tick, (start_zero, zero_grads), ticks)
    acts = lax.dynamic_slice_in_dim(outs_all, section, micro, 0)[None]
    input_grads = lax.dynamic_slice_in_dim(grads_all, 1 - section, micro, 0)[None]
    shares = (
        lax.psum_scatter(
            totals[0].astype(jnp.bfloat16), CTX, scatter_dimension=1, tiled=True
        ).astype(jnp.float32),
        lax.psum_scatter(
            totals[1].astype(jnp.bfloat16), CTX, scatter_dimension=1, tiled=True
        ).astype(jnp.float32),
        lax.psum_scatter(
            totals[2].astype(jnp.bfloat16), CTX, scatter_dimension=1, tiled=True
        ).astype(jnp.float32),
        lax.psum_scatter(
            totals[3].astype(jnp.bfloat16), CTX, scatter_dimension=0, tiled=True
        ).astype(jnp.float32),
        lax.psum_scatter(
            totals[4].astype(jnp.bfloat16), CTX, scatter_dimension=0, tiled=True
        ).astype(jnp.float32),
        lax.psum_scatter(
            totals[5].astype(jnp.bfloat16), CTX, scatter_dimension=0, tiled=True
        ).astype(jnp.float32),
        lax.psum_scatter(
            totals[6].astype(jnp.bfloat16), CTX, scatter_dimension=1, tiled=True
        ).astype(jnp.float32),
        lax.psum_scatter(
            totals[7].astype(jnp.bfloat16), CTX, scatter_dimension=0, tiled=True
        ).astype(jnp.float32),
        lax.psum_scatter(
            totals[8].astype(jnp.bfloat16), CTX, scatter_dimension=0, tiled=True
        ).astype(jnp.float32),
        lax.psum_scatter(
            totals[9].astype(jnp.bfloat16), CTX, scatter_dimension=0, tiled=True
        ).astype(jnp.float32),
    )
    return (
        acts,
        input_grads,
        shares[0][None],
        shares[1][None],
        shares[2][None],
        shares[3][None],
        shares[4][None],
        shares[5][None],
        shares[6][None],
        shares[7][None],
        shares[8][None],
        shares[9][None],
    )


def solution(mesh):
    specs = {
        TOKEN: P(SECTION, None, CTX, TP),
        ROWS: P(SECTION, TP, CTX),
        COLUMNS: P(SECTION, CTX, TP),
        VECTOR: P(SECTION, (TP, CTX)),
        VECTORS: P(SECTION, None, (TP, CTX)),
    }
    weights = (TOKEN, VECTORS, ROWS, VECTOR, COLUMNS, VECTOR, ROWS, VECTOR, VECTOR, VECTOR)
    placed = tuple(specs[name] for name in weights)
    heads = D // HD
    place = {SECTION: 2, CTX: 4, TP: 4}
    whole_heads = heads % (mesh.shape[TP] * mesh.shape[CTX]) == 0
    return jax.shard_map(
        shards if whole_heads and dict(mesh.shape) == place else base_shards,
        mesh=mesh,
        in_specs=(specs[TOKEN], P(), *placed),
        out_specs=(specs[TOKEN], specs[TOKEN], *placed),
        check_vma=False,
    )
```
